128 devices in a mesh: fr: 2 (over core), sr: 16 (over z, x), sc: 4 (over y).
Axes of the slice: x: 4, y: 4, z: 4, core: 2. Of those that a mesh axis runs over, the one named last changes fastest.
Arguments:
- spec_re: bfloat16 [8, 8192, 256], P('fr', ('sr', 'sc')), may hold values from -6 to 6
- spec_im: bfloat16 [8, 8192, 256], P('fr', ('sr', 'sc')), may hold values from -6 to 6
- offsets: int32 [64, 33], P(('sr', 'sc')), may hold values from 0 to 32, each once within a row
Outputs:
- cross: float32 [8, 64, 33, 128, 256], P('fr', ('sr', 'sc'))
The draws below stay inside these ranges and needn't reach their ends.
Inputs may be any that keep to these rules, and one draw needn't show every extreme that they name: Each row of offsets names every offset 0 to 32 exactly once.
All inputs are finite; a program needn't handle non-finite values.
Results may differ from the reference program's by a relative error of at most 0.0003.
Values may be sent and summed in bfloat16 or wider, within the bound.
A program may use at most 128 MiB of HBM per device.

```python
import math
import jax
import jax.numpy as jnp
from jax import lax

BLK = 128
SEG = 256
NB = 64
HALF = 33
STATIONS = 8192
FREQ = 8


def block_levels(stream_key, dims, split, low, top_value):
    gain = 1.0
    for position, blocks in split:
        draws = jax.random.uniform(jax.random.fold_in(jax.random.fold_in(stream_key, 6), position), (blocks,), jnp.float32, low / len(split), top_value / len(split))
        gain = gain * jnp.repeat(jnp.exp(draws), dims[position] // blocks).reshape((-1,) + (1,) * (len(dims) - 1 - position))
    return gain


def centred(key, shape, deviation, reach, cuts=(), held_as=jnp.bfloat16):
    values = jax.random.normal(key, shape, jnp.float32) * deviation
    if len(cuts) > 0:
        values = block_levels(key, shape, cuts, -0.22, 0.18) * values
    return jnp.clip(values, min=-reach, max=reach).astype(held_as)


def setup_inputs(seed: int = 0) -> dict:
    arg_keys = jax.random.split(jax.random.key(seed), 4)
    spec_re = centred(arg_keys[0], (FREQ, STATIONS, SEG), 1.0, 6.0, ((0, 2), (1, 64)))
    spec_im = centred(arg_keys[1], (FREQ, STATIONS, SEG), 1.0, 6.0, ((0, 2), (1, 64)))
    offsets = jax.vmap(lambda own: jax.random.permutation(own, HALF))(jax.random.split(arg_keys[2], NB)).reshape((NB, HALF)).astype(jnp.int32)
    return {"spec_re": spec_re, "spec_im": spec_im, "offsets": offsets}


def reference(spec_re, spec_im, offsets):
    real_full = spec_re.astype(jnp.float32)
    imag_full = spec_im.astype(jnp.float32)
    band_power = lax.optimization_barrier(jnp.sum(real_full * real_full + imag_full * imag_full, axis=(0, 2))) / (FREQ * SEG)
    gain_table = (1.0 / jnp.sqrt(band_power)).reshape(NB, BLK)
    real_blocks = real_full.reshape(FREQ, NB, BLK, SEG)
    imag_blocks = imag_full.reshape(FREQ, NB, BLK, SEG)
    norm_scale = 1.0 / math.sqrt(SEG)
    highest = lax.Precision.HIGHEST

    def one_block(block_index):
        partners = ((block_index + offsets[block_index]) % NB).astype(jnp.int32)
        own_re = real_blocks[:, block_index]
        own_im = imag_blocks[:, block_index]
        other_re = real_blocks[:, partners]
        other_im = imag_blocks[:, partners]
        real_part = jnp.einsum('fis,fmjs->fmij', own_re, other_re, precision=highest) + jnp.einsum('fis,fmjs->fmij', own_im, other_im, precision=highest)
        imag_part = jnp.einsum('fis,fmjs->fmij', own_im, other_re, precision=highest) - jnp.einsum('fis,fmjs->fmij', own_re, other_im, precision=highest)
        weight = gain_table[block_index][None, None, :, None] * gain_table[partners][None, :, None, :] * norm_scale
        return jnp.concatenate([real_part * weight, imag_part * weight], axis=-1)
    joined = lax.map(one_block, jnp.arange(NB, dtype=jnp.int32))
    return jnp.transpose(joined, (1, 0, 2, 3, 4))
```

```python
import functools
import math

import jax
import jax.numpy as jnp
from jax import lax
from jax.experimental import pallas as pl
from jax.experimental.pallas import tpu as pltpu
from jax.sharding import PartitionSpec as P

MESH = pl.DeviceIdType.MESH

PLAN = (
    (0x00000100ffffffffffffffffffffffff, 0x010201030301010300030200ffffffff, 0x00ffffff03ffffff00ffffff00ffffff, 0x030003ff000301ff030101ff030200ff, 0xffffffffffffffffffffffffffffffff, 0x03010002020200010103020000030002),
    (0x02030201ffffffffffffffffffffffff, 0x020302010100020002000302ffffffff, 0x02ffffff01ffffff02ffffff01ffffff, 0x020302ff010002ff020000ff020002ff, 0xffffffffffffffffffffffffffffffff, 0x02030201010002000202000101000303),
    (0x0102030252525051515352503c535052, 0x03010008020303025115060350535052, 0x01515052155250515115521703535052, 0x01025052525250515115061750530152, 0xffffffffffffffffffffffffffffffff, 0x01020303000103020301010303010101),
    (0x0404040451505250525250515150533c, 0x04040404040404040404040451505353, 0x04535251045015500452505104505353, 0x04040451040404500404045104045353, 0xffffffffffffffffffffffffffffffff, 0x04040404040404040404040404040400),
    (0x03513c53503f53525351515353515151, 0x4c000500500550175317510653515151, 0x53525353503f53525317515302515151, 0x00080553030553521708175314511751, 0xffffff55ff575755ff56ff60655558ff, 0x00000500030301060000030202020204),
    (0x434b4d3d545454545454545454545450, 0x434d4d5242104c014d52121854545450, 0x15543e543e5454544d5454544b545450, 0x153c01543e3e15543d52055451545450, 0xffffffffffffffffffffffffffffff58, 0x15140117423e15540854125444545450),
    (0x423e4c3c53533e3c5050535252525254, 0x4d05530f4d024b56424d4c5152525254, 0x3d4e54506053513c3f4b535252525254, 0x3d2b3e503f513c3c501c535252520754, 0xffffff6260ffff5864ff6462678d788f, 0x141515163a3f3e3c424d535252525254),
    (0x4f404f3e403d403f584f623d94554e53, 0x4e4b4f674f4f4d2444514e0a424b4c5a, 0x4e4d4067404f181840511816544b4040, 0x4040403e40574018403c3c1694555040, 0xffffffff5761616656ff575c61875659, 0x18401415403d403f404f3c0a424b1a51),
    (0x3e3c4b433c4c514192a44d4e7e8d3fa4, 0x4f654b6661574f1c4f4b4f6a564d60a0, 0x4050656661513d14164c16283e4c3f3c, 0x173f166616403d143f553d6a3e19083c, 0xffffffff61ff566f61555f6a567a6078, 0x171717503c4c3c413f3f3f28434c4d18),
    (0x3d420d4c3e433f4d4341415a403788a0, 0x50640d624b4e191a434e4d1c45a45aa4, 0x4f4f51134b3c3f24121417388b3b173f, 0x3f454114183c051718533e2b4017093f, 0xffff625d625f5c5f63ff60588b61887a, 0x54093f133e195323281c213840294016),
    (0x4839440a44444e4245454090a24fa44d, 0x651165244561378c58116305634f6359, 0x3e6567644e798c704f11639063616314, 0x3c6567642d793e8f75428f186756787f, 0x576061ff637967706a7963ff585f637f, 0x40393e433d1b4e423d114e254c4e3e4d),
    (0x4e4c4a0d4c3c56463e3e714f36a29088, 0x64684a5512116576174f71884da25761, 0x3f678f684f8d636f118f5f8c65797863, 0x6468303c923d061c1c8f581492796a78, 0xffffff5e7e78ff76756b74ff797e6188, 0x3f113c3c41514b501c1d2d2e4e434930),
    (0x4b4140458d38434f8e565a41929c809a, 0x4b625f63076b571f141318215c5f5972, 0x2868120f8d259e3a131333395c878b9a, 0x2f41452e8d4479928e2902886c7a8014, 0x60625f6c74877e5d5b7a8b5e847c8072, 0x3c3b40453f4f1f3a474c51434b3c0f46),
    (0x492f4139319790456a8f944293979d59, 0x4a0f1151785e11690f09107e61975e6f, 0x64298c25783a674f224f7c1318633874, 0x2c302b1d808f427c1a1d7c8a086c9018, 0x628a63ff78975e698a5e7c5d57638679, 0x2f2f27392f3a394622414130364f3f1c),
    (0x2f340a3780326f1f7e213b939b7e8e49, 0x050d1d5d8a690a660b1b152058576274, 0x6861634d8c1173172c8e61746c4d5f9c, 0x28011d288c6b9e2d928e71933c8d7f80, 0x63696aff5f76737b809387867a737f7e, 0x3e3e0a1b203c46524d503a3305191e49),
    (0x403850058fa1893a904d475c82407d40, 0x0e10771c09621477590e07229b9f6f66, 0x8c4c77118f285f778d72147d239f9972, 0x681c8c4079428e2e7b2a917e562c7d85, 0x7983ff736d85805e7b72947d82567d7d, 0x203c414a4b23352d464447392d1d1c19),
    (0x4d5e484a8a9970a3891f93a4848c467f, 0x078920530f8d6b7018121e0971716184, 0x118a7c395f9025718ea0233528179799, 0x2d838f302e43707e1b7d7a947f6b361a, 0x5c5b5b776a99708789836f8a71709775, 0x434d4d53310d4a3d52211e512b414627),
    (0x4c33210b7f8e8c966f806f969aa49581, 0x136309220d5a7e7e561c0d5c94627755, 0x3838754c7a9c6f8c900f373b2b3d2478, 0x3164352d568e301a0b4390a07d6d7e81, 0x7b5eff91566272776f80939685886f81, 0x194c2f30223245484c2c4b2c4614241e),
    (0x1f240e2e8b909a8d8594a17f5c845a99, 0x708e10208020853785717f845e846d85, 0x708e258c8b9d618d399d3b362a739d28, 0x708e7c1c318d80308483948c0b089658, 0x7677889b5e6e7f71855a7a7f5c84846b, 0x3d3f44364e2048474a450e4e120d4c37),
    (0x21653f626f8c962e3093818196997083, 0x85908c8074855636101d61809699999c, 0x108d4c8224a1397f10904d9f4c124d2a, 0x7f8d6a828f9c7ea4089092895764066e, 0x5887788f797e5d6e9b5c929c6c717e83, 0x1e363b474f214d360a15504147335153),
    (0x45593e63888d92979a8388207d4b1f32, 0x8d59223590328b651f56160b7086a498, 0x768f86a0728a9b8723626c11120f2311, 0x8e9c77a36d9294199e717d90152e0584, 0x896d6979985e949b6e7f588489657098, 0x45534f54530534515136464b45504a40),
    (0x65535f4f978587353a789a80476c9986, 0x90538b648f8e6f7384253112a25d5894, 0x907a5f9b029f9d8f186da36a5e2c4b9d, 0x909d7f9595945e3a7d6d32a4090d8e86, 0x5b7c827f8b807a7f848969995e5b5b9b, 0x4c4e4a515250333850480d48532f310d),
    (0x684f0566839c8d9279778f888895942d, 0x414c905e856a905d8b2100366e828592, 0x8f879ba375628d1514299fa188153269, 0x949386a09e9d5f5506306e362d307749, 0x8a93865c975a5b89866a5a767f5a5e65, 0x4f4f4720504b184f2c24523e4d30503a),
    (0x640d55559b8a83a2469732a2698f8184, 0x7f7f146543178950070725108248757e, 0x839d87a18ea2117358a43f9d141e110f, 0x798491a1817357a3851888392326261e, 0x5f728794649879755d85889d63667770, 0x524b504c0a4e09302618171c2346533e),
    (0x530e07128c80998a9679a37c4f5d846f, 0x63065d81238213860e302e4a6a989297, 0x6c838280239b3186564660253d1f8e27, 0x9c9e8879228c16769672182f179a3f46, 0x86997384806c8a7c7f78956b70866993, 0x5350211d09454c092134065330273a14),
    (0x5236471b9583849c7a9d8a7e97a03d7c, 0x186d124c632479101a8f522e9a5b9395, 0x629c9c850e8e6d65489897897e2b934d, 0x9f9f949a6f5386488245247154104a2c, 0x5a75937c849a6b7282776c9775746d95, 0x4d5249401e062c12151f250933403d06),
    (0x552b4623948f82897f91766b45417a6a, 0x1f3955161955414b648948489d929c9b, 0x93a0968f356d7f2154335c2b53925d7e, 0x8f7e93892a5547675876764b42717175, 0x875a7dff756f82787981997a6e9294ff, 0x511b1b4d192527110c140b113c3a1710),
    (0x1e3f2c3586879591913f78672d7487a3, 0x5f4552365f3345555b5a287899796a93, 0x699b6f79223d4b306865906d58657b70, 0x9590757c8633566b5481504763508468, 0x6b7a6fff86918b9e9e9a6b949affffff, 0x50481c1e1c342dff16233e1e14314eff),
    (0xffffffff9082869b5dff69ff7f7affff, 0xff4461ff4a12ff52ffffffff9593949d, 0x7ba37992ff8c6b1fff6cffffffffffff, 0x8d756f80ffffff8a8834ffffffffffff, 0x737e79ffff72ffff99ffffffffffffff, 0x4930261926ffffffff0f2eff18ffffff),
    (0xffffffff986998ffffffffffffffffff, 0xffffffffffffffffffffffff92ff9aff, 0x4b9f5dffffffffffffffffffffffffff, 0xff616d4affffffffffffffffffffffff, 0xffffffffffffffffffffffffffffffff, 0x2d0f091affffffffffffffffffffffff),
)

LAG = 2
CHUNKS = 5
SLOTS = 33
UNITS = 65
UNIT = 16
CHUNK_UNITS = UNITS // CHUNKS
OPPOSITE = (1, 0, 3, 2, 5, 4)


def neighbour_position(p, d):
    x, y = divmod(p, 4)
    if d == 0:
        x = (x + 1) % 4
    if d == 1:
        x = (x + 3) % 4
    if d == 2:
        y = (y + 1) % 4
    if d == 3:
        y = (y + 3) % 4
    return 4 * x + y


def signed(word):
    return word - (1 << 32) if word >= 1 << 31 else word


def entries(step, d):
    return [(PLAN[step][d] >> (8 * p)) & 255 for p in range(16)]


def mask_of(flags):
    return sum(1 << p for p, flag in enumerate(flags) if flag)


def gather_kernel(re_ref, im_ref, held, part, part_in, send_sem, recv_sem, load_sem, pair_sem):
    bins = re_ref.shape[0]
    tiles = re_ref.shape[1]
    fr = lax.axis_index("fr")
    sr = lax.axis_index("sr")
    sc = lax.axis_index("sc")
    z, x, y = sr // 4, sr % 4, sc
    p = 4 * x + y
    steps = len(PLAN)

    loads = []
    for f in range(bins):
        for i, ref in enumerate((re_ref, im_ref)):
            unit = (2 * f + i) * tiles
            loads.append(
                pltpu.make_async_copy(ref.at[f], held.at[0, pl.ds(unit, tiles)], load_sem.at[2 * f + i])
            )
    for load in loads:
        load.start()

    xp, xm = (x + 1) % 4, (x + 3) % 4
    yp, ym = (y + 1) % 4, (y + 3) % 4
    zp, zm = (z + 1) % 4, (z + 3) % 4
    targets = (
        (fr, 4 * z + xp, y),
        (fr, 4 * z + xm, y),
        (fr, sr, yp),
        (fr, sr, ym),
        (fr, 4 * zp + x, y),
        (fr, 4 * zm + x, y),
    )
    ahead = (4 * (xp - x), 4 * (xm - x), yp - y, ym - y, 16, -16)
    twin = (1 - fr, sr, sc)

    barrier = pltpu.get_barrier_semaphore()
    for device in targets + (twin,):
        pl.semaphore_signal(barrier, inc=1, device_id=device, device_id_type=MESH)
    for load in loads:
        load.wait()
    pl.semaphore_wait(barrier, 7)

    def chosen(step, d):
        words = [signed((PLAN[step][d] >> (32 * i)) & 0xFFFFFFFF) for i in range(4)]
        word = jnp.where(
            x < 2,
            jnp.where(x == 0, jnp.int32(words[0]), jnp.int32(words[1])),
            jnp.where(x == 2, jnp.int32(words[2]), jnp.int32(words[3])),
        )
        return lax.shift_right_logical(word, 8 * y) & 255

    def guarded(mask, action):
        if mask == 0:
            return
        if mask == 0xFFFF:
            action()
            return
        pl.when((lax.shift_right_logical(jnp.int32(mask), p) & 1) == 1)(action)

    def transfer(step, d, slot, chunk):
        rows = pl.ds(chunk * CHUNK_UNITS, CHUNK_UNITS)
        return pltpu.make_async_remote_copy(
            src_ref=held.at[slot, rows],
            dst_ref=held.at[slot - ahead[d], rows],
            send_sem=send_sem.at[d, step],
            recv_sem=recv_sem.at[d, step],
            device_id=targets[d],
            device_id_type=MESH,
        )

    def send(step, d):
        def action():
            entry = chosen(step, d)
            transfer(step, d, entry // CHUNKS, entry % CHUNKS).start()

        guarded(mask_of(v != 255 for v in entries(step, d)), action)

    def waited(step, d, dest):
        rows = pl.ds(0, CHUNK_UNITS)
        return pltpu.make_async_remote_copy(
            src_ref=held.at[0, rows],
            dst_ref=held.at[1, rows],
            send_sem=send_sem.at[d, step],
            recv_sem=recv_sem.at[d, step],
            device_id=targets[d],
            device_id_type=MESH,
        )

    def receive(step, d):
        sent = entries(step, d)
        flags = [sent[neighbour_position(q, OPPOSITE[d])] != 255 for q in range(16)]
        guarded(mask_of(flags), lambda: waited(step, d, None).wait_recv())

    def finish(step, d):
        guarded(
            mask_of(v != 255 for v in entries(step, d)),
            lambda: waited(step, d, None).wait_send(),
        )

    exchange = pltpu.make_async_remote_copy(
        src_ref=part,
        dst_ref=part_in,
        send_sem=pair_sem.at[0],
        recv_sem=pair_sem.at[1],
        device_id=twin,
        device_id_type=MESH,
    )

    for step in range(steps + LAG):
        if step >= LAG:
            for d in range(6):
                receive(step - LAG, d)
        if step < steps:
            for d in range(6):
                send(step, d)
        if step == 0:
            total = jnp.zeros((tiles, UNIT, 256), jnp.float32)
            for i in range(2 * bins):
                piece = held[0, pl.ds(i * tiles, tiles)].astype(jnp.float32)
                total += piece * piece
            total = total.reshape(tiles * UNIT, 256)
            half = total[:, :128] + total[:, 128:]
            power = jnp.sum(half.T, axis=0, keepdims=True)
            part[...] = jnp.broadcast_to(power, part.shape)
            exchange.start()
        if step == 2:
            exchange.wait()
            power = part[...] + part_in[...]
            gain = 1.0 / jnp.sqrt(power * (1.0 / 2048.0))
            gain = jnp.concatenate([gain, gain], axis=0)
            gain = jnp.concatenate([gain, gain], axis=1)
            high = gain.astype(jnp.bfloat16).astype(jnp.float32)
            middle = (gain - high).astype(jnp.bfloat16).astype(jnp.float32)
            low = gain - high - middle
            row = lax.broadcasted_iota(jnp.int32, (UNIT, 256), 0)
            rest = jnp.where(row == 1, middle, low)
            held[0, UNITS - 1] = jnp.where(row == 0, high, rest).astype(jnp.bfloat16)
    for step in range(steps):
        for d in range(6):
            finish(step, d)


def gathered(re, im):
    bins, tiles = re.shape[:2]
    steps = len(PLAN)
    return pl.pallas_call(
        gather_kernel,
        out_shape=jax.ShapeDtypeStruct((SLOTS, UNITS, UNIT, 256), jnp.bfloat16),
        in_specs=[pl.BlockSpec(memory_space=pltpu.HBM)] * 2,
        out_specs=pl.BlockSpec(memory_space=pltpu.VMEM),
        scratch_shapes=[
            pltpu.VMEM((8, 128), jnp.float32),
            pltpu.VMEM((8, 128), jnp.float32),
            pltpu.SemaphoreType.DMA((6, steps)),
            pltpu.SemaphoreType.DMA((6, steps)),
            pltpu.SemaphoreType.DMA((2 * bins,)),
            pltpu.SemaphoreType.DMA((2,)),
        ],
        compiler_params=pltpu.CompilerParams(
            collective_id=0, has_side_effects=True, vmem_limit_bytes=24 << 20
        ),
        name="gather_blocks",
    )(re, im)


GROUP = 3


def gain_row(tile):
    wide = tile.astype(jnp.float32)
    return wide[0:1, :128] + wide[1:2, :128] + wide[2:3, :128]


def cross_kernel(order, held, out):
    step = pl.program_id(0)
    own_row = gain_row(held[0, UNITS - 1]) * (1.0 / 16.0)
    own_column = jnp.broadcast_to(own_row, (128, 128)).T
    for j in range(GROUP):
        slot = order[step * GROUP + j]
        weight = own_column * gain_row(held[slot, UNITS - 1])
        for f in range(out.shape[0]):
            mine = held[0, pl.ds(16 * f, 16)].reshape(256, 256)
            other = held[slot, pl.ds(16 * f, 16)].reshape(256, 256)
            full = lax.dot_general(
                mine, other, (((1,), (1,)), ((), ())), preferred_element_type=jnp.float32
            )
            out[f, j, :, :128] = (full[:128, :128] + full[128:, 128:]) * weight
            out[f, j, :, 128:] = (full[128:, :128] - full[:128, 128:]) * weight


def local(spec_re, spec_im, offsets):
    bins, rows, segs = spec_re.shape
    tiles = rows // UNIT
    re = spec_re.reshape(bins, tiles, UNIT, segs)
    im = spec_im.reshape(bins, tiles, UNIT, segs)
    held = gathered(re, im)
    cross = pl.pallas_call(
        cross_kernel,
        grid_spec=pltpu.PrefetchScalarGridSpec(
            num_scalar_prefetch=1,
            grid=(SLOTS // GROUP,),
            in_specs=[pl.BlockSpec(memory_space=pltpu.VMEM)],
            out_specs=pl.BlockSpec((bins, GROUP, rows, 256), lambda i, order: (0, i, 0, 0)),
        ),
        out_shape=jax.ShapeDtypeStruct((bins, SLOTS, rows, 256), jnp.float32),
        compiler_params=pltpu.CompilerParams(vmem_limit_bytes=30 << 20),
        name="cross_products",
    )(offsets[0], held)
    return cross[:, None]


def solution(mesh):
    placed = (P("fr", ("sr", "sc"), None), P("fr", ("sr", "sc"), None), P(("sr", "sc"), None))
    return jax.shard_map(
        local,
        mesh=mesh,
        in_specs=placed,
        out_specs=P("fr", ("sr", "sc"), None, None, None),
        check_vma=False,
    )
```

```python
import functools
import math

import jax
import jax.numpy as jnp
from jax import lax
from jax.experimental import pallas as pl
from jax.experimental.pallas import tpu as pltpu
from jax.sharding import PartitionSpec as P

MESH = pl.DeviceIdType.MESH

PLAN = (
    (
        0x0027000d000d0000ffffffffffffffffffffffffffffffffffffffffffffffff,
        0x000d0027001a0000000d000d000d0027001a000d00270027ffffffffffffffff,
        0x000dffffffffffff001affffffffffff0000ffffffffffff001affffffffffff,
        0x000d001a0027ffff001a000d0027ffff000d000d001affff0000001a0000ffff,
        0xffffffffffffffffffffffffffffffffffffffffffffffffffffffffffffffff,
        0x00270000000000270027000d0000000d000d0027001a001a00270027000d001a,
    ),
    (
        0x000000000027001affffffffffffffffffffffffffffffffffffffffffffffff,
        0x00000000000d001a0000001a0000001a00000000000d000dffffffffffffffff,
        0x0000ffffffffffff0027ffffffffffff0027ffffffffffff000dffffffffffff,
        0x00000027000dffff0000001a001affff00270000000dffff001a000d0027ffff,
        0xffffffffffffffffffffffffffffffffffffffffffffffffffffffffffffffff,
        0x001a000d0027001a001a0000001a001a0027001a0000000d000d001a0027000d,
    ),
    (
        0x04370410041004370437041d0410041d041d0437042a042a04370319041d042a,
        0x04370410041004370437041d0410041d041d0437042a042a04370437041d042a,
        0x04370410041004370437041d0410041d041d0437042a042a04370437041d042a,
        0x04370410041004370437041d0410041d041d0437042a042a04370437041d042a,
        0xffffffffffffffffffffffffffffffffffffffffffffffffffffffffffffffff,
        0x000d001a001a000d000d002700270000001a000000270027001a000000000027,
    ),
    (
        0x042a041d0437042a042a0410042a042a0437042a0410041d033304370437041d,
        0x042a041d0437042a042a0410042a042a0437042a0410041d041d042a0437041d,
        0x042a041d0437042a042a0410042a042a0437042a0410041d041d042a0437041d,
        0x042a041d0437042a042a0410042a042a0437042a0410041d041d042a0437041d,
        0xffffffffffffffffffffffffffffffffffffffffffffffffffffffffffffffff,
        0x003400340034003400340034000d002700340034003400340034003400340034,
    ),
    (
        0x041d042a042a041d041d043704370410042a0410043704370743071c071c0743,
        0x041d042a03f6041d041d0437043704100367045e03e9046b042a041004100437,
        0x03cf042a042a04fa041d0514051404fa042a0521051405210521053b071c04fa,
        0x041d042a042a041d041d04370514053b042a045e043705210743041004780743,
        0xffff0478045104fa053b04780514053b053bffff047805210521053b071c0743,
        0x00000027000d00000000001a003400340000000d000d00000000000d001a0000,
    ),
    (
        0x044404440444044404440444041d043704440444044404440736041007430736,
        0x044404440444044404440444045e045104440444044404440444044404440444,
        0x04440444044404ed04440521053b04ed04440514052e04fa0444071c052e0743,
        0x044404440444044404440444041d052e044404440444052e0444044404440736,
        0xffff046b045e04ed052e0521053b0451052e0514052e04e00736052e052e052e,
        0x012b012b0111011e03190333032603260333033303190326036703dc03e90437,
    ),
    (
        0x0326030c0326031903330326030c0319035a03cf046b0451042a044404440437,
        0x01110478045104ed0111046b03e904fa053b03cf046b04fa03e9053b03dc04e0,
        0x041d030c012b044403cf04370437052e052e04100437043703e9052e07430521,
        0x0111011e045e0111052e0521045e0437053b0514046b0437053b045e05140521,
        0xffffffffffff0451ffffffff0451ffffffffffff046b0451053b045e051404fa,
        0x0111011e012b011103330326030c03190104011e03330319035a03f603dc0444,
    ),
    (
        0x03dc0437006800d00410042a044404440410041d041d04100680073607360729,
        0x035a03e9046b046b04d3045e0444044404e0046b051404100410041d042a0410,
        0x041004370104041d0410052e04fa0521063f053b053b0514041006db04100729,
        0x0410045e046b04100521045e044405550410046b053b05140736053b042a0729,
        0xffffffff04b9046b0478052e04780521045e053b053b05140729073607360729,
        0x011e01040104004e0326030c03330333036703e9004e04440104041004440410,
    ),
    (
        0x031900410319004e07290743073607360743074307290736077707ec07500444,
        0x0403048504b90478054805480478045e0104011e0111012b077707ec07f90847,
        0x0403053b041d050705210743054807360104054804e00507011e041d042a0444,
        0x053b053b0521030c0729048504850548054806180111055501040319012b0410,
        0xffff04850485050705480548054805480548054804e004ed0750075007500750,
        0x013801380068030c0340034003400444035a03cf0111041003e90444042a030c,
    ),
    (
        0x034003400333030c07430736071c03330367048507430485076a041d042a0410,
        0x0410052e048504850374012b005b0507046b03f605620485076a080607ec0854,
        0x053b052e0138012b054807360736072903cf04ed041d04100548054805480548,
        0x0521052e053b0138046b074304780736022f030c048506320673054804850548,
        0xffffffff04ac0485046b048504850507046b04ed048505070548054805480548,
        0x03400340013803330367012b011104370326030c0041004e030c041d004e00dd,
    ),
    (
        0x0381004e00a900c30736071c0743049f037403f6049f03330410080607f90507,
        0x034d04510104013804e0056205620104004e0111004e011e0548056204ed04b9,
        0x052e0514051404d3030c071c074304440111052e054805480326041008540410,
        0x052e05140514012b0743030c0111074305140451045e0410035a030c03740437,
        0xffffffff049f049f0492045e049f04e005d705620548054805e4070206320625,
        0x0104033303190319030c0319031901040374034003f600c3041003cf03190041,
    ),
    (
        0x034d0333049f04ac07020750075004c60673034004ac072903e9048504b90750,
        0x054800ea040304d304ed04ed011105e403cf049f03f6057c0514056f083a0820,
        0x03f6054804ed071c07360750034004d3074307430340033306250702062504d3,
        0x0548054806320562037407500743056f03260340054805480666048506320485,
        0x046b04e0063204ac04ed04ed05bd056f057c04fa06590702069a056f06180514,
        0x030c011103400326035a03f6005b030c03cf03f603400333034d01110111022f,
    ),
    (
        0x007500750075005b077706f506e804b90736071c04b904c6034d03cf07ec04e0,
        0x03f6056204780104021506320485005b049200dd00410152048503e904b905e4,
        0x0548075006180548021506f506e803400326034005210854034002220403022f,
        0x045e0562054807430485063f0319085406660743015f0340034d01450340046b,
        0x04fa057c04c604c60485063204e0057c0492048504d305fe066606b406e80618,
        0x0326032603330410021503cf03e9034003e903dc0326034003dc03e90403016c,
    ),
    (
        0x040303dc04c604c60680072907290485034d0319034d049f069a034d046b04b9,
        0x004e04d30548055505140555058905890374050704ed049f05070813058904c6,
        0x063f07430729074307500319040305140632071c03cf01c703dc034007500847,
        0x051406320618057c04510632063f0485030c031907290854056f06180451035a,
        0x04d3056f063f05620507050706250589056f056f04ed060b063f061806660589,
        0x02cb030c00ea034003cf03e903dc0410030c031903cf030c0374004103cf01e1,
    ),
    (
        0x03f603e9009c006806db07020784071c0702038103cf040303dc06a7037403b5,
        0x0507056f009c008f064c0589049f015f0485015201380138075d05a30492046b,
        0x051405210750051406db07020729023c030c022f04d3020801d405e403260340,
        0x07500618064c055506800381046b057c047806320326020803740326034d0680,
        0x0632061806db0555064c04b906e8060b05e405f105070589068d064c063f0680,
        0x031903190326044403dc02ff04030381034d0381015f040302080145037403b5,
    ),
    (
        0x050704ac049203c2067307df07f90750030c02ff073603e9025602f2081307b8,
        0x006800dd058905f104ac02ff050705d702ff0555050705fe0596038e04c6060b,
        0x071c0736050705f106f503f602ff084703f6070202150632051403f6020804ed,
        0x0673052107290589026307290367045e016c057c075004850659064c0521022f,
        0x050704ac064c05f106b404ac0680078405f106a7057c05f1063205e404c606e8,
        0x033303dc030c042a03f603b503a802d8027d02ff03b503dc038103c201ee035a,
    ),
    (
        0x0249002703e9008f079106a7049207f9079106a70492080606c107f903cf0451,
        0x049f0555008f01ba007504c600d0016c034d00ea018601fb0784057c04fa049f,
        0x0750062504fa0702072906320521020805d702cb081301fb01e101e10111030c,
        0x071c074306250729071c02150673058907770249034d068d022f022201450208,
        0x070f05f104920589056f04920507068004fa0507068d06f5064c05b0070207b8,
        0x0179040303f6043702d8038103b5035a024902cb034d020801e1038e01450367,
    ),
    (
        0x02cb005b02cb03b506f507f904ac04ac02490492080602b10784045e07d20297,
        0x00c3016c04fa015200f700f705bd060b04fa038e04c6058904ed055505070492,
        0x0736070f06db061800dd021501fb082005e403dc03f606f50618020804fa0514,
        0x0736062507430618036705890249035a035a04b9068d01520548063f06590381,
        0x05fe06250625067305fe06c1078405d704d304b90673076a0589063f065905a3,
        0x023c03f603dc039b03c2021502ff03cf0319022f035a02b1029701e103b50256,
    ),
    (
        0x0492009c008f004106c103c204b90784068d05a303b5079103a803b504c6076a,
        0x04c606e8018605d7070f04920208015201e1056f00d005f105bd0507065905a3,
        0x072905d70625082005fe070f07ec02d802e507df050703cf0222023c04ed01e1,
        0x056f07500736068d056f027d063208200743015f016c0791058902560208045e,
        0x0492070f0702061806c1067304b9079e06c1068d05f106e8050705a3068d06ce,
        0x020803cf0410015f016c01e101fb015202d801d403dc036703a802560410038e,
    ),
    (
        0x049f00f700b600ea06b406c104c603a8028a038e06e804b90297079e07ab06ce,
        0x028a008200d0019303c2009c04fa055503c201ad01ba04c605a3069a060b05d7,
        0x00dd05a30743075000f702cb021505d706c100ea02cb07ec04fa060b02ff0702,
        0x05890736027d076a016c067303b50152027d01ad0555076a023c0270056f0562,
        0x056f05a306c1070205a305a3049206b4079107d205bd068d04fa069a050704b9,
        0x028a03e901ee041d039b042a01c70208028a04030186034d016c00d0026302a4,
    ),
    (
        0x04fa006803a800b607ec03b507b8079e06c1050706f50702028a036702ff0403,
        0x070f070f00b6049206e8056f010402be00ea04b9049f004e03a8049205ca0702,
        0x074306f50403072906b407f903a802e500c303f6061803e9011102e5050705fe,
        0x023c072906800666073603190326046b06730215035a049f014500410104016c,
        0x05d706b4066606f504b904c60562070205bd049206f50791045e049205ca06c1,
        0x03cf0263018602d802970444039b028a02ff041d038103cf02be043702cb02ff,
    ),
    (
        0x008204b900ea049f04ac0478049f045104ed034d034003670507035a018602be,
        0x06f5009c0041017902a403a8019301c70145039b007500ea06c106660485069a,
        0x06db080607ec07ec020801e100d001c701c707f900f700ea00f70111010400ea,
        0x07290249071c045e0104023c01040673005b01380068045101790000023c0555,
        0x059605e40659065905ca04d3063204c605ca05a3049f04c6046b04b904ed0492,
        0x035a044403e902ff03b5027002be02be03f602b1038e03a8015201c701860186,
    ),
    (
        0x054803190082039b02b104b903a8027003c2069a076a057c039b03a808200179,
        0x01fb04c605d7011e015f004106b406f501ee004e005b005b069a0659057c057c,
        0x01ee081308060319070f01040813081304e000f70319060b00ea04ed013802e5,
        0x03670256023c04850410075d076a0270001a07b8076a026302080034005b0179,
        0x05ca06e80507049204ac07ec04c604d3045105ca04ac04ac05ca04ed04e005b0,
        0x03f6043703b502be028a028a02b102970193038e03c2042a01a002b102be03e9,
    ),
    (
        0x052e03c2045e04780297075d07ab0743048501ee02e501520659072901ee0186,
        0x0249015202f202ff071c071c027001a001d40068060b015f047804b903e90562,
        0x0618021507df0854011100f70111011e01d40806020800f7003400d000f70625,
        0x0625058907840340025602b1005b01040784035a004e057c00270777001a012b,
        0x06b4070207df0777045e056204d304b904ac0451063f0478048506db05bd04c6,
        0x03dc03c202be03a8038e038e042a02ff041d043703670270041d01ee0437012b,
    ),
    (
        0x04d3052e046b0521070f02a4045e04ed06db07df063206b4016c019306b406db,
        0x07360729071c04c6011e02700736069a005b015f00dd055507b803c20451052e,
        0x030c07df03c20326077707c506f5069a076a030c011106c1056f011e023c00d0,
        0x024901930333083a0806081307ec071c03670806078403b50555008207d20104,
        0x04b90777057c04b9058906180589048504ed04d306b4055504d304ac0478049f,
        0x03e9042a042a0381044403a80437034d042a039b041002630437027d038103cf,
    ),
    (
        0x04c60485052104fa014507c5070f06e802e502cb033302f20729078403dc0333,
        0x02ff007500ea01ad0750075001380270015f019300f7018605f1079e068d04d3,
        0x050700d007f9079e01520111039b02a401520813079e0444000001d4034000dd,
        0x064c07ec07910333011e00a9004e034007f9015201e107b8003402a400340145,
        0x04c605ca04d3060b0632057c079104920507070206ce0806062504fa0680045e,
        0x04370410043701a0041d0410041d03f604370367044403c203b5039b029703dc,
    ),
    (
        0x03a8020802560485075d01ad06f5072905a3075006a706c1035a03260729063f,
        0x074304fa05a3053b023c013805fe04ac016c0659065901c7079105f1045e04fa,
        0x05e407f900d007f9058905d706ce07b804fa011101ad06db010401ee07ab057c,
        0x01ad081305620854057c071c0784062501c707ec052e0333063f065902b1015f,
        0x056207ab0673069a04fa07ab057c07ec048506f5070f06ce06db049f057c060b,
        0x04100374038e02a4041002be028a0193039b035a01d4043700d0005b01a0034d,
    ),
    (
        0x0222032603400340035a07ab047806c103f603e904d3028a068d06b4032606e8,
        0x012b027001e100dd04fa050701ad0138008201d400c30736052107f9049f0666,
        0x031901e1070f03a80186030c031905f100a9064c05fe071cffff073601ee01d4,
        0x07ec018601fb020801ee011e062503a8068d011102080777013800a9ffff06ce,
        0x06ce064c05b00813060b075d04ac07f9064c05960555ffff06c1ffffffffffff,
        0x0444018603c20186020801d40208ffff008f01ee01c7ffff00a9ffffffffffff,
    ),
    (
        0xffffffffffffffff07c5027d079effff06e8070fffffffff03c2027dffffffff,
        0x0562ffffffffffff045e0222ffffffffffffffffffffffff03dc0451ffffffff,
        0xffff0854030c05feffff0596ffffffffffff0249ffffffffffffffffffffffff,
        0x05ca064cffff0847ffffffffffffffffffffffffffffffffffffffffffffffff,
        0x06e805d7ffffffffffffffffffffffffffffffffffffffffffffffffffffffff,
        0x042a0270ffffffffffffffffffffffffffffffffffffffffffffffffffffffff,
    ),
    (
        0xffffffffffffffff0367ffffffffffffffffffffffffffffffffffffffffffff,
        0xffffffffffffffffffffffffffffffffffffffffffffffff05feffffffffffff,
        0xffff07ecffffffffffffffffffffffffffffffffffffffffffffffffffffffff,
        0xffffffffffff0820ffffffffffffffffffffffffffffffffffffffffffffffff,
        0xffffffffffffffffffffffffffffffffffffffffffffffffffffffffffffffff,
        0x041dffffffffffffffffffffffffffffffffffffffffffffffffffffffffffff,
    ),
)

FIRST_LAG, LATER_LAG, FIRST_STEPS = 2, 3, 4
GAIN_STEP = 2
SLOTS = 33
UNITS = 65
UNIT = 16
STARTS = (0, 13, 26, 39, 52)
OPPOSITE = (1, 0, 3, 2, 5, 4)
NOTHING = 0xFFFF


def lag(step):
    return FIRST_LAG if step < FIRST_STEPS else LATER_LAG


SIZES = dict(zip(STARTS, (b - a for a, b in zip(STARTS, STARTS[1:] + (UNITS,)))))


def size_of(entry):
    return 0 if entry == NOTHING else SIZES[entry % UNITS]


def neighbour_position(p, d):
    x, y = divmod(p, 4)
    if d == 0:
        x = (x + 1) % 4
    if d == 1:
        x = (x + 3) % 4
    if d == 2:
        y = (y + 1) % 4
    if d == 3:
        y = (y + 3) % 4
    return 4 * x + y


def signed(word):
    return word - (1 << 32) if word >= 1 << 31 else word


def entries(step, d):
    return [(PLAN[step][d] >> (16 * p)) & 0xFFFF for p in range(16)]


def mask_of(flags):
    return sum(1 << p for p, flag in enumerate(flags) if flag)


def gather_kernel(re_ref, im_ref, held, part, part_in, send_sem, recv_sem, load_sem, pair_sem):
    bins = re_ref.shape[0]
    tiles = re_ref.shape[1]
    fr = lax.axis_index("fr")
    sr = lax.axis_index("sr")
    sc = lax.axis_index("sc")
    z, x, y = sr // 4, sr % 4, sc
    p = 4 * x + y
    steps = len(PLAN)

    loads = []
    for f in range(bins):
        for i, ref in enumerate((re_ref, im_ref)):
            unit = (2 * f + i) * tiles
            loads.append(
                pltpu.make_async_copy(ref.at[f], held.at[pl.ds(unit, tiles)], load_sem.at[2 * f + i])
            )
    for load in loads:
        load.start()

    xp, xm = (x + 1) % 4, (x + 3) % 4
    yp, ym = (y + 1) % 4, (y + 3) % 4
    zp, zm = (z + 1) % 4, (z + 3) % 4
    targets = (
        (fr, 4 * z + xp, y),
        (fr, 4 * z + xm, y),
        (fr, sr, yp),
        (fr, sr, ym),
        (fr, 4 * zp + x, y),
        (fr, 4 * zm + x, y),
    )
    ahead = (4 * (xp - x), 4 * (xm - x), yp - y, ym - y, 16, -16)
    twin = (1 - fr, sr, sc)
    shift = 16 * (y % 2)

    barrier = pltpu.get_barrier_semaphore()
    for device in targets + (twin,):
        pl.semaphore_signal(barrier, inc=1, device_id=device, device_id_type=MESH)
    for load in loads:
        load.wait()
    pl.semaphore_wait(barrier, 7)

    def chosen(step, d):
        words = [jnp.int32(signed((PLAN[step][d] >> (32 * i)) & 0xFFFFFFFF)) for i in range(8)]
        words = [jnp.where(y < 2, words[i], words[i + 1]) for i in range(0, 8, 2)]
        word = jnp.where(
            x < 2,
            jnp.where(x == 0, words[0], words[1]),
            jnp.where(x == 2, words[2], words[3]),
        )
        return lax.shift_right_logical(word, shift) & 0xFFFF

    def guarded(mask, action):
        if mask == 0:
            return
        if mask == 0xFFFF:
            action()
            return
        pl.when((lax.shift_right_logical(jnp.int32(mask), p) & 1) == 1)(action)

    def transfer(step, d, source, target, size):
        return pltpu.make_async_remote_copy(
            src_ref=held.at[pl.ds(source, size)],
            dst_ref=held.at[pl.ds(target, size)],
            send_sem=send_sem.at[d, step],
            recv_sem=recv_sem.at[d, step],
            device_id=targets[d],
            device_id_type=MESH,
        )

    def for_each_size(sizes, action):
        for size in sorted(set(sizes) - {0}):
            guarded(mask_of(v == size for v in sizes), functools.partial(action, size))

    def send(step, d):
        def action(size):
            source = chosen(step, d)
            transfer(step, d, source, source - UNITS * ahead[d], size).start()

        for_each_size([size_of(v) for v in entries(step, d)], action)

    def receive(step, d):
        sent = [size_of(v) for v in entries(step, d)]
        coming = [sent[neighbour_position(q, OPPOSITE[d])] for q in range(16)]
        for_each_size(coming, lambda size: transfer(step, d, 0, UNITS, size).wait_recv())

    def finish(step, d):
        sent = [size_of(v) for v in entries(step, d)]
        for_each_size(sent, lambda size: transfer(step, d, 0, UNITS, size).wait_send())

    exchange = pltpu.make_async_remote_copy(
        src_ref=part,
        dst_ref=part_in,
        send_sem=pair_sem.at[0],
        recv_sem=pair_sem.at[1],
        device_id=twin,
        device_id_type=MESH,
    )

    for step in range(steps + LATER_LAG):
        for earlier in range(steps):
            if earlier + lag(earlier) == step:
                for d in range(6):
                    receive(earlier, d)
        if step < steps:
            for d in range(6):
                send(step, d)
        if step == 0:
            total = jnp.zeros((tiles, UNIT, 256), jnp.float32)
            for i in range(2 * bins):
                piece = held[pl.ds(i * tiles, tiles)].astype(jnp.float32)
                total += piece * piece
            total = total.reshape(tiles * UNIT, 256)
            half = total[:, :128] + total[:, 128:]
            power = jnp.sum(half.T, axis=0, keepdims=True)
            part[...] = jnp.broadcast_to(power, part.shape)
            exchange.start()
        if step == GAIN_STEP:
            exchange.wait()
            power = part[...] + part_in[...]
            gain = 1.0 / jnp.sqrt(power * (1.0 / 2048.0))
            gain = jnp.concatenate([gain, gain], axis=0)
            gain = jnp.concatenate([gain, gain], axis=1)
            high = gain.astype(jnp.bfloat16).astype(jnp.float32)
            middle = (gain - high).astype(jnp.bfloat16).astype(jnp.float32)
            low = gain - high - middle
            row = lax.broadcasted_iota(jnp.int32, (UNIT, 256), 0)
            rest = jnp.where(row == 1, middle, low)
            held[UNITS - 1] = jnp.where(row == 0, high, rest).astype(jnp.bfloat16)
    for step in range(steps):
        for d in range(6):
            finish(step, d)


def gathered(re, im):
    bins, tiles = re.shape[:2]
    steps = len(PLAN)
    return pl.pallas_call(
        gather_kernel,
        out_shape=jax.ShapeDtypeStruct((SLOTS * UNITS, UNIT, 256), jnp.bfloat16),
        in_specs=[pl.BlockSpec(memory_space=pltpu.HBM)] * 2,
        out_specs=pl.BlockSpec(memory_space=pltpu.VMEM),
        scratch_shapes=[
            pltpu.VMEM((8, 128), jnp.float32),
            pltpu.VMEM((8, 128), jnp.float32),
            pltpu.SemaphoreType.DMA((6, steps)),
            pltpu.SemaphoreType.DMA((6, steps)),
            pltpu.SemaphoreType.DMA((2 * bins,)),
            pltpu.SemaphoreType.DMA((2,)),
        ],
        compiler_params=pltpu.CompilerParams(
            collective_id=0, has_side_effects=True, vmem_limit_bytes=24 << 20
        ),
        name="gather_blocks",
    )(re, im)


GROUP = 11
RING = 3


def gain_row(tile):
    wide = tile.astype(jnp.float32)
    return wide[0:1, :128] + wide[1:2, :128] + wide[2:3, :128]


def cross_kernel(order, held, out, staged, own_column, sems):
    bins = out.shape[0]
    own_row = gain_row(held[UNITS - 1]) * (1.0 / 16.0)
    own_column[...] = jnp.broadcast_to(own_row, (128, 128)).T

    def store(buffer, slot):
        return pltpu.make_async_copy(staged.at[buffer], out.at[:, slot], sems.at[buffer])

    def group(i, carry):
        for j in range(GROUP):
            buffer = (i % RING) * GROUP + j

            @pl.when(i >= RING)
            def _():
                store(buffer, 0).wait()

        for j in range(GROUP):
            buffer = (i % RING) * GROUP + j
            first = order[i * GROUP + j] * UNITS
            weight = own_column[...] * gain_row(held[first + UNITS - 1])
            for f in range(bins):
                mine = held[pl.ds(16 * f, 16)].reshape(256, 256)
                other = held[pl.ds(first + 16 * f, 16)].reshape(256, 256)
                full = lax.dot_general(
                    mine, other, (((1,), (1,)), ((), ())), preferred_element_type=jnp.float32
                )
                staged[buffer, f, :, :128] = (full[:128, :128] + full[128:, 128:]) * weight
                staged[buffer, f, :, 128:] = (full[128:, :128] - full[:128, 128:]) * weight
            store(buffer, i * GROUP + j).start()
        return carry

    groups = SLOTS // GROUP
    lax.fori_loop(0, groups, group, 0)
    for i in range(groups - RING, groups):
        for j in range(GROUP):
            store((i % RING) * GROUP + j, 0).wait()


def local(spec_re, spec_im, offsets):
    bins, rows, segs = spec_re.shape
    tiles = rows // UNIT
    re = spec_re.reshape(bins, tiles, UNIT, segs)
    im = spec_im.reshape(bins, tiles, UNIT, segs)
    re = pltpu.with_memory_space_constraint(re, pltpu.HBM)
    im = pltpu.with_memory_space_constraint(im, pltpu.HBM)
    held = gathered(re, im)
    cross = pl.pallas_call(
        cross_kernel,
        in_specs=[pl.BlockSpec(memory_space=pltpu.SMEM), pl.BlockSpec(memory_space=pltpu.VMEM)],
        out_specs=pl.BlockSpec(memory_space=pltpu.HBM),
        out_shape=jax.ShapeDtypeStruct((bins, SLOTS, rows, 256), jnp.float32),
        scratch_shapes=[
            pltpu.VMEM((RING * GROUP, bins, rows, 256), jnp.float32),
            pltpu.VMEM((rows, rows), jnp.float32),
            pltpu.SemaphoreType.DMA((RING * GROUP,)),
        ],
        compiler_params=pltpu.CompilerParams(vmem_limit_bytes=30 << 20),
        name="cross_products",
    )(offsets[0], held)
    return cross[:, None]


def solution(mesh):
    placed = (P("fr", ("sr", "sc"), None), P("fr", ("sr", "sc"), None), P(("sr", "sc"), None))
    return jax.shard_map(
        local,
        mesh=mesh,
        in_specs=placed,
        out_specs=P("fr", ("sr", "sc"), None, None, None),
        check_vma=False,
    )
```

```python
import functools
import math

import jax
import jax.numpy as jnp
from jax import lax
from jax.experimental import pallas as pl
from jax.experimental.pallas import tpu as pltpu
from jax.sharding import PartitionSpec as P

MESH = pl.DeviceIdType.MESH

PLAN = (
    (
        0x0020004000200000ffffffffffffffffffffffffffffffffffffffffffffffff,
        0x000000400020000000000040000000400040000000400040ffffffffffffffff,
        0x0040ffffffffffff0000ffffffffffff0020ffffffffffff0040ffffffffffff,
        0x004000400000ffff000000200040ffff002000200040ffff000000200040ffff,
        0xffffffffffffffffffffffffffffffffffffffffffffffffffffffffffffffff,
        0x0000002000000020004000200040002000200040002000200020004000200040,
    ),
    (
        0x0000000000400040ffffffffffffffffffffffffffffffffffffffffffffffff,
        0x002000000040004000200000002000000000004000000000ffffffffffffffff,
        0x0020ffffffffffff0020ffffffffffff0000ffffffffffff0000ffffffffffff,
        0x002000000040ffff002000000020ffff000000400000ffff004000000000ffff,
        0xffffffffffffffffffffffffffffffffffffffffffffffffffffffffffffffff,
        0x0020000000400040002000000020000000000000000000000040000000000000,
    ),
    (
        0x0060083008100830085008300850083008300850083008300830085008300850,
        0x0060083008100830085008300850083008300060083008300830085008300850,
        0x08100830081001c3085002440224020400600244020402440830020402440244,
        0x0810083000600830085000600060020400600060083002440830085008300244,
        0xffffffffffffffffffffffffffffffffffffffffffffffffffffffffffffffff,
        0x0810083008100830085008300850083008300850083008300830085008300850,
    ),
    (
        0x0040006000600060083008100830081008100810081008100850064c062c0810,
        0x0040006000600060006000600060006000600020006000600850081008100810,
        0x0060081008500850006002040244018300400204022402040060064c062c01c3,
        0x0060006000200850006000400000024400400810006002040060006000600204,
        0xffffffffffffffffffffffffffffffffffffffffffffffffffffffffffffffff,
        0x0830081008500850083008100830081008100810081008100850081008100810,
    ),
    (
        0x06ad089108b1099310601040106010401040106010401040060c0e3c0e1c0e3c,
        0x07af089108b109930224081000a109d30a540a340a5408b11040106010401060,
        0x07af062c102010400204104010600a3408100a340a5410400a34106010400e3c,
        0x0830089100c11040020408d10a1410400a540a340a540a340a3408b108d10a34,
        0xffff089108b10993ffff0a340a1409d30a540a340a540a340a340e3c0a340a34,
        0x004000c10060000000600040022400400040002000a100600000002000400060,
    ),
    (
        0x07af078f085008501040064c062c1020062c064c062c10201040106010201060,
        0x06ad078f08500850083000a1083008100810085008100a340a34102008d108b1,
        0x078f10400224024408301020104010400830106010400a34085010200a341060,
        0x022408100850024408300810083010200830085008101040085002040e1c1060,
        0xffffffffffffffffffff08d1ffff0a34ffffffff089108b1ffff08b108d108b1,
        0x00600040002000e1000000600060006002040060006000c1066c0264062c0020,
    ),
    (
        0x078f07cf07cf060c0ebd0fdf10400e3c102010201020060c1060102010401020,
        0x0830081007cf0a5400810081018300e101c30810089102640fdf0fbf10201020,
        0x08300f9f0fbf10600e3c02640e3c102001c31020102010200264022410201020,
        0x0e5c0e3c0e5c10600e3c0e5c0a34026400c100e10891102000c100e100a11020,
        0xffffffff0912093209b30fdf09b30a9508b109d30c180c3808b10c380e1c09b3,
        0x0850006008700810087008500000085008500830020408700810083008500870,
    ),
    (
        0x062c08d100e100e1060c060c060c0850085008300fbf09930fdf08300ebd0f9f,
        0x0a3408b10204093200c10a9509520a9508b101a30ab509930810083009320870,
        0x0e5c0204062c0e3c01c30fdf02640b9709b301830fbf09930c580fbf08500a34,
        0x062c08b1062c08100244060c0e3c0e3c04280a1408b10c380c580ab50c580870,
        0xffffffff0fbf09120fbf09930952ffff09b30ad50fbf0ad50c580ab50dbb0e3c,
        0x0870085008300060081008700870087000600870087000400060006000e10830,
    ),
    (
        0x06cd08b1089109320f9f087008910e1c0fdf0870087008700f9f0fbf08500870,
        0x00c10204089108f101830993026409b30a1409d3026408d108b10a7408500830,
        0x0a34085004280e1c0428099309b30e1c0e3c0fbf0e1c08700e7c08300fdf0870,
        0x02440a1400e10e1c0ebd08b10a54060c08b1024408d10e5c02640a740e3c0ab5,
        0x09d30f3e0ebd0edd0f9f0fbf0fbf0c580ebd0fbf0e1c0bd70f9f09b30fdf0bb7,
        0x0244087000c100a1026402640810026400c10183004001c3026400810060060c,
    ),
    (
        0x05ab00e1062c01c31080106008700fbf0e5c0f9f08b108d10e7c08d10ddb0830,
        0x09d309b300e1091200e102640a5402640264024408b100e10e9d0f9f0f9f0952,
        0x09d309b30fdf0c3802440fbf09d310600183087008700e1c03c70f9f0a140830,
        0x0cb90edd0ebd0edd0e9d02440e1c10600e5c0e1c0e3c02640a1402240a14066c,
        0x0cb90ddb0dbb0c380e9d0ebd0ab50ab50fdf0f9f0f9f09120fdf0ddb0ddb0f9f,
        0x00c1044800e101e3024401a300c100e1028500c1038700e103c7022401c300e1,
    ),
    (
        0x068d0850087008f110200ebd0edd10800f9f1080108008500e9d087008f11040,
        0x02040224093201a309b3087000e101e300c102850a140932087007cf08f11080,
        0x0e3c044810400264064c1080108010800a14104002641080087008700ddb1080,
        0x020402240a1402640c380ebd08100ab50264062c00e108d106ed0edd08f11040,
        0x0f1e0edd09320fdf08b10ab50edd0b360f9f0e1c09b309320e9d0f9f0f9f0952,
        0x020402240142087001e301e3010201e30870062c0850085008700870087000c1,
    ),
    (
        0x0850066c068d064c048910800d9b0ebd10600d9b0850066c10200ddb08701080,
        0x07cf02c508d1022401e30a14093200810850099307ef09d30a740f5e10600b97,
        0x0a541080108010200a740dbb10200a740e5c0f9f07ef09d30c180bd70870066c,
        0x0c99066c0a950c180e1c066c0891066c0e9d0e5c0a1410800a7408910e5c0ad5,
        0x0d9b0e5c0a950c1809120dbb0d9b0ad50d9b0d9b0a950bb70c180f5e09b30ad5,
        0x01830468068d02240081024400e1066c02640142016201e300c1014202640264,
    ),
    (
        0x00c1087008f1016208700d9b0fdf0870087008d1064c0ebd0870089109d308f1,
        0x089100e1087001e3078f02c50870087000e107ef01c302e507af0870087008f1,
        0x0e7c0e5c066c081008100d9b066c066c07ef0264064c062c0244099307af1040,
        0x068d06ad0244087000e100e108d1087000e104a9060c062c04e900810af50830,
        0x0891099309930f3e0f3e0f1e09320e9d0c780c990e9d09520f1e0a950af50fff,
        0x040805ab066c016200e10081018306cd00e10468064c02e504e907cf01620468,
    ),
    (
        0x083001a3093209b30fff09f30e7c066c074e066c0fff106007ef076e0fff0972,
        0x026408d102a50a74093209f30a950b160102026402e501620ebd108009d30ad5,
        0x02640a34040810800a54062c0fff08700c78062c1080106007af104010800264,
        0x02640a3402e50e7c04890e7c0e7c0ad5074e0e3c06ad10600870060c0c1808d1,
        0x0e1c0d3a0d9b0a950d9b0fff0a950b160fbf0dbb09120fbf0c380d5a0c180972,
        0x0264028502e501c30408062c06ad07cf07ef066c018303e707ef06ed00a1066c,
    ),
    (
        0x058b05ab06ed01420e5c0f9f0fff0e7c10800952066c0e3c08d107ef10800ebd,
        0x099301c301c30a95040807af09f308b108d1076e095209f30a540b9710800bd7,
        0x0204064c09930224040810600fdf04280e1c0bd70972066c078f0c78066c0d9b,
        0x0e7c0e5c0a54064c04e90e9d08f1064c0e1c0edd046808f10ebd0af50a7408f1,
        0x0c990fbf0cd90dbb0fff0e9d0f9f0af50efd0f1e09520c990c990b970c990b97,
        0x046801c30326058b048904c9068d0346074e076e01c3046806ed076e05eb054a,
    ),
    (
        0x066c064c00c100a10d3a0fff064c064c064c068d0edd08f110800d5a097207cf,
        0x00e102a5099302c501c3070e01620af507ef02e5085001420f1e095209720b76,
        0x0e1c0fff0b9701e30d9b0b9709930edd066c01a30d9b0a740c380e7c04680c58,
        0x066c04080cd902e50e5c044806cd0edd0a7404c90e5c0af5068d06ed064c04e9,
        0x09320d1a0b970fff0d1a093209d30ebd0cd90bd70b360ebd09120bd70f5e0c18,
        0x00e1040801c302e506ed0408016200c10081016202e506ed02e5048904680244,
    ),
    (
        0x070e070e078f097205ab05eb091208910fff0e3c097209720fbf08f105eb0fbf,
        0x08b10a54018302e50a340ab50ad502040b360a14078f03060fff0af50c180b36,
        0x09b305eb0bb7064c01e305eb0e7c062c03870e7c0fdf0264062c09f301e3060c,
        0x0c180a95066c0366008104080efd0efd0468044802e50e7c08b102e50c380efd,
        0x08b10cb90c780bb70a95095209f30fbf0b360f3e0c580fdf0ab50ebd09320a95,
        0x078f02c506ed06ad046802e502e503a702c507cf052a076e074e05ab01420204,
    ),
    (
        0x03c7008100a10122058b0e3c0efd09720efd07cf0dfb03460bd70f3e0efd0952,
        0x081009520af5072e09d308910b160b5601e302a5018301220bf70f3e0b760bf7,
        0x0a7409d30ddb0bd70e7c0f9f03a70e5c0204064c0bf70f9f042805ab05ab054a,
        0x04480cb90edd02c504c90cd90ebd0c780e3c0489064c06ed02440489068d06ed,
        0x0d5a09520dfb0cb90fdf0f7e0b160cb90b560b970edd0b3609520d9b0cb90912,
        0x04c902e501e305cb02c503c703c7058b010205eb05ab0346076e056a008107cf,
    ),
    (
        0x012206ad010200810d5a0edd0dfb0efd05eb0e7c07cf076e070e0efd076e0e5c,
        0x01a309120a740b56072e012208d10ad50183097201a30102095209720ab50e9d,
        0x0d9b0b970448058b046801e30a540fdf0bb701c304680428044803a70dbb0387,
        0x06ed0efd0a340c780e7c06cd04a908f104c9068d0e9d0efd0e9d04e904e906cd,
        0x0b3609120f5e0fbf0b160b970f1e0c9909720b560bd70dfb09320edd0b560c38,
        0x06ed07cf03c7044801830162042804c902e504c9076e07ef018304e9076e074e,
    ),
    (
        0x07cf052a072e07ef0d7a0f7e0e5c0f1e07cf0f3e0ebd0efd0f5e0dbb0b3606ad,
        0x02a5058b09520b1609f309320912036601a3016208d10af509120fff0fbf09d3,
        0x0c780d9b0c7809f30c58066c04680bf7058b0dbb0b970dfb0b97062c02040c78,
        0x08f10c1808d1068d0c780cb9099308910972087004c9081004890c580cb90264,
        0x0f7e0b360edd0f9f0d3a0bb70f3e09720ab50d1a0f5e0ab50b560c180b360cd9,
        0x03a704e9060c068d04c9048903a7078f076e056a03660366030603e706cd0183,
    ),
    (
        0x0285050a05ab09120dfb0dbb0ebd0e9d0346056a06ed07cf064c08b106ad0fdf,
        0x01420b1603260bf702e5054a028508500081070e00c103870f7e0efd0b560932,
        0x0a140fbf0f9f0fbf0c38074e0dfb08500ddb05ab01a307af0468060c0bd705ab,
        0x0e1c0b970af50ebd0af5048904c904e9038700a10cf906cd00810cd902240346,
        0x091209320d3a0b1609320f3e0bf70f3e0c9909120b560d9b0cd909f30c380c58,
        0x056a060c0366052a05ab05cb00a10366040802a50428072e060c060c03870346,
    ),
    (
        0x048903c70122076e056a076e0f1e068d058b0d3a0f7e03060d7a0e5c0e7c064c,
        0x054a02e5036605eb09120224010203a706ed01420d1a09120d3a0c9909120d5a,
        0x0cd90fdf050a07ef0a950bb705ab0c99034609d30f7e0e5c0326052a01a30204,
        0x01620cd904890c58050a04c9068d04a908100ebd070e04e90a540cf904a9076e,
        0x0af50d5a0bf70d5a0ab50b160b3609320bb70d3a0cf90d3a09720cd90c580c99,
        0x07cf076e056a076e0162054a076e074e050a024406ed068d032605eb03060081,
    ),
    (
        0x056affffffffffff05eb095205ab0f7e0d7a0af50f1e070e0e5c0f5e07cf0d1a,
        0x09f3014201420b36050a01a309b30a140b56010201e3ffff08d1076e0af50d1a,
        0x0b560b360bf70f9fffff0bd70c780cd9ffff0c180e5c060cffff0a3403a705cb,
        0x03a7076e0e7c08d1066c0c180cf90a5402850cd9ffff0489ffffffffffff068d,
        0x0fff0b160b560cf90ebdffff0b76ffff0f3e0b76ffffffff09f3ffffffffffff,
        0x03c7034602c5ffff03a7ffffffffffff01e3ffffffffffffffffffffffffffff,
    ),
    (
        0xffffffffffffffff0fbf0cb90e3cffff05cbffffffffffff0ebdffffffffffff,
        0x0d7affffffffffffffffffffffffffffffffffffffffffff0af5ffffffffffff,
        0xffff0f1e0c58ffffffffffffffffffffffffffffffffffffffffffffffffffff,
        0x0e3cffffffff0dbbffffffffffffffffffffffffffffffffffffffffffffffff,
        0x0d3affffffffffffffffffffffffffffffffffffffffffffffffffffffffffff,
        0x0387ffffffffffffffffffffffffffffffffffffffffffffffffffffffffffff,
    ),
)
SEMAPHORES = (
    (0, 6, 12, 18, 24, 30),
    (1, 7, 13, 19, 24, 31),
    (2, 8, 14, 20, 24, 32),
    (3, 9, 15, 21, 24, 33),
    (4, 10, 16, 22, 24, 34),
    (5, 11, 17, 23, 25, 35),
    (0, 6, 12, 18, 26, 36),
    (1, 7, 13, 19, 27, 37),
    (2, 8, 14, 20, 28, 38),
    (3, 9, 15, 21, 29, 39),
    (4, 10, 16, 22, 24, 30),
    (5, 11, 17, 23, 25, 31),
    (0, 6, 12, 18, 26, 32),
    (1, 7, 13, 19, 27, 33),
    (2, 8, 14, 20, 28, 34),
    (3, 9, 15, 21, 29, 35),
    (4, 10, 16, 22, 24, 36),
    (5, 11, 17, 23, 25, 37),
    (0, 6, 12, 18, 26, 38),
    (1, 7, 13, 19, 27, 39),
    (2, 8, 14, 20, 28, 30),
    (3, 9, 15, 21, 29, 31),
    (4, 10, 16, 22, 24, 32),
    (5, 11, 17, 23, 25, 33),
)
NEEDS = (
    (
        0xffffffffffffffffffffffffffffffff,
        0xffffffffffffffffffffffffffffffff,
        0xffffffffffffffffffffffffffffffff,
        0xffffffffffffffffffffffffffffffff,
        0xffffffffffffffffffffffffffffffff,
        0xffffffffffffffffffffffffffffffff,
    ),
    (
        0xffffffffffffffffffffffffffffffff,
        0xffffffffffffffffffffffffffffffff,
        0xffffffffffffffffffffffffffffffff,
        0xffffffffffffffffffffffffffffffff,
        0xffffffffffffffffffffffffffffffff,
        0xffffffffffffffffffffffffffffffff,
    ),
    (
        0xffffffffffffffffffffffffffffffff,
        0xffffffffffffffffffffffffffffffff,
        0xffffff0cff0606ffff0606ffff0606ff,
        0xffffffffffffff06ffffff06ffffff06,
        0xffffffffffffffffffffffffffffffff,
        0x1e1e1e1e1e1e1e1e1e1e1e1e1e1e1e1e,
    ),
    (
        0xffffffffffffffffffffffffffffffff,
        0xffffffffffffffffffffffffffffffff,
        0xffffffffff0707ffff0707ffffffffff,
        0xffffffffffffff07ffffff07ffffff07,
        0xffffffffffffffffffffffffffffffff,
        0x1f1f1f1f1f1f1f1f1f1f1f1f1f1f1f1f,
    ),
    (
        0x14ffffff20ffffff202020ffff0202ff,
        0x0eff140effffff0effffff1420202020,
        0xff0220ffff202008ffffff20ffffff02,
        0xff14ff20ff1408200808080808141408,
        0xffffffffff08ffffffffffffffff08ff,
        0xffffffffffffffffffffffffffffffff,
    ),
    (
        0xffffffff21ffffffffffff21ffff21ff,
        0xffffffffffffffffffffffffff21ffff,
        0x0fffffffff2121ffffffffffffffffff,
        0xffffffffffffff21ffffffffffffffff,
        0xffffffffffffffffffff15ffffffffff,
        0xffffffffffffffffffffffffffffffff,
    ),
    (
        0xffffffff1610ff04ffffffffffffffff,
        0xffffff0affffffffffffffff1010ffff,
        0xff1010ffffff04ffffffffffffffffff,
        0x040404ff040422ffffffffffffffffff,
        0xffff16100aff101616100404160affff,
        0x22ff22222222ff222222ff2222222222,
    ),
    (
        0xffffffffffffffffffffffffffffffff,
        0xffffffffffffffffffffffffffffffff,
        0xffffffffffffffffffffffffffffffff,
        0xffffffffffffffffffffffffffffffff,
        0xffffff11ff0bffffffffffffffffffff,
        0x232323ff23232323ff2323ffffffff23,
    ),
    (
        0xffffffffffffffffffffffffffffffff,
        0xffffffffffffffffffffffffffffffff,
        0xffffffffffffffffffffffffffffffff,
        0xffffffffffffffffffffffffffffffff,
        0x060c1212ffffff06ffffffffffffffff,
        0xff24ffffffff24ffffffffffffffffff,
    ),
    (
        0xffffffffffffffffffffffffffffffff,
        0xffffffffffffffffffffffffffffffff,
        0xffffffffffffffffffffffffffffffff,
        0xffffffffffffffffffffffffffffffff,
        0xffff0dffffffffffffffffffffffffff,
        0xffffffffffffffffffffffffffffffff,
    ),
    (
        0xffffffffffffffffffffffffffffffff,
        0xffffffffffffffffffffffffffffffff,
        0xffffffffffffffffffffffffffffffff,
        0xffffffffffffffffffffffffffffffff,
        0xffffffffffffffffffffffffffffffff,
        0xffffffffffffffffffff26ffffff26ff,
    ),
    (
        0xffffffffffffffffffffffffffffffff,
        0xffffffffffffffffffffffffffffffff,
        0xffffffffffffffffffffffffffffffff,
        0xffffffffffffffffffffffffffffffff,
        0xff03ffffffffffffffffffffffffffff,
        0xffffffffffffffffffffffffffffffff,
    ),
    (
        0xffffffffffffffffffffffffffffffff,
        0xffffffffffffffffffffffffffffffff,
        0xffffffffffffffffffffffffffffffff,
        0xffffffffffffffffffffffffffffffff,
        0xffffffffffffffffffffffffffffffff,
        0xffffffffffffffffffffffffffffffff,
    ),
    (
        0xffffffffffffffffffffffffffffffff,
        0xffffffffffffffffffffffffffffffff,
        0xffffffffffffffffffffffffffffffff,
        0xffffffffffffffffffffffffffffffff,
        0xffffffffffffffffffffffffffffffff,
        0xffffffffffffffffffffffffffffffff,
    ),
    (
        0xffffffffffffffffffffffffffffffff,
        0xffffffffffffffffffffffffffffffff,
        0xffffffffffffffffffffffffffffffff,
        0xffffffffffffffffffffffffffffffff,
        0xffffffffffffffffffffffffffffffff,
        0xffffffffffffffffffffffffffffffff,
    ),
    (
        0xffffffffffffffffffffffffffffffff,
        0xffffffffffffffffffffffffffffffff,
        0xffffffffffffffffffffffffffffffff,
        0xffffffffffffffffffffffffffffffff,
        0xffffffffffffffffffffffffffffffff,
        0xffffffffffffffffffffffffffffffff,
    ),
    (
        0xffffffffffffffffffffffffffffffff,
        0xffffffffffffffffffffffffffffffff,
        0xffffffffffffffffffffffffffffffff,
        0xffffffffffffffffffffffffffffffff,
        0xffffffffffffffffffffffffffffffff,
        0xffffffffffffffffffffffffffffffff,
    ),
    (
        0xffffffffffffffffffffffffffffffff,
        0xffffffffffffffffffffffffffffffff,
        0xffffffffffffffffffffffffffffffff,
        0xffffffffffffffffffffffffffffffff,
        0xffffffffffffffffffffffffffffffff,
        0xffffffffffffffffffffffffffffffff,
    ),
    (
        0xffffffffffffffffffffffffffffffff,
        0xffffffffffffffffffffffffffffffff,
        0xffffffffffffffffffffffffffffffff,
        0xffffffffffffffffffffffffffffffff,
        0xffffffffffffffffffffffffffffffff,
        0xffffffffffffffffffffffffffffffff,
    ),
    (
        0xffffffffffffffffffffffffffffffff,
        0xffffffffffffffffffffffffffffffff,
        0xffffffffffffffffffffffffffffffff,
        0xffffffffffffffffffffffffffffffff,
        0xffffffffffffffffffffffffffffffff,
        0xffffffffffffffffffffffffffffffff,
    ),
    (
        0xffffffffffffffffffffffffffffffff,
        0xffffffffffffffffffffffffffffffff,
        0xffffffffffffffffffffffffffffffff,
        0xffffffffffffffffffffffffffffffff,
        0xffffffffffffffffffffffffffffffff,
        0xffffffffffffffffffffffffffffffff,
    ),
    (
        0xffffffffffffffffffffffffffffffff,
        0xffffffffffffffffffffffffffffffff,
        0xffffffffffffffffffffffffffffffff,
        0xffffffffffffffffffffffffffffffff,
        0xffffffffffffffffffffffffffffffff,
        0xffffffffffffffffffffffffffffffff,
    ),
    (
        0xffffffffffffffffffffffffffffffff,
        0xffffffffffffffffff1cffffffffffff,
        0xffffffffffffffffffffffffffffffff,
        0xffffffffffffffffffffffffffffffff,
        0xffffffffffffffffffffffffffffffff,
        0xffffffffffffffffffffffffffffffff,
    ),
    (
        0xffffffffffffffffffffffffffffffff,
        0xffffffffffffffffffffffffffffffff,
        0xffffffffffffffffffffffffffffffff,
        0xffffffffffffffffffffffffffffffff,
        0xffffffffffffffffffffffffffffffff,
        0xffffffffffffffffffffffffffffffff,
    ),
)
LATE = (
    (0x000f, 0x0888, 0x0111, 0x7777, 0x0000, 0x0000),
    (0x000f, 0x088e, 0x1111, 0x7777, 0x0000, 0x0000),
    (0xbff8, 0xf804, 0x6eff, 0x1be9, 0x0000, 0xc000),
    (0xffff, 0xffff, 0x7fff, 0xffdf, 0x0000, 0xf0e9),
    (0x10cf, 0xe7fb, 0x89b3, 0xd677, 0x77ff, 0x4020),
    (0xffff, 0xfbff, 0xefff, 0xffff, 0x0537, 0x109e),
    (0xffff, 0x7eff, 0xbfff, 0xcfff, 0x3fff, 0xbdff),
    (0xffff, 0xffff, 0xdfff, 0xffff, 0x3eff, 0xffff),
    (0xffff, 0xffff, 0xffff, 0xffff, 0xffff, 0xffdd),
    (0xbfff, 0xffff, 0xffff, 0xffff, 0xffff, 0xffff),
    (0xffff, 0xffff, 0xffff, 0xffff, 0xffff, 0xffff),
    (0xffff, 0xffff, 0xffff, 0xffff, 0xffff, 0xffff),
    (0xffff, 0xffff, 0xffff, 0xffff, 0xffff, 0xffff),
    (0xffff, 0xffff, 0xffff, 0xffff, 0xffff, 0xffff),
    (0xffff, 0xffff, 0xffff, 0xffff, 0xffff, 0xffff),
    (0xffff, 0xffff, 0xffff, 0xffff, 0xffff, 0xffff),
    (0xffff, 0xffff, 0xffff, 0xffff, 0xffff, 0xffff),
    (0xffff, 0xffff, 0xffff, 0xffff, 0xffff, 0xffff),
    (0xffff, 0xffff, 0xffff, 0xffff, 0xffff, 0xffff),
    (0xffff, 0xffff, 0xffff, 0xffff, 0xffff, 0xffff),
    (0xffff, 0xffff, 0xffff, 0xffff, 0xffbf, 0xffff),
    (0xffff, 0xffff, 0xffff, 0xffff, 0xffff, 0xffff),
    (0xfff8, 0xfffe, 0xfeee, 0xffe8, 0xfac8, 0xe880),
    (0xe880, 0x8800, 0xc000, 0xc000, 0x8000, 0x8000),
)
LATE_BY = 3
NO_WAIT = 0xFF
GAIN_STEP = 1
SLOTS = 33
UNITS = 129
UNIT = 16
LANES = 128
STARTS = (0, 32, 64, 96)
OPPOSITE = (1, 0, 3, 2, 5, 4)
ORDER = (5, 3, 1, 2, 0, 4)
SENDS = 3
NOTHING = 0xFFFF


SIZES = dict(zip(STARTS, (b - a for a, b in zip(STARTS, STARTS[1:] + (UNITS,)))))


def size_of(entry):
    return 0 if entry == NOTHING else SIZES[entry % UNITS]


def neighbour_position(p, d):
    x, y = divmod(p, 4)
    if d == 0:
        x = (x + 1) % 4
    if d == 1:
        x = (x + 3) % 4
    if d == 2:
        y = (y + 1) % 4
    if d == 3:
        y = (y + 3) % 4
    return 4 * x + y


def signed(word):
    return word - (1 << 32) if word >= 1 << 31 else word


def entries(step, d):
    return [(PLAN[step][d] >> (16 * p)) & 0xFFFF for p in range(16)]


def mask_of(flags):
    return sum(1 << p for p, flag in enumerate(flags) if flag)


def gather_kernel(re_ref, im_ref, held, part, part_in, send_sem, recv_sem, load_sem, pair_sem):
    bins = re_ref.shape[0]
    tiles = re_ref.shape[1]
    fr = lax.axis_index("fr")
    sr = lax.axis_index("sr")
    sc = lax.axis_index("sc")
    z, x, y = sr // 4, sr % 4, sc
    p = 4 * x + y
    steps = len(PLAN)

    loads = []
    for f in range(bins):
        for half in range(2):
            for i, ref in enumerate((re_ref, im_ref)):
                place = 4 * f + 2 * half + i
                source = ref.at[f, :, :, pl.ds(half * LANES, LANES)]
                target = held.at[pl.ds(place * tiles, tiles)]
                loads.append(pltpu.make_async_copy(source, target, load_sem.at[0]))
    for load in loads:
        load.start()

    xp, xm = (x + 1) % 4, (x + 3) % 4
    yp, ym = (y + 1) % 4, (y + 3) % 4
    zp, zm = (z + 1) % 4, (z + 3) % 4
    targets = (
        (fr, 4 * z + xp, y),
        (fr, 4 * z + xm, y),
        (fr, sr, yp),
        (fr, sr, ym),
        (fr, 4 * zp + x, y),
        (fr, 4 * zm + x, y),
    )
    ahead = (4 * (xp - x), 4 * (xm - x), yp - y, ym - y, 16, -16)
    twin = (1 - fr, sr, sc)
    shift = 16 * (y % 2)

    barrier = pltpu.get_barrier_semaphore()
    for device in targets + (twin,):
        pl.semaphore_signal(barrier, inc=1, device_id=device, device_id_type=MESH)
    everything = held.at[pl.ds(0, UNITS - 1)]
    pltpu.make_async_copy(everything, everything, load_sem.at[0]).wait()
    pl.semaphore_wait(barrier, 7)

    def chosen(step, d):
        words = [jnp.int32(signed((PLAN[step][d] >> (32 * i)) & 0xFFFFFFFF)) for i in range(8)]
        words = [jnp.where(y < 2, words[i], words[i + 1]) for i in range(0, 8, 2)]
        word = jnp.where(
            x < 2,
            jnp.where(x == 0, words[0], words[1]),
            jnp.where(x == 2, words[2], words[3]),
        )
        return lax.shift_right_logical(word, shift) & 0xFFFF

    def needed(step, d):
        words = [jnp.int32(signed((NEEDS[step][d] >> (32 * i)) & 0xFFFFFFFF)) for i in range(4)]
        word = jnp.where(
            x < 2,
            jnp.where(x == 0, words[0], words[1]),
            jnp.where(x == 2, words[2], words[3]),
        )
        return lax.shift_right_logical(word, 8 * y) & 0xFF

    def guarded(mask, action):
        if mask == 0:
            return
        if mask == 0xFFFF:
            action()
            return
        pl.when((lax.shift_right_logical(jnp.int32(mask), p) & 1) == 1)(action)

    def transfer(step, d, source, target, size, arrival):
        return pltpu.make_async_remote_copy(
            src_ref=held.at[pl.ds(source, size)],
            dst_ref=held.at[pl.ds(target, size)],
            send_sem=send_sem.at[SENDS * d + step % SENDS],
            recv_sem=recv_sem.at[arrival],
            device_id=targets[d],
            device_id_type=MESH,
        )

    def for_each_size(sizes, action, among=0xFFFF):
        for size in sorted(set(sizes) - {0}):
            guarded(mask_of(v == size for v in sizes) & among, functools.partial(action, size))

    def send(step, d):
        waits = mask_of((NEEDS[step][d] >> (8 * q)) & 255 != NO_WAIT for q in range(16))

        def arrived(size):
            transfer(step, d, 0, UNITS, size, needed(step, d)).wait_recv()

        def action(size):
            source = chosen(step, d)
            transfer(step, d, source, source - UNITS * ahead[d], size, SEMAPHORES[step][d]).start()

        sizes = [size_of(v) for v in entries(step, d)]
        for_each_size(sizes, arrived, waits)
        for_each_size(sizes, action)

    def receive(step, d):
        sent = [size_of(v) for v in entries(step, d)]
        coming = [sent[neighbour_position(q, OPPOSITE[d])] for q in range(16)]
        for_each_size(coming, lambda size: transfer(step, d, 0, UNITS, size, SEMAPHORES[step][d]).wait_recv(), LATE[step][d])

    def finish(step, d):
        sent = [size_of(v) for v in entries(step, d)]
        for_each_size(sent, lambda size: transfer(step, d, 0, UNITS, size, SEMAPHORES[step][d]).wait_send())

    exchange = pltpu.make_async_remote_copy(
        src_ref=part,
        dst_ref=part_in,
        send_sem=pair_sem.at[0],
        recv_sem=pair_sem.at[1],
        device_id=twin,
        device_id_type=MESH,
    )

    for step in range(steps):
        if step >= LATE_BY:
            for d in range(6):
                receive(step - LATE_BY, d)
        for d in ORDER:
            if step >= SENDS:
                finish(step - SENDS, d)
            send(step, d)
        if step == 0:
            total = jnp.zeros((tiles, UNIT, LANES), jnp.float32)
            for i in range(4 * bins):
                piece = held[pl.ds(i * tiles, tiles)].astype(jnp.float32)
                total += piece * piece
            total = total.reshape(tiles * UNIT, LANES)
            power = jnp.sum(total.T, axis=0, keepdims=True)
            part[...] = jnp.broadcast_to(power, part.shape)
            exchange.start()
        if step == GAIN_STEP:
            exchange.wait()
            power = part[...] + part_in[...]
            gain = 1.0 / jnp.sqrt(power * (1.0 / 2048.0))
            gain = jnp.concatenate([gain, gain], axis=0)
            high = gain.astype(jnp.bfloat16).astype(jnp.float32)
            middle = (gain - high).astype(jnp.bfloat16).astype(jnp.float32)
            low = gain - high - middle
            row = lax.broadcasted_iota(jnp.int32, (UNIT, LANES), 0)
            rest = jnp.where(row == 1, middle, low)
            held[UNITS - 1] = jnp.where(row == 0, high, rest).astype(jnp.bfloat16)
    for step in range(steps - LATE_BY, steps):
        for d in range(6):
            receive(step, d)
    for step in range(steps - SENDS, steps):
        for d in range(6):
            finish(step, d)


def gathered(re, im):
    bins, tiles = re.shape[:2]
    steps = len(PLAN)
    return pl.pallas_call(
        gather_kernel,
        out_shape=jax.ShapeDtypeStruct((SLOTS * UNITS, UNIT, LANES), jnp.bfloat16),
        in_specs=[pl.BlockSpec(memory_space=pltpu.HBM)] * 2,
        out_specs=pl.BlockSpec(memory_space=pltpu.VMEM),
        scratch_shapes=[
            pltpu.VMEM((8, 128), jnp.float32),
            pltpu.VMEM((8, 128), jnp.float32),
            pltpu.SemaphoreType.DMA((6 * SENDS,)),
            pltpu.SemaphoreType.DMA((max(map(max, SEMAPHORES)) + 1,)),
            pltpu.SemaphoreType.DMA((1,)),
            pltpu.SemaphoreType.DMA((2,)),
        ],
        compiler_params=pltpu.CompilerParams(
            collective_id=0, has_side_effects=True, vmem_limit_bytes=24 << 20
        ),
        name="gather_blocks",
    )(re, im)


GROUP = 11


def gain_row(tile):
    wide = tile.astype(jnp.float32)
    return wide[0:1] + wide[1:2] + wide[2:3]


def spectra(held, f, first):
    halves = [held[pl.ds(first + 32 * f + 16 * h, 16)].reshape(256, LANES) for h in range(2)]
    return jnp.concatenate(halves, axis=1)


def cross_kernel(order, held, out, staged, own_column, sem):
    bins = out.shape[0]
    own_row = gain_row(held[UNITS - 1]) * (1.0 / 16.0)
    own_column[...] = jnp.broadcast_to(own_row, (128, 128)).T

    def group(i, carry):
        for j in range(GROUP):
            place = i * GROUP + j
            first = order[place] * UNITS
            weight = own_column[...] * gain_row(held[first + UNITS - 1])
            for f in range(bins):
                mine, other = spectra(held, f, 0), spectra(held, f, first)
                full = lax.dot_general(
                    mine, other, (((1,), (1,)), ((), ())), preferred_element_type=jnp.float32
                )
                staged[place, f, :, :128] = (full[:128, :128] + full[128:, 128:]) * weight
                staged[place, f, :, 128:] = (full[128:, :128] - full[:128, 128:]) * weight
            pltpu.make_async_copy(staged.at[place], out.at[:, place], sem).start()
        return carry

    lax.fori_loop(0, SLOTS // GROUP, group, 0)
    pltpu.make_async_copy(staged, staged, sem).wait()


def local(spec_re, spec_im, offsets):
    bins, rows, segs = spec_re.shape
    tiles = rows // UNIT
    re = spec_re.reshape(bins, tiles, UNIT, segs)
    im = spec_im.reshape(bins, tiles, UNIT, segs)
    re = pltpu.with_memory_space_constraint(re, pltpu.HBM)
    im = pltpu.with_memory_space_constraint(im, pltpu.HBM)
    held = gathered(re, im)
    cross = pl.pallas_call(
        cross_kernel,
        in_specs=[pl.BlockSpec(memory_space=pltpu.SMEM), pl.BlockSpec(memory_space=pltpu.VMEM)],
        out_specs=pl.BlockSpec(memory_space=pltpu.HBM),
        out_shape=jax.ShapeDtypeStruct((bins, SLOTS, rows, 256), jnp.float32),
        scratch_shapes=[
            pltpu.VMEM((SLOTS, bins, rows, 256), jnp.float32),
            pltpu.VMEM((rows, rows), jnp.float32),
            pltpu.SemaphoreType.DMA,
        ],
        compiler_params=pltpu.CompilerParams(vmem_limit_bytes=30 << 20),
        name="cross_products",
    )(offsets[0], held)
    return cross[:, None]


def solution(mesh):
    placed = (P("fr", ("sr", "sc"), None), P("fr", ("sr", "sc"), None), P(("sr", "sc"), None))
    return jax.shard_map(
        local,
        mesh=mesh,
        in_specs=placed,
        out_specs=P("fr", ("sr", "sc"), None, None, None),
        check_vma=False,
    )
```

```python
import functools
import math

import jax
import jax.numpy as jnp
from jax import lax
from jax.experimental import pallas as pl
from jax.experimental.pallas import tpu as pltpu
from jax.sharding import PartitionSpec as P

MESH = pl.DeviceIdType.MESH

PLAN = (
    (
        0x00270068000d0000ffffffffffffffffffffffffffffffffffffffffffffffff,
        0x004e005b000d0041004e002700340000000000270068005bffffffffffffffff,
        0x0034ffffffffffff0027ffffffffffff000dffffffffffff001affffffffffff,
        0x001a004e000dffff0034001a004effff001a0068001affff004e0027000dffff,
        0xffffffffffffffffffffffffffffffffffffffffffffffffffffffffffffffff,
        0x0027005b005b002700270034001a00680034000000270034000d005b001a0000,
    ),
    (
        0x0068000d001a000dffffffffffffffffffffffffffffffffffffffffffffffff,
        0x004100270027000d0041004e0027005b0041001a00000041ffffffffffffffff,
        0x0041ffffffffffff0068ffffffffffff004effffffffffff0041ffffffffffff,
        0x0041001a001affff000d0041005bffff0068005b0041ffff0041004e0034ffff,
        0xffffffffffffffffffffffffffffffffffffffffffffffffffffffffffffffff,
        0x0041000d004e000d005b004e0041000d005b001a0000004e00680068004e0068,
    ),
    (
        0x0000000000340034ffffffffffffffffffffffffffffffffffffffffffffffff,
        0x000000410000005b001a005b0068004100270041000d0027ffffffffffffffff,
        0x000dffffffffffff0000ffffffffffff0027ffffffffffff0027ffffffffffff,
        0x000000000068ffff0000005b000dffff00270041004effff00000000005bffff,
        0xffffffffffffffffffffffffffffffffffffffffffffffffffffffffffffffff,
        0x005b00000000005b00000068000d0034002700410034000000270000005b001a,
    ),
    (
        0x005b00340041004effffffffffffffffffffffffffffffffffffffffffffffff,
        0x001a003400410068000d000d00000027004e000d005b001affffffffffffffff,
        0x005bffffffffffff001affffffffffff0034ffffffffffff005bffffffffffff,
        0x000d00340041ffff0068000d0000ffff000d004e005bffff005b00410041ffff,
        0xffffffffffffffffffffffffffffffffffffffffffffffffffffffffffffffff,
        0x003400340041001a004e000d0000001a001a0034005b0068005b001a0027004e,
    ),
    (
        0x0075086b086b083708370844082a0878084408100837084406330674082a060c,
        0x08370075086b083708370844082a08780844081008370844081d086b082a0810,
        0x0837086b086b01b70075025f021102450075022b02380204081d022b026c019d,
        0x0837086b086b083708370844082a02450844081008370204081d086b082a025f,
        0xffffffffffffffffffffffffffffffffffffffffffffffffffffffffffffffff,
        0x0837086b086b083708370844082a08780844081008370844081d086b082a0810,
    ),
    (
        0x08510075085e0075086b085e0851081d086b082a0810085e081d086b06190810,
        0x0068081d00750075086b000000750075086b00750075000d08780878085e0878,
        0x0068081d085e083700410844082a01aa0000081008370190007506740619025f,
        0x0075081d0075081d086b0000007508780041007500750844007500340000060c,
        0xffffffffffffffffffffffffffffffffffffffffffffffffffffffffffffffff,
        0x0851081d085e081d086b085e0851081d086b082a0810085e08780878085e0878,
    ),
    (
        0x0837081d0810081d08100878081d084408370851084408100674087806260878,
        0x086b001a085e001a003400750851081d007500680034085e08370810086b082a,
        0x004e0810081001c4086b022b022b01eb086b0252022b025f0878021e02040245,
        0x086b0027085e086b0075085e08510211086b082a0810025f08780878085e0245,
        0xffffffffffffffffffffffffffffffffffffffffffffffffffffffffffffffff,
        0x086b08100810086b08100878081d0844083708510844081008370810086b082a,
    ),
    (
        0x084408100068086b085e081d0810082a082a0844086b0878060c060c06400640,
        0x007508100068003408100878081d08440068003400410810086b082a0837085e,
        0x001a084408510190004e02450204025f0068025f026c0245003402450211022b,
        0x004e00410810082a004108780068025f004e0034084402450837000d0068022b,
        0xffffffffffffffffffffffffffffffffffffffffffffffffffffffffffffffff,
        0x084408440851082a085e081d0810082a082a0844086b0878086b082a0837085e,
    ),
    (
        0x06b407ea0626082a10471054103a1088105404701047040808370e770e770e43,
        0x084408b808ec08ec0075004108c5082a082a0a48089108780a48089e08ec1020,
        0x07ea025f021e09ba0a3b02790a6f1088082a0a480a2e10540a48107b103a1020,
        0x0844007500cf0204085e002708c50a3b0a3b08c508910a7c0a48082a08371020,
        0xffff08b808ec08ec0a3b08b808c508ab0a3b08c508910a7c0a48089e08ec08ab,
        0x001a004e00cf0068000d0075005b004e0211005b004e0075003400750075005b,
    ),
    (
        0x079c065a064d0041107b06260633065a107b103a0626106e1088082a106e065a,
        0x079c07dd089e004e00680a21009b08ab0a6f07b6001a009b10881088106e0a48,
        0x079c026c0252102d0034106e1061102d0a6f103a1020106e004e1088106e1088,
        0x006800680027026c001a08ec009b102d0a6f000d00cf106e0a6f089e00751088,
        0xffffffff089e09baffff08ec0a6f0a3b0a6f0a480a2e08b80a6f0a140a3b0a48,
        0x000d001a009b004e0034001a004e00cf0000004e00cf022b004e02110000065a,
    ),
    (
        0x060c06740619064010201088060c102d10471061042210200e5d1020107b103a,
        0x078f08ec07b608df0a6f02450a6208d206c1005b08ab089110471020107b103a,
        0x078f0204025f107b0a6f1088102d10540a3b1061105410200e5d1020107b103a,
        0x003408ec0034021e0252007508df1054007508ec08ab10200e5d08f90e6a103a,
        0xffff08ecffff08df0a6f0a210a6208d2ffff08ec0a5508910e5d08f90e6a09a0,
        0x004e002700750075025200000279026c004101b7023802790000004e0068000d,
    ),
    (
        0x001a001a007500e90633064d0640060c06c1067410540674107b06810e1c085e,
        0x06a707d000cf0891021e00f608df00dc00dc00c2022b0075102d107b08f91088,
        0x07c306740619103a026c102d1020103a02111054107b1088020401eb02790211,
        0x022b00f600a8061900c20a1408f9103a0a1400c2000d10880034022b00b50211,
        0xffffffffffff0891ffff0a1408df09ee0a140a7c08ab0a210e5008b80e1c0a62,
        0x0000008e002700e900410041002700dc008101aa0075001a00410027000d0041,
    ),
    (
        0x065a0619060c0626106e06401007103a103a086b0fd308850e500fb910470e77,
        0x07c3085e09390a1401aa08df005b004e0a21008e027900c2107b103a0f9f086b,
        0x0e430e500e360252081d09ee1007027901de0a7c0a55022b0000103a1047106e,
        0x0e430e500e360e840a4808df0e43026c0a21022b00f60a480a2e008100c2106e,
        0xffffffff0939096d0a4808df08f90af008f909ad0a2108c50a2e0e7708ab0a14,
        0x082a085e00340878081d0885086b085e0068086b085e0885084408850885086b,
    ),
    (
        0x004e0041002708780e770fe00fac085e0e840f9f0e6a1088084408850885086b,
        0x081d00f608ab096d027900c2004e085e01de020400e902790844088510070a7c,
        0x0a7c085e0fac08780a4808850e43085e040801eb085e0279068108850245021e,
        0x0a7c008108ab087808b800c20aa20279021e002700e90279027900f6008e021e,
        0xffffffff0fac091f08b809ee100709460eeb0c730fd30a2e0cc00fb90f9f0e36,
        0x081d082a00f6085e0844082a085e00410810085e0041043c085e000d08100027,
    ),
    (
        0x082a07d008df009b0fed08850fd308df0810085e085e0a3b04890fed08100e36,
        0x000d009b00340a2e00c2082a00c208df000d085e085e0a3b085e0a210810081d,
        0x0e77021e0ffa0a2e0e77026c026c0238085102450a210a3b026c0a21081001c4,
        0x0e1c0a140a62085e0844026c0a890238081000e90a480a3b001a088500a8029f,
        0xffffffff0ffa09120eaa0fac0fac09600e840e1c0e6a09ad0ffa0fed100708b8,
        0x085e0837088508850068081000a801f8085100e9008e00270810085e0878081d,
    ),
    (
        0x07c300e908ab01eb0ed10f9f0fb90e1c0eeb0fd30f9f0a891007085e0fb9081d,
        0x0a3b089e0a6f00b50a6200e90a8900e9008100cf01de02450810085e087808b8,
        0x0a3b06190fb901eb01f80e5d0a890a7c01aa09c7043c0a4801aa027901c4081d,
        0x0e770e840a6f08850ed10e5d00c20e1c00810e1c02790a2e00dc02790878086b,
        0xffffffff096d09460ed10f9f0fd30ae30fe00fd30e770e360eb70ffa08f90a7c,
        0x0810004108370000085108510837019d004e00cf0885082a08510837081d0851,
    ),
    (
        0x081d083700c20946102d0f8608370ec40fd30ffa0885082a085e0837081d0851,
        0x025f008100c208f9084401900081019d021e025f088509120eeb0fc608850851,
        0x08100db5099308f901c40810021e019d027909ba027908850a2e0190081d0851,
        0x0a6f08370ed10e36085100f6021e020400dc00f600680885008e083708ab0851,
        0x0d010ec40fb90fc60fac09d40fb90a950fd30ffa100709120e9d0ede0a950a95,
        0x00750068001a009b007500f6006800e9007500f6000d000d008e004100410034,
    ),
    (
        0x069a085e083700a80e360667107b08ec0891107b0a48036108510a210878107b,
        0x082a00e90837025f01f8014300f6024500c2086b01c4017708510837081d107b,
        0x0a6f103a08370fc60e430667107b106e026c107b01c4082a0851026c1095107b,
        0x042f0a2e0906025f0e43066700a8106e0891025f00dc043c00a80a21026c107b,
        0x0dcf0db509930eb709c70a62096009a00e770aa20e430c730eeb0c250fed0e77,
        0x00680075000d003400c2005b0075005b000d0068001a0041001a0034003400b5,
    ),
    (
        0x06f500f6084400b51054103a106e0681085107dd0851109508100fc610950fe0,
        0x0238027908440885080409d407dd0a7c00f607dd01f8008e106e081d10200837,
        0x0a210ddc09fb106e0804082a106e06810e7706810fed10950804081d021e0837,
        0x0e6a0afd00e90ae300f60885008106810f0506810e4304560844081d00cf0837,
        0x0c730f2b09fb092c08ab0d9b0aaf0bf20f050a950fed092c0c180fc60c180e84,
        0x02380279084400b500f60027009b011c064007dd00a8005b007500f600c20075,
    ),
    (
        0x06db089e00e908f9060c102008b80ffa102009c70e4308371020078f10880837,
        0x0252041509060211087808c5016a01b708b80891010f08371020106e10880c3f,
        0x0de9104702040211060c065a083709a001c4106e01aa08370211106e047d102d,
        0x025204150a950211087808c50837083708b8089100a80837085e085e02ed102d,
        0x0de90e9d0da80ae309930ac90dcf0b0a08b808910c180ac909a00a620a620c3f,
        0x06db041500e902110878009b016a00f600dc002700680190016a009b00b500c2,
    ),
    (
        0x081000cf0102081010611061066708510e0308df0681103a0eeb081d102d1061,
        0x07dd0252026c008e01c402fa014301c4085e08df085101f810611047102d1061,
        0x02040d9b026c08100a62106107dd020408780ffa0851103a025208371088060c,
        0x02040252026c0af000b5064006670b0a028508df0885103a048902d3081d02c6,
        0x0ccd0d9b0db50bbe0c3f0a080c730c3209460a2e0c8d09d40fb90ddc0eeb0c32,
        0x019d085100c208100279014301430204085e00750851008e00dc014301770136,
    ),
    (
        0x0598068108b806db088509060d9b08f9088508f9081d081d089e085108510844,
        0x08df0a6f02040245078f01eb087808f9016a08f90a4809d4089e085108510844,
        0x0885043c02791095079c019d08780885089101f8081d081d0e36085108510e6a,
        0x08df0af00f0502450dcf0906068108f900f608f906190ae3089e0c250a890844,
        0x08df0f380a9509930dcf0df60ede0afd093909a00e9d0ae30e290e4309060f52,
        0x0598043c082a06db00b5019008780000016a01eb00f6009b011c085108510844,
    ),
    (
        0x087807b6081d06e80eeb086b0fed086b064d0878082a0851082a08440e430f52,
        0x00dc022b081d00a808d2086b09fb0afd01aa0878081d0851082a0844084408c5,
        0x024509ba0e77024508d20ffa0885086b0c660878082a0c4c082a084408440844,
        0x0245022b02790cc00eeb065a0a3b086b064d0aa2089e085102e002fa03e208c5,
        0x0c320ddc0e7709870eeb0ffa09fb0fc60c660db50f9f0c320ca610140ffa0bb1,
        0x087807b6027906e8001a086b00dc086b08850878082a0851082a0844084401f8,
    ),
    (
        0x0702009b043c00c2068d0851065a0fc6081d0f8610070ac906b40e4307b60885,
        0x0a62021108b80ba407a9078f08b801020939091208b8086b0885090608d20885,
        0x0a4802110633022b0a2e05d906810fc60e5007dd1095086b079c09e103c80885,
        0x0a4802110a14022b043c0aa20e5008510e50091208b8086b06b408c508d20885,
        0x0e500e360fed0ba40ce70dcf0a9509870a080bd809e10ffa0f0509e1091f0987,
        0x070202110633022b064d05d9064d0851081d008e010f086b06b4015d07b60885,
    ),
    (
        0x07dd0878082a092c064d08ab0885063306b408370878086b097a08ab084408c5,
        0x0a1402d3021108ab01eb0837011c090606b4029f08780150097a08ab08c508d2,
        0x0a620e1c0211047d01eb08370a4806330e1c083708780a89097a0408102d0a3b,
        0x008e0e1c020408ab064d08ab064d09060e1c065a0878082a097a08ab047d08d2,
        0x0fb90e1c0aaf0cc00ddc09e10b0a0c180fed0ac909460ddc0eaa0eaa0eb7092c,
        0x008e02d30177047d01eb065a0885063306b401f80878017701f8027902fa037b,
    ),
    (
        0x0496059806b409870fe00d9b08440e360f790db50fb9089e08850906098708d2,
        0x0d1a0a6202e008440987013601b703470a7c0245016a0a890fed095309870946,
        0x0e5d0a3b0da80a550bff01eb0470062608850db507a9085107ea095303fc1061,
        0x0e5d0e5d08d208440c3f045604700e360eb706330e91089e009b0a6f0c251061,
        0x0e5d0eeb0e6a0b160fe00fed09460be50f790ae309600c3f0fed10070c250b16,
        0x049601eb02e0004101c407c300c2088508780633081d081d010f019001c4021e,
    ),
    (
        0x06810702079c064d108809a00dcf0a08069a064d064d08ab07d010140ffa1054,
        0x06db071b0a1402380885090609870a89027902fa080408ab092c07d00ffa089e,
        0x029202450fed02380c8009a00dcf08510422058b064d0c730e1c01f810201054,
        0x02920a89081d023806810e3604080702069a0bd80c18064006c10c8d06191054,
        0x0d5b0f7910140a0809870aa2091f091f0fb90f9f09120ad608c50afd0de90bd8,
        0x02920245024502380885029f0681029200c2064d00e9016a07d007d0021e03fc,
    ),
    (
        0x096d0728016a089107a90dcf064d092c062607d008b809a0074207c310540946,
        0x08780238023802b909e10a620b0a092c0ad607d002e0036107c31054105409ad,
        0x0e500e36023804560dcf061909fb08100626064010610d0109a010540e500f52,
        0x08780e36049602b90e5002ed047d0afd0e77061908510d010e840a7c0a550f05,
        0x0d1a097a09ad0af00c990af00d9b0bcb0e9d0f6c0db5091f0abc0e6a0aa20bcb,
        0x021e0463016a02b907a902ed06e803ef06260640029f0361074207c301de032d,
    ),
    (
        0x05d905b206330a3b08040df60ede08b8106e08850e9d068107020ede08040a08,
        0x027902fa0b7e0a3b011c0ac90abc08b80a0807ea09930de90702073508040a6f,
        0x02790a89105403c80e36041507ea0be507d0061910140e5d0b3d0a6208041095,
        0x0a550e9d02ac0eeb0e360ac90ede06740c6604fe00c2107b0eeb0a620ec40a7c,
        0x0fc609600b7e0dc20ae30ec40f4508b80e030f860bff0de90b3d0c8d0c4c0fb9,
        0x00a802fa02920279044904150422078f064d061907ea06810702081d01430463,
    ),
    (
        0x0449097a096d065a082a0953097a064d07b61020091f09fb069a0fac0fac06ce,
        0x089e010f0102092c06db08f90a95091f078f022b0143092c0a080a890abc0b16,
        0x0d1a07d00db50bbe0c1809d4080404150a7c0bd80c660f9f04220ddc0fac0bd8,
        0x0f120ae3085110200c1806ce02450a95065a0a950a210ec40e1c08b80ca606ce,
        0x09600df60e9d0be50c18093909ba0da808ab0e9d0b230f9f0dcf0df60ca60e43,
        0x088507d001020387068106f50804047007f708850143058b02fa04a303fc03ef,
    ),
    (
        0x064006db07a9085106190fd309460d820946062609600ddc0ffa069a0f9f0f93,
        0x06e803470b710bf20a210aa20b230b71094609390bcb09ee08d20a7c07ea092c,
        0x0e6a0b9710950df60a210c7301de0d820e030c730c3f0ffa0e290dc202380e77,
        0x0e500c4c0aaf0c8d08ab0fd304e402ac08c50ae306b40c730ede0a950cc00e36,
        0x09ba0af00f050df610070f520af008c50ffa0ed10c3f0a4810070af00af00c4c,
        0x04080190043c084402e001aa01de02110245047d0347054b02c60292031303d5,
    ),
    (
        0x072808b8098708ec0d7506000e9106a70d340e10102d0e500e9d07420fd306a7,
        0x096d0a140b0a02c609fb0a080aa20aaf0d3409fb0ae30a14080409a00a2e0b0a,
        0x0d9b019d103a0f6c068109c706260bf203ef03bb102d09ad0285101406260ce7,
        0x07280ef80b0a0a9509fb07020eb7043c08f90e5d062608ab0e9d02380e3606c1,
        0x09e10d270b0a09530f790bb10b3d0bbe0d340e100ae30bf20aa20aaf0c590b0a,
        0x072801f801b706f5068d019d06260810071b03bb043c06ce03e202fa037b00f6,
    ),
    (
        0x078f078f03d500cf0ce70d4e091f107b07f70de90fed0d4e0dcf10070ed10e29,
        0x0a21097a07dd029209930cc001c400810702099307c303470960096d0afd0a95,
        0x0e1c09fb09ad0ba40993021e0c3f0da80a1409930fd30c8d0c2509ba0e6a03bb,
        0x0e2902ac0ede04560ce70ed10c660ae3061902850e6a069a0c250ede04080a95,
        0x09390f6c0bcb0fe009a0097a0c3f0ed10c5909930d0e0c800d010ba40fb90e9d,
        0x078f00c2045606330783008106b4012907b6083701de034701aa012903c804fe,
    ),
    (
        0x063304b0015d06740e6a0e6a0eb70f9f0fb907f71088091206ce0df60da80f38,
        0x00f60afd09d40a55096d091f07350af008ab09d4078f08b809e10a6209460fb9,
        0x036e0df609d4102005d90e6a0d9b0bb107c309d410880e910e50025207d00fb9,
        0x0e84009b0cda08100ae3029f0ef804490ef803060c8d0e5d0f1206a706ce0a14,
        0x0d680d820e030f860eb7091f0abc0bb10ce70c3f0ddc0fd30de909ee0ae30f45,
        0x036e03470619064d0081013606db047d02850306025f0408048906a7058b0354,
    ),
    (
        0x0885074f0804088506b40d820e0309ad10880f930df607a906e80e9d08d21047,
        0x09ba01290b640be5091f075c092c09870878077601d1030608f90fe00d0e0b8b,
        0x09e1066709ee0a3b0a890681040808370be510950df607a90da8078f0a080c66,
        0x00dc031306b4089e04b00f050c990c3f0ec403ef068d09870d0e08df0d0e069a,
        0x096d0f930b640bff091f0dc20e030c3f09930abc0df60d010f790d340d0e0c66,
        0x06260129087802c604fe02fa05b2083704b00347028503060387042f036e01d1,
    ),
    (
        0x05f3082a077606f509fb0e1c0b640f520ef8089e0d9b08040f050f860de9092c,
        0x0d6809120aaf0bbe0912018309460bcb0a5502ed036e08c509a00aaf0ca60bb1,
        0x0e840c25065a0fed0e6a107b0fac0c8009fb0f9f0bcb0d5b0c73025f0fb90633,
        0x0c1806670456095308df0e1c065a0ed108d206ce0b640aaf0c800ce702e00ca6,
        0x0b1610140ede0fd308df0eb70b4a097a0c730af00ac90aaf0c730ce70c32096d,
        0x03bb059802c6046305980674075c008e00f6062606b40456066706810354036e,
    ),
    (
        0x054b03fc05a5015d07830769108809060f2b0e50079c0fd30fed0d340db508f9,
        0x09e109a00a21033a078309390d820e0307690a080b570bbe0fd309d40b230ad6,
        0x0b7109a0068104490e5d0c1810950ffa07690e430619074207f70e7704490c4c,
        0x0c730bf2046302ed0e1c0c660e5d04f10e840e500e8408d20d010e77025f089e,
        0x0b710bf20eeb0bf20d750ed10d750b710bf209d4096d0d750cb309ba0ce70b30,
        0x02c603130449044906e8076907ea064d05bf015d0279074201430361047d0150,
    ),
    (
        0x09600517059801500e910ed10f52109505cc0cda0ccd0ec406a70f6c0fed091f,
        0x009b092c0aa202ac076907ea0b3d0bbe0b8b0c0c0d0e09530f930b0a0f5f0c18,
        0x0da80fd3019d0dc20b710be505a50bd80e5d02110db50ddc0633062607dd0fed,
        0x085e00cf0af00c320c590cc00f5204ca08ab0c660e770e360292024506a706db,
        0x091209ba0cda0f520b710bbe0d0e0b4a0df60ec40ca60eeb0ba40c4c0f5f0fe0,
        0x0489044906b403c807c304fe07830804059807020783024505f3064006f501aa,
    ),
    (
        0x06c10769074207d005b20d1a10140f790fc60fac0ffa0d9b0d010f93070e06db,
        0x0b1602920912048908c502e0025f0bf202b90ccd01aa0c4c0cda0f93092c0b3d,
        0x0e290c730c6610540204060c0d27018305cc10140bff0d9b096005e609930fd3,
        0x06c1074f0c4c0c18097a08910abc10950c730ed10c3f0ede049606190f790667,
        0x0b0a0bcb0c8d0f9f096d0d1a0eb70f5209ad0ccd0d9b0bbe0cda0b3d0dcf0ef8,
        0x06c1074f04f108510422028501c40702040806a703c807a9074f0347070e0565,
    ),
    (
        0x09ba064d008107a904bd0f520dc210540600060c0da810540ed10f9f1007102d,
        0x0912078f08d2032d082a012907f70c0c00e901b70102070e0b4a0c3f0b570bd8,
        0x09ba101409c70d9b0bbe0dc20d0e0f9f0ec40e1c0da8026c0d9b081009c70e43,
        0x0b3d06a706400f05049602fa0e840e4309600f45060c02380cc00abc00810e9d,
        0x0ddc0dcf0dcf0b7e0aa20f860c990d1a0b97097a09c70f860d9b0f2b0f930f93,
        0x0320010f02ed041501f806ce071b0489050a06740702018303ae064d01900211,
    ),
    (
        0x05a505d906f508040db506f50f860f380e501095092c091f0ca60f1e06a70eeb,
        0x09ad0af002c6057f019d02ed036e0bff096002e00aaf0b300a7c0ca60a210b30,
        0x011c0da80de90e5d09e1062607d00d9b0df60bbe01d103e2047d020409e10d01,
        0x064d0ede0ad606b40cf40e840cb30c180667026c0c4c0aa20c73069a06f50279,
        0x0c660fd30b710d4e09460c0c0e9d0f380c990b230f1e0c250b230c800da80ca6,
        0x071b0361081d016a061907b6078f079c053e07a9020406a7053e019d02b90489,
    ),
    (
        0x07b605e606ce07c30ffa109505a50fed0d0108ec0bb108f90be50d8f0bb10735,
        0x0b7e0d340804019000f6088509060960092c02b90a6f0aaf0d820af00a7c0b7e,
        0x06000bcb05a50fd3083707a90abc043c0a480c25025f021e0be506330c320dc2,
        0x0de906b4068d0626090608b802ac06260af00abc0cc00b710c3f0e2904220cf4,
        0x0d750b7e0e840f6c0ffa092c0b230b230be50c250cc00b8b0d0e0d8f0e100d8f,
        0x042f066706e8012901aa07a9060c015d03ae025202e001aa0885011c04e400dc,
    ),
    (
        0x05bf075c071b00f60d270d680ef8069a09530939089e071b05580640096009ba,
        0x013609d401d10b71069a09600d27094603c806ce092c02c60d410b160a950bcb,
        0x054b0fc610880e4304560456101402520de90be50d410a210d8f0e91068103a1,
        0x0c9909600aa20ad600cf0cda0ca60e5d02d306b406db0f050d820d820ba40252,
        0x0b3d0afd0d4e0fed09120fe00d820ce70b8b0ce70f860fe00d8f0b16097a0d27,
        0x0354078f03d5073505580837044904f104fe081d074f071b028506db033a0361,
    ),
    (
        0x0939096d0129078f05f30d8f0df6088505170d8f0e9107c30fb9095308ab0906,
        0x0d9b015d0252032008b80252008e0da807c302c6030603ef0b0a0fd30b0a0be5,
        0x023803610e100bcb09530c0c05bf0dcf0b23060005e60572090601b707ea01b7,
        0x02fa03610a890d5b02fa04bd0d0e04fe042f0e3604150f1204080408004e0456,
        0x09870b4a0e100ccd09530d8f0ac90cf40bcb0f930f520dcf0f9309870d5b0fd3,
        0x0415079c03fc053103c804bd060004fe0728069a057f06c1017702c602c601b7,
    ),
    (
        0x05cc0285072805b2109507f7098710140939068d07280c7304a30e360eb7096d,
        0x0b30094609ba09530d410c7304e409ad021109600b8b02d30c250fb90bd80c0c,
        0x05cc04fe07f70e770b300d0e0f930e5d0a2107b60cda06400c660abc07f70a7c,
        0x0d820d9b071b0e5d0c320d0e09600c4c0ccd00a8070202d3022b04a3042f054b,
        0x0d820b970d410e9d0d410b7e0bff0d9b0f1e0d820bf20d3409390d750c660da8,
        0x02ed05b2037b0804077607f707d0037b0681029f02c603fc0422074206ce054b,
    ),
    (
        0x012900dc036106c10cc00eb7075c0fac10140e430906065a06190f5f0f790d41,
        0x09390953015d0b570da80d1a03200ba408100a2e096d094608b80b3d0b160bff,
        0x0d2706330bbe06330dc209ad0c7303d50b970fe00e770f860d411007067401de,
        0x0c6604f10d8208910e6a0eb70f050ede04ca0b3d02b90ef80e770cf402b9068d,
        0x0a950f050d750d7509600b160d010dc20b160bbe0ce709ee0c8009120d010d41,
        0x07f7009b0415057f036e051704700783042204fe00b5069a065a023806740387,
    ),
    (
        0x015006ce00dc08d2057f0ede0e9d0fe00bf20c8d0ba409390f6c03130ef809e1,
        0x06f5086b097a05cc00e906ce0d680de906a7094601eb0d750993092c0f520b64,
        0x05980c18107b0f2b03c80c4c0e910d4103fc0fed04630b230bff066703d50674,
        0x0aaf0456097a0e7704d704d70ce70f120cc00463085e090602ed0c4c02520c4c,
        0x0aaf0be50eb70c320d270ba40b570b1609fb0b7e0d410cf409600f1e0e770dcf,
        0x0449088507f7050a058b04d7065a06db019002110572015d05650183077607f7,
    ),
    (
        0x050a060c068d097a096005f310540b640d4e0b160db506a70d4e0fd3065a075c,
        0x011c01b701f801f80c3f09ad0c590b23025207c3036109a00f520aa2091f106e,
        0x0df60b4a0f9f0b970c32078f0e360a140912041506000c18019006190640026c,
        0x0b300d1a0bcb104700810a7c0e360e840bcb0eb70f1208c50c990640043c0489,
        0x0d9b0ccd0f6c0ffa0b160b300f050b6409c70d680b640be508f909460db50f2b,
        0x07dd07dd0496029f0742069a059804ca06000681079c07b60804070203e2075c,
    ),
    (
        0x057f0449040809ba05cc06330f930be50c590e840ede07d0029206ce0f6c0bcb,
        0x02e00b5703c80bd8012908d20313008e07d0021e009b03c80c800b570d5b0fac,
        0x09c704630ddc0c59064005cc0aaf051706190da802520953086b04ca0fc6064d,
        0x0b7e04a30d010e430d820c4c0df6089e04960ccd030602e00aaf0d5b02c60b7e,
        0x0b230ed10cf40d5b0cda0ad609ad0f5f091f0dc20bb10ec40c4c0be50d4e0d34,
        0x03ef0600010f05bf03940735069a053e06ce074f07d0074f079c021e064d074f,
    ),
    (
        0x06e8079c00f601020e8407830ce7106e06740fe0058b052402d3106e0e290742,
        0x0081050a02ac0a6f03d5015d01aa0d4108df0b23019d0b4a0e9d096009930fd3,
        0x0d5b0f2b07b6104703d5042f05720211038706330c800cb3070e0f9f042f0667,
        0x07760a3b0e43107b08ec09ad0e2905650b230d9b0d9b042f04bd02e008b8065a,
        0x0ce70d680de90d9b0d1a0c730bf20e0309530d1a0f2b10070d340cc00f5209fb,
        0x077603c8064d0456074f0387026c01eb0320040806db068d00cf0489068d069a,
    ),
    (
        0x016a0081015001830d5b05310e430fb90cda04b005cc102d06f506a7079c0b64,
        0x04560517032d0cf403610aaf0bbe0bb100b5019d025f02e00d8f0ffa0d750ec4,
        0x0a2e10950b3d0de90c8d0ba402380ad6096d0fd3065a021102ed0fac04d7043c,
        0x10070b230b8b06a70abc0b8b0eeb04d7089e0a7c02d306f506a7031302380c80,
        0x0b4a0d4e0df610070abc0b570d1a0df60db50df60f050cc00b300bf20cc00c25,
        0x027906330702042f080405310667036e042f07b604f1057202e0022b010202e0,
    ),
    (
        0x07d000b5028501d10b970e9107830cc007760c590de90e29074f0d9b0600106e,
        0x095303610810078f0a890851017702fa019d0292029f01aa1007078310470ffa,
        0x0e360ffa0d82053e078f04080fe0066703060f5207c3065a036e01830306054b,
        0x0e360cb30885106102d30b0a09ad059807830449057f0d5b050a043c00e904fe,
        0x0bb10b160fd30da80bff0bd80d5b0ffa0d9b0b8b0d750df60b4a0d680d410d82,
        0x07d000f60470070204bd023807b6045603a105cc0252070e05a500dc06810804,
    ),
    (
        0x011c00a805f301900ac905a50ac90e84072806a705a50a95049607f70c3f06c1,
        0x019d0a2e029f07c30bd8032003ef00a8009b01eb0354033a0f0507420fac0fe0,
        0x0b300fed0b160d410d1a036e07a90d750470081d0a080eb70456023801eb0598,
        0x0a2e0bb10c250a2e0bd80b4a0a480f7903540e77049604ca03060306056506b4,
        0x0f520ef80bff0b570f120da8096d0f790912092c0ba40b7e0b640de909e10dc2,
        0x074f03940320060c073506330524071b065a06db036107280558037b050a05f3,
    ),
    (
        0x071b074200a8070e06e80e100d5b0f120e7706b4096d097a0e100c18032008ec,
        0x0a0809c7050a0ac908df050a0d41010f01eb00b5012901de0f120e9d103a091f,
        0x091f05980cb3101408df0d2705650598085e0eaa050a07ea0b57068105f30600,
        0x04080a480e50108804490ede0f860b9700b504bd09ee06db00cf00a8022b057f,
        0x0cda0bbe0cb30b8b0bcb0be50f860fed0b7e0b300be509460be50d5b09930d68,
        0x037b056501f8078307b606e807020496029f06ce069a0449019d03bb03ae0183,
    ),
    (
        0x04150572046301de0e100f120db50d010b3d0f380ce709ad0bbe05a5074f0ddc,
        0x0e36091f01aa07d00d9b021e01360394022b03ae0d41089e0ef8074f0f380ca6,
        0x0b7e0b710dc20fac0d9b0f450eaa060002fa0d7507ea04ca0408043c0e360a2e,
        0x0c250c660eb70dcf0af0021103471088037b043c029f0e290bf201770e5002e0,
        0x09530c180ed10b7109e10bf20f520d8f0d410d410c990dc20b710d410c80ffff,
        0x03d5042f0517055806ce070e01b70143070200a801770804027904bd071bffff,
    ),
    (
        0x03e2ffffffffffff0f52102d0e1c0eeb0cb308910a9508b80e8408f90af00ede,
        0x0d34069a02b9036e09060afd07d00c800143ffffffffffff0fe00fed0e9d0d75,
        0x0b16102d0d010ddcffff05bf05f3091fffff10070fac03aeffff05f303a10238,
        0x0d680e100c590f450a620e50ffff0f86082a0afdffff102d02b900cfffff0d01,
        0x0b570f1e0bbe0b640f6c0b4a0de9ffff092c0f450d68ffff0891ffffffffffff,
        0x057f070207760517019d03ef043cffff025204700524ffff0136ffffffffffff,
    ),
    (
        0xffffffffffffffff0ad60ec4078fffff0d0effffffffffff0517ffffffffffff,
        0x05d9ffffffffffff015dffffffffffffffffffffffffffff0ffa0ae30912ffff,
        0xffff0f9f0fd30d8fffff0facffffffffffff0361ffffffffffffffffffffffff,
        0x0a210eb7ffff0d41ffffffffffff04b0ffffffffffff0b57ffffffffffffffff,
        0x0f790cda0f1effff0e84ffffffffffff0c4cffffffffffffffffffffffffffff,
        0x011c018307d0ffff008effffffffffffffffffffffffffffffffffffffffffff,
    ),
    (
        0xffffffffffffffff101404bdffffffffffffffffffffffffffffffffffffffff,
        0xffffffffffffffffffffffffffffffffffffffffffffffff0fac070effffffff,
        0xffff10541007ffffffffffffffffffffffffffffffffffffffffffffffffffff,
        0x0ec4ffffffff103affffffffffffffffffffffffffffffffffffffffffffffff,
        0x1014ffffffffffffffffffffffffffffffffffffffffffffffffffffffffffff,
        0x07eaffffffffffffffffffffffffffffffffffffffffffffffffffffffffffff,
    ),
    (
        0xffffffffffffffff0f45ffffffffffffffffffffffffffffffffffffffffffff,
        0xffffffffffffffffffffffffffffffffffffffffffffffff071bffffffffffff,
        0xffff0e84ffffffffffffffffffffffffffffffffffffffffffffffffffffffff,
        0xffffffffffff0e91ffffffffffffffffffffffffffffffffffffffffffffffff,
        0xffffffffffffffffffffffffffffffffffffffffffffffffffffffffffffffff,
        0xffffffffffffffffffffffffffffffffffffffffffffffffffffffffffffffff,
    ),
)
SEMAPHORES = (
    (0, 10, 20, 30, 40, 50),
    (1, 11, 21, 31, 40, 51),
    (2, 12, 22, 32, 40, 52),
    (3, 13, 23, 33, 40, 53),
    (4, 14, 24, 34, 40, 54),
    (5, 15, 25, 35, 40, 55),
    (6, 16, 26, 36, 40, 56),
    (7, 17, 27, 37, 40, 57),
    (8, 18, 28, 38, 40, 58),
    (9, 19, 29, 39, 41, 59),
    (0, 10, 20, 30, 42, 60),
    (1, 11, 21, 31, 43, 61),
    (2, 12, 22, 32, 44, 62),
    (3, 13, 23, 33, 45, 63),
    (4, 14, 24, 34, 46, 64),
    (5, 15, 25, 35, 47, 65),
    (6, 16, 26, 36, 48, 66),
    (7, 17, 27, 37, 49, 67),
    (8, 18, 28, 38, 40, 50),
    (9, 19, 29, 39, 41, 51),
    (0, 10, 20, 30, 42, 52),
    (1, 11, 21, 31, 43, 53),
    (2, 12, 22, 32, 44, 54),
    (3, 13, 23, 33, 45, 55),
    (4, 14, 24, 34, 46, 56),
    (5, 15, 25, 35, 47, 57),
    (6, 16, 26, 36, 48, 58),
    (7, 17, 27, 37, 49, 59),
    (8, 18, 28, 38, 40, 60),
    (9, 19, 29, 39, 41, 61),
    (0, 10, 20, 30, 42, 62),
    (1, 11, 21, 31, 43, 63),
    (2, 12, 22, 32, 44, 64),
    (3, 13, 23, 33, 45, 65),
    (4, 14, 24, 34, 46, 66),
    (5, 15, 25, 35, 47, 67),
    (6, 16, 26, 36, 48, 50),
    (7, 17, 27, 37, 49, 51),
    (8, 18, 28, 38, 40, 52),
    (9, 19, 29, 39, 41, 53),
    (0, 10, 20, 30, 42, 54),
    (1, 11, 21, 31, 43, 55),
    (2, 12, 22, 32, 44, 56),
    (3, 13, 23, 33, 45, 57),
    (4, 14, 24, 34, 46, 58),
    (5, 15, 25, 35, 47, 59),
    (6, 16, 26, 36, 48, 60),
    (7, 17, 27, 37, 49, 61),
    (8, 18, 28, 38, 40, 62),
    (9, 19, 29, 39, 41, 63),
    (0, 10, 20, 30, 42, 64),
    (1, 11, 21, 31, 43, 65),
    (2, 12, 22, 32, 44, 66),
    (3, 13, 23, 33, 45, 67),
    (4, 14, 24, 34, 46, 50),
    (5, 15, 25, 35, 47, 51),
    (6, 16, 26, 36, 48, 52),
    (7, 17, 27, 37, 49, 53),
    (8, 18, 28, 38, 40, 54),
)
NEEDS = (
    (
        0xffffffffffffffffffffffffffffffff,
        0xffffffffffffffffffffffffffffffff,
        0xffffffffffffffffffffffffffffffff,
        0xffffffffffffffffffffffffffffffff,
        0xffffffffffffffffffffffffffffffff,
        0xffffffffffffffffffffffffffffffff,
    ),
    (
        0xffffffffffffffffffffffffffffffff,
        0xffffffffffffffffffffffffffffffff,
        0xffffffffffffffffffffffffffffffff,
        0xffffffffffffffffffffffffffffffff,
        0xffffffffffffffffffffffffffffffff,
        0xffffffffffffffffffffffffffffffff,
    ),
    (
        0xffffffffffffffffffffffffffffffff,
        0xffffffffffffffffffffffffffffffff,
        0xffffffffffffffffffffffffffffffff,
        0xffffffffffffffffffffffffffffffff,
        0xffffffffffffffffffffffffffffffff,
        0xffffffffffffffffffffffffffffffff,
    ),
    (
        0xffffffffffffffffffffffffffffffff,
        0xffffffffffffffffffffffffffffffff,
        0xffffffffffffffffffffffffffffffff,
        0xffffffffffffffffffffffffffffffff,
        0xffffffffffffffffffffffffffffffff,
        0xffffffffffffffffffffffffffffffff,
    ),
    (
        0xffffffffffffffffffffffff0000ff00,
        0xffffffffffffffffffffffffffffffff,
        0xffffff14ff0a0affff0a0affff0a0a14,
        0xffffffffffffff0affffff0affffff0a,
        0xffffffffffffffffffffffffffffffff,
        0x32323232323232323232323232323232,
    ),
    (
        0xffffffffffffffffffffffffffffffff,
        0xffffffffffffffffffffffffffffffff,
        0xffffffffffffffffffffffffffffffff,
        0xffffffffffffffffffffffffffffffff,
        0xffffffffffffffffffffffffffffffff,
        0x33333333333333333333333333333333,
    ),
    (
        0xffffffffffffffffffffffffffffffff,
        0xffffffffffffffffffffffffffffffff,
        0xffffffffffffffffffffffffffffffff,
        0xffffffffffffffffffffffffffffffff,
        0xffffffffffffffffffffffffffffffff,
        0x34343434343434343434343434343434,
    ),
    (
        0xffffffffffffffffffffffffffffffff,
        0xffffffffffffffffffffffffffffffff,
        0xffffffffffffffffffffffffffffffff,
        0xffffffffffffffffffffffffffffffff,
        0xffffffffffffffffffffffffffffffff,
        0x35353535353535353535353535353535,
    ),
    (
        0x221804ff363636ff36043604ff040404,
        0xff222222ffffffffff0effffff2222ff,
        0x180e0e180e0e0e36ffff0e36ff3636ff,
        0xffffff0effff220e0e22220e0effff36,
        0xffffffffff22ff22ffffffffffffff22,
        0xffffffffffffffffffffffffffffffff,
    ),
    (
        0xff0505ff3705ff0537ffffffffffffff,
        0x191923ffff0fffffff19ffff373737ff,
        0xff0f0f37ff3737ffff3737ffffffffff,
        0xffffff0fff23ff370fffff370fffff37,
        0xffffffffffffffffffffffffffffffff,
        0xffffffffffffffffffffffffffffffff,
    ),
    (
        0x0606060638ffffff38ff06ffffffffff,
        0x1affff2410ff1024ffffff24383838ff,
        0xff101038ff3838ffff3838ffffffffff,
        0xff24ff10ffff2438ff242438ff24ff38,
        0xffffffffffffffffffff10ffffffffff,
        0xffffffffffffffffffffffffffffffff,
    ),
    (
        0xffffffffffffffffffffffff39ffffff,
        0x251bff25ffffffffffffffffffffffff,
        0x1bffff39ff3939ffff3939ffffffffff,
        0xffffffffff11253911ffff39ffffffff,
        0xffffffffffffffffff11ffff0725ffff,
        0xffffffffffffffffffffffffffffffff,
    ),
    (
        0xffffffffffffffffffff1cffff1cffff,
        0xffff1c12ffffffffffffffffffff1cff,
        0xffffffffff1c1cffffffffffffffffff,
        0x08080808122608ff3affffff12ffffff,
        0xffffff1cffffff12261cffffffff26ff,
        0x3a3aff3a3a3a3a3aff3a3a3a3a3a3a3a,
    ),
    (
        0xffffffff091d1dff091d09ffffffffff,
        0xffffffffffffffffffffffffffff1dff,
        0xffff1dffffffffffffffffffffffffff,
        0x13ff3bffffff13ffffffffffffffffff,
        0xffffff1dffffffff27ffffffffffffff,
        0x3b3bff3b3b3b3bff3b3bffff3bff3bff,
    ),
    (
        0xffffffffffff14ffffffffffffffffff,
        0xffffff0affffffffffffffffffffffff,
        0xffff14ffffffffffffffffffffffffff,
        0x000affffffff3cffffff3cffffffffff,
        0xffffff14ff14ff1eff00ffffffffffff,
        0x3c3c3c3cff3cffff3cffffff3c3c3c3c,
    ),
    (
        0xffffffffff1515ffffffffffffffffff,
        0xff3dffffffffffffffffffffffffffff,
        0xffff15ffffffffffffffffffffffffff,
        0xffffffffffffffffffffffffffffffff,
        0xffffff15ffffffffffffffffffffffff,
        0x3dff3dff3d3d3dffffff3d3d3d3d3d3d,
    ),
    (
        0xffffffff3e16ff20ffffffffffffffff,
        0xffffffffffffffffffffffff2016ffff,
        0xff160cffffffffffffffffffffffffff,
        0x0cff2002ffffffffffffffffffffffff,
        0x2020ff16ffffffffffffffffffffffff,
        0xffffffffffffffffffffffffffffffff,
    ),
    (
        0xffffffffffffffffffffffffffffffff,
        0xffffffffffffffffffffffffffffffff,
        0xff3fffffffffffffffffffffffffffff,
        0xffff3fffffffffffffffffffffffffff,
        0xffffffffffffffffffffffffffffffff,
        0xffffffffffffffffffffffffffffffff,
    ),
    (
        0xffffffffffffffffffffffffffffffff,
        0xffffffffffffffffffffffffffffffff,
        0xffffffffffffffffffffffffffffffff,
        0xffffff22ffffffffffffffffffffffff,
        0xffffffffffffffffffffffffffffffff,
        0xffffffffffffffffffffffffffffffff,
    ),
    (
        0xffffffffffffffffffffffffffffffff,
        0xffffffffffffffffffffffffffffffff,
        0xffffffffffffffffffffffffffffffff,
        0xffffffffffffffffffffffffffffffff,
        0xffffffffffffffffffffffffffffffff,
        0xffffffffffffffffffffffffffffffff,
    ),
    (
        0xffffffffffffffffffffffffffffffff,
        0xffffffffffffffffffffffffffffffff,
        0xffffffffffffffffffffffffffffffff,
        0xffffffffffffffffffffffffffffffff,
        0xffffffffffffffffffffffffffffffff,
        0xffffffffffffffffffffffffffffffff,
    ),
    (
        0xffffffffffffffffffffffffffffffff,
        0xffffffffffffffffffffffffffffffff,
        0xffffffffffffffffffffffffffffffff,
        0xffffffffffffffffffffffffffffffff,
        0xffffffffffffffffffffffffffffffff,
        0xffffffffffffffffffffffffffffffff,
    ),
    (
        0xffffffffffffffffffffffffffffffff,
        0xffffffffffffffffffffffffffffffff,
        0xffffffffffffffffffffffffffffffff,
        0xffffffffffffffffffffffffffffffff,
        0xffffffffffffffffffffffffffffffff,
        0xffffffffffffffffffffffffffffffff,
    ),
    (
        0xffffffffffffffffffffffffffffffff,
        0xffffffffffffffffffffffffffffffff,
        0xffffffffffffffffffffffffffffffff,
        0xffffffffffffffffffffffffffffffff,
        0xffffffffffffffffffffffffffffffff,
        0xffffffffffffffffffffffffffffffff,
    ),
    (
        0xffffffffffffffffffffffffffffffff,
        0xffffffffffffffffffffffffffffffff,
        0xffffffffffffffffffffffffffffffff,
        0xffffffffffffffffffffffffffffffff,
        0xffffffffffffffffffffffffffffffff,
        0xffffffffffffffffffffffffffffffff,
    ),
    (
        0xffffffffffffffffffffffffffffffff,
        0xffffffffffffffffffffffffffffffff,
        0xffffffffffffffffffffffffffffffff,
        0xffffffffffffffffffffffffffffffff,
        0xffffffffffffffffffffffffffffffff,
        0xffffffffffffffffffffffffffffffff,
    ),
    (
        0xffffffffffffffffffffffffffffffff,
        0xffffffffffffffffffffffffffffffff,
        0xffffffffffffffffffffffffffffffff,
        0xffffffffffffffffffffffffffffffff,
        0xffffffffffffffffffffffffffffffff,
        0xffffffffffffffffffffffffffffffff,
    ),
    (
        0xffffffffffffffffffffffffffffffff,
        0xffffffffffffffffffffffffffffffff,
        0xffffffffffffffffffffffffffffffff,
        0xffffffffffffffffffffffffffffffff,
        0xffffffffffffffffffffffffffffffff,
        0xffffffffffffffffffffffffffffffff,
    ),
    (
        0xffffffffffffffffffffffffffffffff,
        0xffffffffffffffffffffffffffffffff,
        0xffffffffffffffffffffffffffffffff,
        0xffffffffffffffffffffffffffffffff,
        0xffffffffffffffffffffffffffffffff,
        0xffffffffffffffffffffffffffffffff,
    ),
    (
        0xffffffffffffffffffffffffffffffff,
        0xffffffffffffffffffffffffffffffff,
        0xffffffffffffffffffffffffffffffff,
        0xffffffffffffffffffffffffffffffff,
        0xffffffffffffffffffffffffffffffff,
        0xffffffffffffffffffffffffffffffff,
    ),
    (
        0xffffffffffffffffffffffffffffffff,
        0xffffffffffffffffffffffffffffffff,
        0xffffffffffffffffffffffffffffffff,
        0xffffffffffffffffffffffffffffffff,
        0xffffffffffffffffffffffffffffffff,
        0xffffffffffffffffffffffffffffffff,
    ),
    (
        0xffffffffffffffffffffffffffffffff,
        0xffffffffffffffffffffffffffffffff,
        0xffffffffffffffffffffffffffffffff,
        0xffffffffffffffffffffffffffffffff,
        0xffffffffffffffffffffffffffffffff,
        0xffffffffffffffffffffffffffffffff,
    ),
    (
        0xffffffffffffffffffffffffffffffff,
        0xffffffffffffffffffffffffffffffff,
        0xffffffffffffffffffffffffffffffff,
        0xffffffffffffffffffffffffffffffff,
        0xffffffffffffffffffffffffffffffff,
        0xffffffffffffffffffffffffffffffff,
    ),
    (
        0xffffffffffffffffffffffffffffffff,
        0xffffffffffffffffffffffffffffffff,
        0xffffffffffffffffffffffffffffffff,
        0xffffffffffffffffffffffffffffffff,
        0xffffffffffffffffffffffffffffffff,
        0xffffffffffffffffffffffffffffffff,
    ),
    (
        0xffffffffffffffffffffffffffffffff,
        0xffffffffffffffffffffffffffffffff,
        0xffffffffffffffffffffffffffffffff,
        0xffffffffffffffffffffffffffffffff,
        0xffffffffffffffffffffffffffffffff,
        0xffffffffffffffffffffffffffffffff,
    ),
    (
        0xffffffffffffffffffffffffffffffff,
        0xffffffffffffffffffffffffffffffff,
        0xffffffffffffffffffffffffffffffff,
        0xffffffffffffffffffffffffffffffff,
        0xffffffffffffffffffffffffffffffff,
        0xffffffffffffffffffffffffffffffff,
    ),
    (
        0xffffffffffffffffffffffffffffffff,
        0xffffffffffffffffffffffffffffffff,
        0xffffffffffffffffffffffffffffffff,
        0xffffffffffffffffffffffffffffffff,
        0xffffffffffffffffffffffffffffffff,
        0xffffffffffffffffffffffffffffffff,
    ),
    (
        0xffffffffffffffffffffffffffffffff,
        0xffffffffffffffffffffffffffffffff,
        0xffffffffffffffffffffffffffffffff,
        0xffffffffffffffffffffffffffffffff,
        0xffffffffffffffffffffffffffffffff,
        0xffffffffffffffffffffffffffffffff,
    ),
    (
        0xffffffffffffffffffffffffffffffff,
        0xffffffffffffffffffffffffffffffff,
        0xffffffffffffffffffffffffffffffff,
        0xffffffffffffffffffffffffffffffff,
        0xffffffffffffffffffffffffffffffff,
        0xffffffffffffffffffffffffffffffff,
    ),
    (
        0xffffffffffffffffffffffffffffffff,
        0xffffffffffffffffffffffffffffffff,
        0xffffffffffffffffffffffffffffffff,
        0xffffffffffffffffffffffffffffffff,
        0xffffffffffffffffffffffffffffffff,
        0xffffffffffffffffffffffffffffffff,
    ),
    (
        0xffffffffffffffffffffffffffffffff,
        0xffffffffffffffffffffffffffffffff,
        0xffffffffffffffffffffffffffffffff,
        0xffffffffffffffffffffffffffffffff,
        0xffffffffffffffffffffffffffffffff,
        0xffffffffffffffffffffffffffffffff,
    ),
    (
        0xffffffffffffffffffffffffffffffff,
        0xffffffffffffffffffffffffffffffff,
        0xffffffffffffffffffffffffffffffff,
        0xffffffffffffffffffffffffffffffff,
        0xffffffffffffffffffffffffffffffff,
        0xffffffffffffffffffffffffffffffff,
    ),
    (
        0xffffffffffffffffffffffffffffffff,
        0xffffffffffffffffffffffffffffffff,
        0xffffffffffffffffffffffffffffffff,
        0xffffffffffffffffffffffffffffffff,
        0xffffffffffffffffffffffffffffffff,
        0xffffffffffffffffffffffffffffffff,
    ),
    (
        0xffffffffffffffffffffffffffffffff,
        0xffffffffffffffffffffffffffffffff,
        0xffffffffffffffffffffffffffffffff,
        0xffffffffffffffffffffffffffffffff,
        0xffffffffffffffffffffffffffffffff,
        0xffffffffffffffffffffffffffffffff,
    ),
    (
        0xffffffffffffffffffffffffffffffff,
        0xffffffffffffffffffffffffffffffff,
        0xffffffffffffffffffffffffffffffff,
        0xffffffffffffffffffffffffffffffff,
        0xffffffffffffffffffffffffffffffff,
        0xffffffffffffffffffffffffffffffff,
    ),
    (
        0xffffffffffffffffffffffffffffffff,
        0xffffffffffffffffffffffffffffffff,
        0xffffffffffffffffffffffffffffffff,
        0xffffffffffffffffffffffffffffffff,
        0xffffffffffffffffffffffffffffffff,
        0xffffffffffffffffffffffffffffffff,
    ),
    (
        0xffffffffffffffffffffffffffffffff,
        0xffffffffffffffffffffffffffffffff,
        0xffffffffffffffffffffffffffffffff,
        0xffffffffffffffffffffffffffffffff,
        0xffffffffffffffffffffffffffffffff,
        0xffffffffffffffffffffffffffffffff,
    ),
    (
        0xffffffffffffffffffffffffffffffff,
        0xffffffffffffffffffffffffffffffff,
        0xffffffffffffffffffffffffffffffff,
        0xffffffffffffffffffffffffffffffff,
        0xffffffffffffffffffffffffffffffff,
        0xffffffffffffffffffffffffffffffff,
    ),
    (
        0xffffffffffffffffffffffffffffffff,
        0xffffffffffffffffffffffffffffffff,
        0xffffffffffffffffffffffffffffffff,
        0xffffffffffffffffffffffffffffffff,
        0xffffffffffffffffffffffffffffffff,
        0xffffffffffffffffffffffffffffffff,
    ),
    (
        0xffffffffffffffffffffffffffffffff,
        0xffffffffffffffffffffffffffffffff,
        0xffffffffffffffffffffffffffffffff,
        0xffffffffffffffffffffffffffffffff,
        0xffffffffffffffffffffffffffffffff,
        0xffffffffffffffffffffffffffffffff,
    ),
    (
        0xffffffffffffffffffffffffffffffff,
        0xffffffffffffffffffffffffffffffff,
        0xff3cffffffffffffffffffffffffffff,
        0xffffffffffffffffffffffffffffffff,
        0xffffffffffffffffffffffffffffffff,
        0xffffffffffffffffffffffffffffffff,
    ),
    (
        0xffffffffffffffffffffffffffffffff,
        0xffffffffffffffffffffffffffffffff,
        0xffffffffffffffffffffffffffffffff,
        0xffffffffffffffffffffffffffffffff,
        0xffffffffffffffffffffffffffffffff,
        0xffffffffffffffffffffffffffffffff,
    ),
    (
        0xffffffffffffffffffffffffffffffff,
        0xffffffffffffffffffffffffffffffff,
        0xffffffffffffffffffffffffffffffff,
        0xffffffffffffffffffffffffffffffff,
        0xffffffffffffffffffffffffffffffff,
        0xffffffffffffffffffffffffffffffff,
    ),
    (
        0xffffffffffffffffffffffffffffffff,
        0xffffffffffffffffffffffffffffffff,
        0xffffffffffffffffffffffffffffffff,
        0xffffffffffffffffffffffffffffffff,
        0xffffffffffffffffffffffffffffffff,
        0xffffffffffffffffffffffffffffffff,
    ),
    (
        0xffffffffffffffffffffffffffffffff,
        0xffffffffffffffffffffffffffffffff,
        0xffffffffffffffffffffffffffffffff,
        0xffffffffffffffffffffffffffffffff,
        0xffffffffffffffffffffffffffffffff,
        0xffffffffffffffffffffffffffffffff,
    ),
    (
        0xffffffffffffffffffffffffffffffff,
        0xffffffffffffffffffffffffffffffff,
        0xffffffffffffffffffffffffffffffff,
        0xffffffffffffffffffffffffffffffff,
        0xffffffffffffffffffffffffffffffff,
        0xffffffffffffffffffffffffffffffff,
    ),
    (
        0xffffffffffffffffffffffffffffffff,
        0xffffffffffffffffffffffffffffffff,
        0xffffffffffffffffffffffffffffffff,
        0xffffffffffffffffffffffffffffffff,
        0xffffffffffffffffffffffffffffffff,
        0xffffffffffffffffffffffffffffffff,
    ),
    (
        0xffffffffffffffffffffffffffffffff,
        0xffffffffffffffffffffffffffffffff,
        0xffffffffffffffffffffffffffffffff,
        0xffffffffffffffffffffffffffffffff,
        0xffffffffffffffffffffffffffffffff,
        0xffffffffffffffffffffffffffffffff,
    ),
    (
        0xffffffffffffffffffffffffffffffff,
        0xffffffffffffffffffffffffffffffff,
        0xffffffffffffffffffffffffffffffff,
        0xffffffffffffffffffffffffffffffff,
        0xffffffffffffffffffffffffffffffff,
        0xffffffffffffffffffffffffffffffff,
    ),
)
LATE = (
    (0x0002, 0x0888, 0x0110, 0x7777, 0x0000, 0x0000),
    (0x000f, 0x0fff, 0x1111, 0x7777, 0x0000, 0x0000),
    (0x000f, 0x0fff, 0x1111, 0x7777, 0x0000, 0x0000),
    (0x000f, 0x0fff, 0x1111, 0x7777, 0x0000, 0x0000),
    (0xdfa8, 0x8007, 0x2fff, 0x0898, 0x0000, 0xf048),
    (0x9aff, 0x8b77, 0x3fbf, 0xdbff, 0x0000, 0xe000),
    (0x0fdf, 0x85df, 0x7fff, 0xac8b, 0x0000, 0xe000),
    (0xfff7, 0xfb3f, 0x3fff, 0x6dfb, 0x0000, 0xe887),
    (0x0dff, 0xe6f7, 0xc999, 0xfb7d, 0x7fff, 0x2000),
    (0xf75f, 0x7dff, 0xc9bd, 0xff7f, 0x37ff, 0x0135),
    (0x7fbf, 0xafff, 0xc9ff, 0xfeff, 0x5f7f, 0x0950),
    (0xffff, 0xffff, 0xc9ff, 0xffff, 0x17ff, 0x11c0),
    (0xefff, 0x5fff, 0xabfb, 0x1ef7, 0x3fff, 0xf7ff),
    (0xffff, 0xffff, 0xffff, 0xffff, 0x3fff, 0x9fff),
    (0xffff, 0xffff, 0xffff, 0xefff, 0x3fff, 0xffff),
    (0xffff, 0xffff, 0xffff, 0xffff, 0x3fff, 0xffff),
    (0xffff, 0xffff, 0xffff, 0xffff, 0xffff, 0xffff),
    (0xffff, 0xffff, 0xffff, 0xffff, 0xffff, 0xffff),
    (0xffff, 0xffff, 0xffff, 0xffff, 0xffff, 0xffff),
    (0xffff, 0xffff, 0xffff, 0xffff, 0xffff, 0xffff),
    (0xffff, 0xffff, 0xffff, 0xffff, 0xffff, 0xffff),
    (0xffff, 0xffff, 0xffff, 0xffff, 0xffff, 0xffff),
    (0xffff, 0xffff, 0xffff, 0xffff, 0xffff, 0xffff),
    (0xffff, 0xffff, 0xffff, 0xffff, 0xffff, 0xffff),
    (0xffff, 0xffff, 0xffff, 0xffff, 0xffff, 0xffff),
    (0xffff, 0xffff, 0xffff, 0xffff, 0xffff, 0xffff),
    (0xffff, 0xffff, 0xffff, 0xffff, 0xffff, 0xffff),
    (0xffff, 0xffff, 0xffff, 0xffff, 0xffff, 0xffff),
    (0xffff, 0xffff, 0xffff, 0xffff, 0xffff, 0xffff),
    (0xffff, 0xffff, 0xffff, 0xffff, 0xffff, 0xffff),
    (0xffff, 0xffff, 0xffff, 0xffff, 0xffff, 0xffff),
    (0xffff, 0xffff, 0xffff, 0xffff, 0xffff, 0xffff),
    (0xffff, 0xffff, 0xffff, 0xffff, 0xffff, 0xffff),
    (0xffff, 0xffff, 0xffff, 0xffff, 0xffff, 0xffff),
    (0xffff, 0xffff, 0xffff, 0xffff, 0xffff, 0xffff),
    (0xffff, 0xffff, 0xffff, 0xffff, 0xffff, 0xffff),
    (0xffff, 0xffff, 0xffff, 0xffff, 0xffff, 0xffff),
    (0xffff, 0xffff, 0xffff, 0xffff, 0xffff, 0xffff),
    (0xffff, 0xffff, 0xffff, 0xffff, 0xffff, 0xffff),
    (0xffff, 0xffff, 0xffff, 0xffff, 0xffff, 0xffff),
    (0xffff, 0xffff, 0xffff, 0xffff, 0xffff, 0xffff),
    (0xffff, 0xffff, 0xffff, 0xffff, 0xffff, 0xffff),
    (0xffff, 0xffff, 0xffff, 0xffff, 0xffff, 0xffff),
    (0xffff, 0xffff, 0xffff, 0xffff, 0xffff, 0xffff),
    (0xffff, 0xffff, 0xffff, 0xffff, 0xffff, 0xffff),
    (0xffff, 0xffff, 0xffff, 0xffff, 0xffff, 0xffff),
    (0xffff, 0xffff, 0xffff, 0xffff, 0xffff, 0xbfff),
    (0xffff, 0xffff, 0xffff, 0xffff, 0xffff, 0xffff),
    (0xffff, 0xffff, 0xffff, 0xffff, 0xffff, 0xffff),
    (0xffff, 0xffff, 0xffff, 0xffff, 0xffff, 0xffff),
    (0xffff, 0xffff, 0xffff, 0xffff, 0xffff, 0xffff),
    (0xffff, 0xffff, 0xffff, 0xffff, 0xffff, 0xffff),
    (0xffff, 0xffff, 0xffff, 0xffff, 0xffff, 0xffff),
    (0xffff, 0xffff, 0xffff, 0xffff, 0xffff, 0xffff),
    (0xffff, 0xffff, 0xffff, 0xffff, 0xfffe, 0xfffe),
    (0xfff8, 0xfff8, 0xfeee, 0xfeee, 0xfee8, 0xfee8),
    (0xe880, 0xe880, 0xe880, 0xe880, 0xe880, 0xe800),
    (0xc000, 0xc000, 0xc000, 0xc000, 0x8000, 0x8000),
    (0x8000, 0x8000, 0x8000, 0x8000, 0x0000, 0x0000),
)
LATE_BY = 5
NO_WAIT = 0xFF
GAIN_STEP = 2
SLOTS = 33
UNITS = 129
UNIT = 16
LANES = 128
STARTS = (0, 13, 26, 39, 52, 65, 78, 91, 104, 117)
OPPOSITE = (1, 0, 3, 2, 5, 4)
ORDER = (5, 3, 1, 2, 0, 4)
SENDS = 3
NOTHING = 0xFFFF


SIZES = dict(zip(STARTS, (b - a for a, b in zip(STARTS, STARTS[1:] + (UNITS,)))))


def size_of(entry):
    return 0 if entry == NOTHING else SIZES[entry % UNITS]


def neighbour_position(p, d):
    x, y = divmod(p, 4)
    if d == 0:
        x = (x + 1) % 4
    if d == 1:
        x = (x + 3) % 4
    if d == 2:
        y = (y + 1) % 4
    if d == 3:
        y = (y + 3) % 4
    return 4 * x + y


def signed(word):
    return word - (1 << 32) if word >= 1 << 31 else word


def entries(step, d):
    return [(PLAN[step][d] >> (16 * p)) & 0xFFFF for p in range(16)]


def mask_of(flags):
    return sum(1 << p for p, flag in enumerate(flags) if flag)


def gather_kernel(re_ref, im_ref, held, part, part_in, send_sem, recv_sem, load_sem, pair_sem):
    bins = re_ref.shape[0]
    tiles = re_ref.shape[1]
    fr = lax.axis_index("fr")
    sr = lax.axis_index("sr")
    sc = lax.axis_index("sc")
    z, x, y = sr // 4, sr % 4, sc
    p = 4 * x + y
    steps = len(PLAN)

    xp, xm = (x + 1) % 4, (x + 3) % 4
    yp, ym = (y + 1) % 4, (y + 3) % 4
    zp, zm = (z + 1) % 4, (z + 3) % 4
    targets = (
        (fr, 4 * z + xp, y),
        (fr, 4 * z + xm, y),
        (fr, sr, yp),
        (fr, sr, ym),
        (fr, 4 * zp + x, y),
        (fr, 4 * zm + x, y),
    )
    ahead = (4 * (xp - x), 4 * (xm - x), yp - y, ym - y, 16, -16)
    twin = (1 - fr, sr, sc)
    shift = 16 * (y % 2)

    barrier = pltpu.get_barrier_semaphore()
    for device in targets + (twin,):
        pl.semaphore_signal(barrier, inc=1, device_id=device, device_id_type=MESH)
    loads = []
    for f in range(bins):
        for half in range(2):
            for i, ref in enumerate((re_ref, im_ref)):
                place = 4 * f + 2 * half + i
                source = ref.at[f, :, :, pl.ds(half * LANES, LANES)]
                target = held.at[pl.ds(place * tiles, tiles)]
                loads.append(pltpu.make_async_copy(source, target, load_sem.at[0]))
    for load in loads:
        load.start()

    everything = held.at[pl.ds(0, UNITS - 1)]
    pltpu.make_async_copy(everything, everything, load_sem.at[0]).wait()
    pl.semaphore_wait(barrier, 7)

    def chosen(step, d):
        words = [jnp.int32(signed((PLAN[step][d] >> (32 * i)) & 0xFFFFFFFF)) for i in range(8)]
        words = [jnp.where(y < 2, words[i], words[i + 1]) for i in range(0, 8, 2)]
        word = jnp.where(
            x < 2,
            jnp.where(x == 0, words[0], words[1]),
            jnp.where(x == 2, words[2], words[3]),
        )
        return lax.shift_right_logical(word, shift) & 0xFFFF

    def needed(step, d):
        words = [jnp.int32(signed((NEEDS[step][d] >> (32 * i)) & 0xFFFFFFFF)) for i in range(4)]
        word = jnp.where(
            x < 2,
            jnp.where(x == 0, words[0], words[1]),
            jnp.where(x == 2, words[2], words[3]),
        )
        return lax.shift_right_logical(word, 8 * y) & 0xFF

    def guarded(mask, action):
        if mask == 0:
            return
        if mask == 0xFFFF:
            action()
            return
        pl.when((lax.shift_right_logical(jnp.int32(mask), p) & 1) == 1)(action)

    def transfer(step, d, source, target, size, arrival):
        return pltpu.make_async_remote_copy(
            src_ref=held.at[pl.ds(source, size)],
            dst_ref=held.at[pl.ds(target, size)],
            send_sem=send_sem.at[SENDS * d + step % SENDS],
            recv_sem=recv_sem.at[arrival],
            device_id=targets[d],
            device_id_type=MESH,
        )

    def for_each_size(sizes, action, among=0xFFFF):
        for size in sorted(set(sizes) - {0}):
            guarded(mask_of(v == size for v in sizes) & among, functools.partial(action, size))

    def send(step, d):
        waits = mask_of((NEEDS[step][d] >> (8 * q)) & 255 != NO_WAIT for q in range(16))

        def arrived(size):
            transfer(step, d, 0, UNITS, size, needed(step, d)).wait_recv()

        def action(size):
            source = chosen(step, d)
            transfer(step, d, source, source - UNITS * ahead[d], size, SEMAPHORES[step][d]).start()

        sizes = [size_of(v) for v in entries(step, d)]
        for_each_size(sizes, arrived, waits)
        for_each_size(sizes, action)

    def receive(step, d):
        sent = [size_of(v) for v in entries(step, d)]
        coming = [sent[neighbour_position(q, OPPOSITE[d])] for q in range(16)]
        for_each_size(coming, lambda size: transfer(step, d, 0, UNITS, size, SEMAPHORES[step][d]).wait_recv(), LATE[step][d])

    def finish(step, d):
        sent = [size_of(v) for v in entries(step, d)]
        for_each_size(sent, lambda size: transfer(step, d, 0, UNITS, size, SEMAPHORES[step][d]).wait_send())

    exchange = pltpu.make_async_remote_copy(
        src_ref=part,
        dst_ref=part_in,
        send_sem=pair_sem.at[0],
        recv_sem=pair_sem.at[1],
        device_id=twin,
        device_id_type=MESH,
    )

    for step in range(steps):
        if step >= LATE_BY:
            for d in range(6):
                receive(step - LATE_BY, d)
        for d in ORDER:
            if step >= SENDS:
                finish(step - SENDS, d)
            send(step, d)
        if step == 0:
            total = jnp.zeros((tiles, UNIT, LANES), jnp.float32)
            for i in range(4 * bins):
                piece = held[pl.ds(i * tiles, tiles)].astype(jnp.float32)
                total += piece * piece
            total = total.reshape(tiles * UNIT, LANES)
            power = jnp.sum(total.T, axis=0, keepdims=True)
            part[...] = jnp.broadcast_to(power, part.shape)
            exchange.start()
        if step == GAIN_STEP:
            exchange.wait()
            power = part[...] + part_in[...]
            gain = 1.0 / jnp.sqrt(power * (1.0 / 2048.0))
            gain = jnp.concatenate([gain, gain], axis=0)
            high = gain.astype(jnp.bfloat16).astype(jnp.float32)
            middle = (gain - high).astype(jnp.bfloat16).astype(jnp.float32)
            low = gain - high - middle
            row = lax.broadcasted_iota(jnp.int32, (UNIT, LANES), 0)
            rest = jnp.where(row == 1, middle, low)
            held[UNITS - 1] = jnp.where(row == 0, high, rest).astype(jnp.bfloat16)
    for step in range(steps - LATE_BY, steps):
        for d in range(6):
            receive(step, d)
    for step in range(steps - SENDS, steps):
        for d in range(6):
            finish(step, d)


def gathered(re, im):
    bins, tiles = re.shape[:2]
    steps = len(PLAN)
    return pl.pallas_call(
        gather_kernel,
        out_shape=jax.ShapeDtypeStruct((SLOTS * UNITS, UNIT, LANES), jnp.bfloat16),
        in_specs=[pl.BlockSpec(memory_space=pltpu.HBM)] * 2,
        out_specs=pl.BlockSpec(memory_space=pltpu.VMEM),
        scratch_shapes=[
            pltpu.VMEM((8, 128), jnp.float32),
            pltpu.VMEM((8, 128), jnp.float32),
            pltpu.SemaphoreType.DMA((6 * SENDS,)),
            pltpu.SemaphoreType.DMA((max(map(max, SEMAPHORES)) + 1,)),
            pltpu.SemaphoreType.DMA((1,)),
            pltpu.SemaphoreType.DMA((2,)),
        ],
        compiler_params=pltpu.CompilerParams(
            collective_id=0, has_side_effects=True, vmem_limit_bytes=24 << 20
        ),
        name="gather_blocks",
    )(re, im)


GROUP = 11


def gain_row(tile):
    wide = tile.astype(jnp.float32)
    return wide[0:1] + wide[1:2] + wide[2:3]


def spectra(held, f, first):
    halves = [held[pl.ds(first + 32 * f + 16 * h, 16)].reshape(256, LANES) for h in range(2)]
    return jnp.concatenate(halves, axis=1)


def cross_kernel(plan, held, out, order, staged, own_column, sem, order_sem):
    bins = out.shape[0]
    fetch = pltpu.make_async_copy(plan, order, order_sem)
    fetch.start()
    own_row = gain_row(held[UNITS - 1]) * (1.0 / 16.0)
    own_column[...] = jnp.broadcast_to(own_row, (128, 128)).T
    fetch.wait()

    def group(i, carry):
        for j in range(GROUP):
            place = i * GROUP + j
            first = order[0, place] * UNITS
            weight = own_column[...] * gain_row(held[first + UNITS - 1])
            for f in range(bins):
                mine, other = spectra(held, f, 0), spectra(held, f, first)
                full = lax.dot_general(
                    mine, other, (((1,), (1,)), ((), ())), preferred_element_type=jnp.float32
                )
                staged[place, f, :, :128] = (full[:128, :128] + full[128:, 128:]) * weight
                staged[place, f, :, 128:] = (full[128:, :128] - full[:128, 128:]) * weight
            pltpu.make_async_copy(staged.at[place], out.at[:, place], sem).start()
        return carry

    lax.fori_loop(0, SLOTS // GROUP, group, 0)
    pltpu.make_async_copy(staged, staged, sem).wait()


def local(spec_re, spec_im, offsets):
    bins, rows, segs = spec_re.shape
    tiles = rows // UNIT
    re = spec_re.reshape(bins, tiles, UNIT, segs)
    im = spec_im.reshape(bins, tiles, UNIT, segs)
    re = pltpu.with_memory_space_constraint(re, pltpu.HBM)
    im = pltpu.with_memory_space_constraint(im, pltpu.HBM)
    held = gathered(re, im)
    cross = pl.pallas_call(
        cross_kernel,
        in_specs=[pl.BlockSpec(memory_space=pl.ANY), pl.BlockSpec(memory_space=pltpu.VMEM)],
        out_specs=pl.BlockSpec(memory_space=pltpu.HBM),
        out_shape=jax.ShapeDtypeStruct((bins, SLOTS, rows, 256), jnp.float32),
        scratch_shapes=[
            pltpu.SMEM((1, SLOTS), jnp.int32),
            pltpu.VMEM((SLOTS, bins, rows, 256), jnp.float32),
            pltpu.VMEM((rows, rows), jnp.float32),
            pltpu.SemaphoreType.DMA,
            pltpu.SemaphoreType.DMA,
        ],
        compiler_params=pltpu.CompilerParams(vmem_limit_bytes=30 << 20),
        name="cross_products",
    )(offsets, held)
    return cross[:, None]


def solution(mesh):
    placed = (P("fr", ("sr", "sc"), None), P("fr", ("sr", "sc"), None), P(("sr", "sc"), None))
    return jax.shard_map(
        local,
        mesh=mesh,
        in_specs=placed,
        out_specs=P("fr", ("sr", "sc"), None, None, None),
        check_vma=False,
    )
```

```python
import functools
import math

import jax
import jax.numpy as jnp
from jax import lax
from jax.experimental import pallas as pl
from jax.experimental.pallas import tpu as pltpu
from jax.sharding import PartitionSpec as P

MESH = pl.DeviceIdType.MESH

PLAN = (
    (
        0x0010000800500000ffffffffffffffffffffffffffffffffffffffffffffffff,
        0x001800400040006800000010005800480058004800280030ffffffffffffffff,
        0x0060ffffffffffff0028ffffffffffff0038ffffffffffff0038ffffffffffff,
        0x002800300000ffff004800380008ffff007000180048ffff005000480040ffff,
        0xffffffffffffffffffffffffffffffffffffffffffffffffffffffffffffffff,
        0x0060005000700038003800300038002000580020003800080030004800000068,
    ),
    (
        0x0050001000580070ffffffffffffffffffffffffffffffffffffffffffffffff,
        0x007000300010001000100040002000680030001000500028ffffffffffffffff,
        0x0068ffffffffffff0020ffffffffffff0010ffffffffffff0068ffffffffffff,
        0x006800200020ffff001000400038ffff005000500030ffff004000400050ffff,
        0xffffffffffffffffffffffffffffffffffffffffffffffffffffffffffffffff,
        0x0030002800480018006000700020002800280008005000480070003000180028,
    ),
    (
        0x0048003800400050ffffffffffffffffffffffffffffffffffffffffffffffff,
        0x004000680008002000500028001000100048006800100000ffffffffffffffff,
        0x0008ffffffffffff0038ffffffffffff0018ffffffffffff0048ffffffffffff,
        0x004800600068ffff005800580048ffff001800700068ffff002800700030ffff,
        0xffffffffffffffffffffffffffffffffffffffffffffffffffffffffffffffff,
        0x0050005800500020003000180050005000380040001800680000002800280030,
    ),
    (
        0x0058006800600060ffffffffffffffffffffffffffffffffffffffffffffffff,
        0x005800180030004800700030005000180068006000400058ffffffffffffffff,
        0x0040ffffffffffff0008ffffffffffff0070ffffffffffff0028ffffffffffff,
        0x002000380028ffff001800000040ffff006000600040ffff000000200060ffff,
        0xffffffffffffffffffffffffffffffffffffffffffffffffffffffffffffffff,
        0x0070003800300058000000500028006000680000004800600008006000480000,
    ),
    (
        0x0020004800380038ffffffffffffffffffffffffffffffffffffffffffffffff,
        0x002800500018004000680058006800380060002800000068ffffffffffffffff,
        0x0010ffffffffffff0018ffffffffffff0028ffffffffffff0060ffffffffffff,
        0x003000480060ffff002800680058ffff000000000070ffff006000680068ffff,
        0xffffffffffffffffffffffffffffffffffffffffffffffffffffffffffffffff,
        0x0038004000000060004800600000005800080028002000100060001800580060,
    ),
    (
        0x0870086008800848084808400848083008680830084808180840061408100878,
        0x0870086008800848084808400848083008680830084808180840085808100878,
        0x08700860088001e3084802440244026c08680214084801bb0840024c022c01bb,
        0x0870086008800848084808400848026c086808300848024c0840085808100878,
        0xffffffffffffffffffffffffffffffffffffffffffffffffffffffffffffffff,
        0x0870086008800848084808400848083008680830084808180840085808100878,
    ),
    (
        0x084008380858082808700880083008380838081808600858061c0858065c060c,
        0x0840083808580828087008800830083808380818086008580880084008280838,
        0x084008380858084808700840084801ab08380830025c024c08800858065c060c,
        0x084008380858082808700880083008300838081808600818088008400828060c,
        0xffffffffffffffffffffffffffffffffffffffffffffffffffffffffffffffff,
        0x0840083808580828087008800830083808380818086008580880084008280838,
    ),
    (
        0x000008680008083008400828086008600848085008280878065c061c0664067c,
        0x0860086808600028084008280860086000100850082808780810083808380840,
        0x08600868086001eb08400234021401a3084808180860019308100214082801eb,
        0x08600868086008300840082808600838084808500828026c081008380838067c,
        0xffffffffffffffffffffffffffffffffffffffffffffffffffffffffffffffff,
        0x0860086808600830084008280860086008480850082808780810083808380840,
    ),
    (
        0x08600018086008680810086008380870087808100858087008800840064c065c,
        0x0880084800200830081000600838007808480810085800200818087008580810,
        0x088008480840018b08100880020c083800400244021402140078026c08380234,
        0x088008480840086800780860083802140078081000580214001800c10858022c,
        0xffffffffffffffffffffffffffffffffffffffffffffffffffffffffffffffff,
        0x0880084808400868081008600838087008780810085808700818087008580810,
    ),
    (
        0x088008480840000808580870081008680818083808300820081806740858066c,
        0x003800000840086808580860081008700878007000f108700870082808680870,
        0x08480850081001c30070026c023402240878022c0828019b0818061c066c025c,
        0x0848085008100870081000200060024c08780838085808700818087000100234,
        0xffffffffffffffffffffffffffffffffffffffffffffffffffffffffffffffff,
        0x0848085008100870085808700810086808180838083008200870082808680870,
    ),
    (
        0x0848085008100870105810501058104010781040105810280654087006440840,
        0x0848085008100870021c08700008086808180838083008201050106810201088,
        0x07df10701090105808580870021c018b08180850026c021c087006140204065c,
        0x007808f1001810580858087008100244081800380830023c0870082808680204,
        0xffff08f108e109010a7408c90a840a4c0a4c08e90a4c0a340e7c0a340a4c0891,
        0x000000000038018b001000780018003000500050000800380020003806440010,
    ),
    (
        0x06c5063c0644062c10801090104010481048041008b108c910500e6c10201088,
        0x06c507ff08e10901005800d90a8408c90a4c07c708b108c91090105010381048,
        0x07b71048106810380a740a641058104000501040105810280a6c0a3410200a1c,
        0x000808c1001010380a7408c908c110400a4c08e908b10a340a6c08c108d90a1c,
        0xffffffff08b908d90a4408f108c109f30a7408b908b109eb0e4c0e6c0e8c0a1c,
        0x0018007000e100e9004000080040007000780030006000180010005000100018,
    ),
    (
        0x066c07d707c70634105010381070107004181028107010681090106810381048,
        0x007807d7006808d90a440a3c0a5c0a2c01930a840a3408e11020104810481050,
        0x00781078107010400a440a3c10400a2c0a740a840a3410680e7c0a1c10381048,
        0x0058007808e910400a440a3c09010a2c0a740a440a3410680a3c090108c11048,
        0xffff08e108e909c30a640a3c09010a2c0a440a84089908e10a3c08c108c10a5c,
        0x002000600068000800080000007800080254001800780050005800d100080040,
    ),
    (
        0x06a5062408e908e1102010701048108010581060103810881020104810481050,
        0x07e707df0078007807bf0a6c08a908e10a4408c90a640a641028108010681020,
        0x00181058105010780a6410381070107007970a2c10380a640a3c105010480a7c,
        0x000008e1000810780a6408c108a910700a4408c908d1108802340a540a2c0a7c,
        0xffff0901ffff08e1ffff08c108a909c3ffff0a2c08d108a90a4c0a1c08b908a9,
        0x0028007800580010022c00480060000000480058026c00b1024c000800780078,
    ),
    (
        0x06e5065c08c90030067410801020107810881020106810801028108010681020,
        0x06e507bf002808c106b50a4c07b708b90a1407df0099007006f5103810781080,
        0x07c7065c10200a030a841070104810800a1410200a3c108000580a1410681020,
        0x00400070007802040a8400f908e11080002000780891108000200a1408b90a5c,
        0xffff08c908d108c1ffff0a4c08e108e10a5c08c90a3c0a3c0e8c0a140a5c08b9,
        0x00400020007800a900680099012a004000200081021400f101eb005800a10070,
    ),
    (
        0x06ad08c9060c00280e740e3c062c061c10281048104010301080103810781080,
        0x06ed08c908d1003000e900380081000806ed08f9006800e91080089108f1099b,
        0x07cf0a5c0a14108000501080102010780a5c10480a1410300a7c103810781050,
        0x0e5408c900a10e3c00c90028007010780a5c00f908b90a74004800000a5c1050,
        0xffffffffffff09cbffff0a6c0a5c0993ffff08f90a140a740a1c090108f10993,
        0x00580810004001930058003800700038004000990000027c0193007000c10058,
    ),
    (
        0x081008100018099b106808880e540e240860086008180458083008480e540e3c,
        0x081008100848099b07ef0888082808400860086008180848083008480a2c0820,
        0x0810100f0fd7099b0820019b02240a740860025c019b0a6c083010480e540a24,
        0x081008100848108008200888082808400040086008180a64083008480e541080,
        0xffffffff0fb7096209e308910a140a6c08b1089908b90a6c0e54089908a908e9,
        0x08100018084800a1082008880828084008600860081808480830084802140820,
    ),
    (
        0x0828088008f100400e440fd70fbf0880045008400fa70848059b05eb0e4c0e7c,
        0x0828088008f108f9085008180850088008880840087008280820086008200828,
        0x08280a440a2c0a3c085001930122022c0888084010400e8408200a3c08200204,
        0x0828088008f10a3c085008180850088008880840087010300820086008200828,
        0xffffffff094209e308c90a0308f108b90c480a640fa708b108990f9f0e1c0a03,
        0x0828088000c90091085008180850088008880840087008280820086008200828,
    ),
    (
        0x083008700028081808500e240e6c0e640e4c0e640e1c0e440ec508e105db0614,
        0x0830004800c9081808180810088808180a64007808880860086808e108180850,
        0x0a440a3c0e3c0a44027c0810085008180a6401db020c10880868065408180224,
        0x08300a5c0e3c0a440818021c088808180a6400580888027c086808e108180850,
        0xffffffff0fbf0a0308a909db0a6409420ee50c400fe709fb0ec50e740e4c0a24,
        0x0830087008780818081808100888081800700828088808600868000008180850,
    ),
    (
        0x08380888086808200fb70e5c0e3408100f05041808700478048902b508880820,
        0x00680888086808200078085808700810000008280a7c08c10a5c0fc708880888,
        0x08380a740a5c0a1401b3085808700810085801eb0a7c0e4c0a5c081802440993,
        0x0e1c088808680a1400c108580870027c085808680a7c082800a9081808880888,
        0xffffffff0ff7096a0eed09e309ab09db0f050e440e34095208f90e5c0ad508d9,
        0x0838088808680820007808580870081008580868002800400078081808880888,
    ),
    (
        0x08500830088800480efd08580e640e7c08300891088808c10fcf0868066c0880,
        0x08500830006008b900c908a9093a085008300891020c090109fb086808b10880,
        0x08300f9f0ff70a7408180fc7027c027c083004100a24090109fb086801b31080,
        0x08380a2c08880a74087808100e641048083000e10a24090109fb086808b11020,
        0x0cb909930962093a08e90fef0fff089108b909bb0e440a6408d90c680a2c0a74,
        0x0850083008880030087800280030085008300068020c026c0040086800200880,
    ),
    (
        0x086800f9085008b908780e440880084008500e34081008600868086008d10828,
        0x086800e908880a7c087808480048004000e908a908100a8c0fb7088008d10868,
        0x086810200a6c09a30a3c01c3093a08800850086801930a8c09a301ab016a01fb,
        0x086808300a6c081808680848093a022c0850004800b90a8c0078088000810868,
        0x09db0ed50982095208f10acd0ff709820e7c0af50e740e1c099b0aed0a34099b,
        0x086800e908500048086808480880084808500048081000700018088000380868,
    ),
    (
        0x0078003000b108b1103010981038105008581070102808990ecd10580a241030,
        0x0a84082808910089082008a108800848085008680a240078104010580a1c1030,
        0x0850023c105809930e2408180888023401db0a8c0a2c09e3001802640a1c0a4c,
        0x0850082808500e74007008a900a1084800c908a90a2c105809a30e1c0a240634,
        0x0c700c38089109930a140af5090908a908e10a8c0a2c08990ecd0fe708c90a4c,
        0x00480828002000400070002000a101f300300038011200280264007800500008,
    ),
    (
        0x006808280901067c0e54102810600818107003e70faf08281030107008180888,
        0x09c3002008d909a3002000f900700afd00700a1c00e100401030107010301038,
        0x0a1c1090091a0a7c08780a840af510900193011a0a541038026410700a740274,
        0x0a1c0e7c08d908b100e9001000e910500a540a1c0a5410380a8c007800700a2c,
        0x0c4008a90c5008c90efd0a840af50afd0a540a1c0e030a840efd0e8c0efd0a2c,
        0x000800680010007801eb005800e900c901c30060004000780048002000600038,
    ),
    (
        0x000800c9001009a30e2408a91098102808801038109810700e3c081010300850,
        0x026400c9091a08b106bd0020003001a301db0a140a8c021c06cd081010281060,
        0x09bb09ab10881028086808a910980a1c08801050108010700234081001a31030,
        0x0a7408b1089109a30a3c026c00c10909088008910a8c0a1c021408100a8c025c,
        0x09c309ab09c309720a340f9f089909090a1c0ae50a5409090c6808e90a8c09b3,
        0x006800c900080050002000680058027c088000100058002001cb081001a301ab,
    ),
    (
        0x09f30684091a060c106010200e3c102010980868083804080797081810981098,
        0x025c00780909021c07d70068078f00c900910a5c08e9024c1078102810980a64,
        0x0e6410981078103008880a8c0a6c0a2403971078046010580797102801db1098,
        0x0a1400680909103000f9021408d910200285022c08380a140038001000200e2c,
        0x0db309bb09bb08e90ef5089908d909a309f308d90a740a140a8c0a6408990ac5,
        0x00780010001800700888023400c10010009101db08380850088801c300680020,
    ),
    (
        0x05db08b9016a084010280838108010600a6408a903d70afd07e7107808300932,
        0x03ef09bb00a10274026c08f9084001f307bf00e10a740a540850107808301090,
        0x0a74108010980274078f083808401060003010380a1c0a540397027c08301090,
        0x08f100080a5c08b9088808380880106000b9082800f90a7c088800c908300ac5,
        0x08f10c580aad09bb0f4608f90fbf0a1c0dcb0aad08c109b30a340a2c09620b7e,
        0x00e9003000280840011a0838084002340010087800b900d90850001000300050,
    ),
    (
        0x06ed08f908d9085810781068093a10900909085810200a8c09a3109008481078,
        0x08f1027402a5025c00c1018b01ab0abd01c30038024c08800828109008481078,
        0x0a14104002c50c60064c08480880105001c30aad024c088008280274084801ab,
        0x089108f902c50214027c068d00b9105809090a4c0810088008280aad08480c90,
        0x09ab09eb099309eb09bb0c600a6c0abd0e1c0a5c0a0b0aa50a6408a10a740a64,
        0x045002d502c5085800c100100122004800c900700880088008280274084800e9,
    ),
    (
        0x067408d10878085008800e6c109010580285107808800838085008880e5c0818,
        0x021400d908500858011a083008b1012208800858019b00d906e5088808601098,
        0x0e2c0c401060027c01eb109801ab0a03038f09a301120478088801c30a240818,
        0x0a3400f908a90a24088008e908b106bd02ed0858082006240a740888086002ed,
        0x0f9f0c40092208d10c4808d1092a09d30a0b0a140b3e0afd0e440a9509cb0ebd,
        0x08580048083000280880083002640068077e0078082008380081088800400048,
    ),
    (
        0x01bb08e908a900680e6c1058084008d908400848085008500858102808701060,
        0x01bb0878027c08a109fb086808f9027c09d3087000f9088808580a240a240848,
        0x0a240a640a240a2409fb08680e24062402ed084809220888085809f308700244,
        0x0a240a4c0e34088806bd0868026408d900e90e6c00f1085008580b0d00e90244,
        0x0f1e0c200e5c0c780a030fbf0ad50bbf0ead09ab0a9d0d010fef099b08e90b05,
        0x08180878082000680112086801eb016a08400848024c08880068006808600818,
    ),
    (
        0x085806a50818086008300e3408680e2c0ed50fff092a0aa504f9088008600848,
        0x00c108a9081800990830083801fb08f1022409a3086808380c681020087009bb,
        0x085810070a1c0e240830020c0868027409d30828086808380a54012201830848,
        0x082008a90a2402740ecd02cd0030027408c108b10234107002ed012a0870027c,
        0x0c2010070e34095a0fef0c30099b09eb08c10fff0fef08f108a90c200c800b26,
        0x0820000802a50860083001420868024401930870006800e9003800a900700848,
    ),
    (
        0x08880820082808a110980878063409bb0fcf082010480e940888083010280830,
        0x0a2402d50828090901b30878020c09bb08a1090101930850109809d310170818,
        0x0a840e1c0e5c0a540a140e6c0e64020408a1026c083808c102140e3c109809bb,
        0x0a6c001008180a5400910a4408400a24084008700a1c106008500a2400910830,
        0x092a0dd308a9098a0a0b0e340a4c0ab509db0ad50a8c0be70c180aad0faf0899,
        0x088800f908180000067c087801ab00180099085808680030012a027c08700830,
    ),
    (
        0x07360634067c06140e9d0868105006bd08f90870092208300942082008400860,
        0x073609db0a8c0a840868017a01b30a44016a09eb09220a4c0a74082008400860,
        0x0e5c0274027c1050062c0a2c060c0a440060099b09d30a7c0850088808780830,
        0x024408200a8c1050046008a10091047809d30afd0a4408300942082008400860,
        0x0e240fd70c600add0edd0a740dab095a0ed50fbf09120b0d09420b0d0c780aa5,
        0x024406a5083808800828014a02950820027c03e7062c08300593082008780860,
    ),
    (
        0x069508b107af034607c7063c0e9409eb08d910880868109008281020087809ab,
        0x069502440ad50a2c08800a4408d1085806fd014a01cb013a0a540a95087808f9,
        0x0a3402d5023c0a6c092a0fef0e94046007e70e8c0644109001fb0a8401f31038,
        0x0e740204023c021c08600e6c060c10900274006806cd109006a50a8400f90274,
        0x0fbf0e240e7c0b3e09eb0bbf0b1e09120899098a09eb08910e5c0c480b2e08c9,
        0x021c0840023c0850064c07ff00910858006006dd0850017a00d9015a013a01eb,
    ),
    (
        0x0091078f0830088806c51040070e06340eb5099b062c0614089107af08500858,
        0x00910ae50089095a06fd090104a90a8c084002fd005802cd0891083008500858,
        0x09f31017025408380e6c10400a74063405e30870085006140a7409a308500860,
        0x00c10a6402540e540e6c014a0e1c06340eb50888020c06140a640a5c08500858,
        0x0e2c0c680faf0912101709eb09a309fb08910e340fb708a10cf109a30e9d09a3,
        0x072e0858025408380081082004a90089038f088803d7000008580132085000f1,
    ),
    (
        0x064c09a3091208800edd10780a74099b077e0880080710981060087809091028,
        0x09e302040254023c0a0308b9017a0a5c0922011a080708b90878087807970830,
        0x0c60027c0c38023c063c10480e6c0a5c07c706841090109809c30878026c027c,
        0x04500ae50c380878063c09090a74025406cd016a00c910980705087809010848,
        0x0cf90ab50c6809b30e9d0b050fef0a0b08f109930e2c09db0c4809f30c18091a,
        0x00d908200224023c07c70644067c064c02c5011a066c021c087808780840025c,
    ),
    (
        0x0654099b093208780cd107e70e1c0820059309a3093208e9084807ef08801058,
        0x00d9099b021403460756019309fb0aa5015a07e708780af5084808b9088008b1,
        0x024c099b0820107007b70a3410780e6c041807e708780e740848082008800858,
        0x0e240a6c0a1c023c0cd1047808680e6c0eed0e8c0a5c08f908780c8809b30818,
        0x09f30a1c093209db0cd10da30c180fa70eed0c5009320aad09720c880c900c90,
        0x08780818082803af00f1019301d3025402ed07e708780172084800b908800858,
    ),
    (
        0x062c0674017a098a067c1088064c0828082008880878062c06ad0edd093a1040,
        0x0a3403c70a0b08100a0b012a09320b0d08f9099b0afd08400bd707ef10800a0b,
        0x0e240ae50da30a2c0e9404d90e440478079f10801098084001e30a6c08401040,
        0x0a8c0a140efd03af0edd06640e940b0d068408800850064408f108d909621040,
        0x0fff0ddb09d3092a0deb0aad0ac50b9f09220add0fff0cc10c800a6c0aed0c58,
        0x024c03c7073607b701b3068d070e06bd068408800162040800b1010201b30112,
    ),
    (
        0x00f108a9063c012206fd0e1c0e2409120fb71068063c104006dd07f7108808e1,
        0x07050214097a025407e7082008e9019b06ad00c10acd03260aa5103009b31070,
        0x09e309a3063c025407c708200a1c1030064c0fb70e3c106007c707f709b31070,
        0x0e2c0214023402540e8c02dd072608f906ad061c063c0e840c6800990b2e1070,
        0x0a8c10170bdf0e540e940bdf09f308f9091a09520b7e0e7c0dbb0e3c09420c88,
        0x070502c5023406d50860017a00080878079f082003ff065c039707af016a016a,
    ),
    (
        0x061407f70112099306f506440fcf085806540664103008400878096a0eb508a1,
        0x021c08d90a4c0bf70091095208a103ff07c709ab00b10a030993096a07af1040,
        0x0c6801db08180e5405f3100f067c0c3007bf0e7406cd0a5c0891023c10700850,
        0x0c200aed0e8c089906d50e84070e0c900edd0e7c08d90e2c06b5096a0c881058,
        0x0f8608a1092a0aed0dcb0e130da30c400e2c09d30c600e4409c30c4009fb0c50,
        0x065c01bb00890810075607ef034e082808200306063c0840016a083001ab033e,
    ),
    (
        0x092a0858014208d1092a058b05a308f908701098066c065406d50ef5106009fb,
        0x0a2c09090244032e09ab00a102cd0b970274017a01db03f706d507cf094a0901,
        0x0a2c0c30026c03af0e8409eb01b30e8c0e0b0fd7064c06540a3407cf0a5c1028,
        0x06ad027c0244020c0c880acd0e440234049108c106740ae506d50edd09090901,
        0x0ecd0fdf0da30bc70f6e0de309820e8c09010aa50ad5099b0cb909cb0e940c20,
        0x046804890244024c00a902ed071e0888068d00e10593065406d507cf02fd0634,
    ),
    (
        0x070e087808700142057a06540e8c08a108a90684067408880e9d1088100f08f1,
        0x0a5409eb09d30ba704b101420cb909eb00b1074e0a9d051a08e908d910880a8c,
        0x0a5401fb0a3404b90deb066c0cb90c880e7c0674065c0810018b10881050067c,
        0x026c026c0acd10900ec5066c00f90e94068d0ad50e3c041004f90410060c08e1,
        0x0c500aa509a30cb90af50deb0eed09620f150abd0fd70a440d420cb10add0932,
        0x01fb01d301bb02d5079706bd04580634039702fd0840005800f905eb01830420,
    ),
    (
        0x072e079f092a09bb0d01095a0e440e5c05e30e440dcb0e4c108808c90ed50909,
        0x0a6c0285027403af02dd07ff02240aad07a702240b7e0aad093a07ff0a7c0aa5,
        0x0d9b01bb0fef0bb701f30da303df07cf0dcb05c301db0b970bd7067c0c8809b3,
        0x04480e3c0e7c10480d010e5c0a6c06e50e5c0e54067c0e740aa50b0504080cf9,
        0x0cd90a9d0e940eb50fbf0b9f09420c900c070afd0ac5093a0ca109eb0c500c18,
        0x026c02ad0418034602dd061c0726054a064403df067c074e079f01eb06bd03b7,
    ),
    (
        0x04e904d1064c08c107360e13067c0b7e0ead0fb707bf0982103808d90fb70b7e,
        0x022c0a1402e50b9f07360a14027c08e901cb0aa5022c029507f707bf0912091a,
        0x0a8c0e640bdf0fe7046002040624105809f30e1c07bf01cb078f0fc710800bdf,
        0x0a5c0ef50e4c0bbf0eed0e1c08f10e9d08e102dd0e4408400ebd0abd06bd0aad,
        0x09e30e5409ab0f7e09b30eed0a9510170cc10c6809930b970c780ba70c280acd,
        0x03ef01e30448045807d7067c064c07af04a9038f07bf0193036e07ff0244060c,
    ),
    (
        0x07cf0912066401db0ec5080707b7093a0fff06740e340952079f0ff70e34093a,
        0x08910af509f309eb08e90a0309db025c01eb036e0aed022c0eed08c9097a0a6c,
        0x0e541088079f046803bf0fbf0204025c0a0b0c500684060c0da3099b05db0e5c,
        0x0a840a840089106008e90e240aa510300e24027c0e940ac506dd0c180c380e64,
        0x0acd0dbb09f30c070ce90ae50c0f0c800bff09b30eed0ca909eb0de30d010baf,
        0x02850634050a087804b10797004807a704c105c307360766077607c7058b052a,
    ),
    (
        0x08180060017209db0f6e0820098a0e3c069d07ef0909092208e90ec50efd0942,
        0x00e902a50b6e02cd0099027c01a30982076602c50ad5039f09db0abd099b1028,
        0x0e4c05c30e1c06540c38065405a307970e9401830c58061c01cb0a8c0e3c0264,
        0x0e4c0c400e5407b708c90f0d0a4c0ee50f0d0766045806bd0c3802c502240eed,
        0x1017099b09fb0deb09ab0f5e0b0d0ba70a0309420aad0c3008f10e030f1e0bd7,
        0x0470035e017a0654014204e1072e03ff0776076606cd07a7080706d507860397,
    ),
    (
        0x072607bf097a079707e7060308180e9d0644098a09fb09cb05d30f9f094a095a,
        0x01e30d2201520aa508b9089907ff0962010a013a01eb0ad50972097208990bf7,
        0x0387038710480ee5066c0bdf0faf0e5c0c07109006640cc10a4c0fbf09a30e7c,
        0x04e90e540a4410700f6604500e2c0b5e00890e4404d1069d0ed50ce900e10e6c,
        0x09220ef5094a0faf093a0d520faf100709620cd90acd0ad50cf90ebd0dbb09e3,
        0x062c0244033e01eb06950132066c01420870016a05d3047806fd0183045005fb,
    ),
    (
        0x07e7079709d3019b0e940909072e0f6e039709ab096a0912077e0ed50e1c0a03,
        0x03870a2409320b97089907bf0ad503af009902e50b56025c0a03091209c30ae5,
        0x026c0fd701a30888045803af1038042807a707df10500fff027c0a6406440e24,
        0x0e6c0c300c8802b502c506240e6c0e6406f5043000d102fd0ca1025406641060,
        0x091a0e1c0acd0ba7098a0d090e0b092a0e0b0f6e0dcb0d110e340eb50eb509c3,
        0x072605bb01a30624038f07bf08180428000005eb00e9039f04b1031e03df0366,
    ),
    (
        0x07760091016208d9061c100f0fdf0ee507c70e840eed0f4e0fb70d9b09420fff,
        0x027c02ed029d094a0d220b05030e0af5096208c10aa5012a09cb09f30c800a14,
        0x0a7c0c200a0b0e1c0dcb06030e2c09f30e5c0bf7103007cf035e05eb10170478,
        0x04f90440020404a904200e440cb90c3006b50e340e5c0d010c180c9000991098,
        0x0e740e9d0ebd0b660f8e0bef0c500c07095a0cf10bff09420ca90c900c880d09,
        0x0089044002fd02f502f5048001f3037604a10684078f086804f9023c071e072e,
    ),
    (
        0x05c3008100a901b30cb10e94089909420f56074e105008f90b76078f0faf0366,
        0x092a028d09cb03cf01830ac501cb0b0500a10abd0a0b09e30da309420a6c0c07,
        0x0e940c3804700a5c0a5401b301a30e3c04380c180e0b02240c8007af0468018b,
        0x0cf90a1c0a140c580e9d046008e906c506950e1c0e340c900ee504a10a6c02f5,
        0x0f8e0b0d09120fdf0d010d820f050da30baf0acd0cd108b90c500afd099b0c38,
        0x0376041803a704b907e70489074e0450001807f7028506fd077e073607d70489,
    ),
    (
        0x0a6408a100d107360cc10ecd098209090ff70512094a096a06140ebd07760e44,
        0x01cb09b301d3097209c30cf90aa50a4c025c03460942099b08d90fdf0ddb0bc7,
        0x0de303c70f6610200e7410880c90053203b70e6404280ca90468065c0fa7066c,
        0x0a2c0c380a74065c06f509520f2e0fb704d90eed0ebd0c48020c0afd0d01063c,
        0x08c10bb70fff0baf096a0f460ea50dab0cc909620df309120c600ed50dd30909,
        0x07cf04c902950736077601a306e507bf073e05db042806dd03ef075e0430068d,
    ),
    (
        0x063400d100e900c9049906840f8e09b30cd108d907e7073e0f8607970f96094a,
        0x032e0b0d09930a9d0d6209e3010a09c309f3094202c501ab0a0b0cb90b8e08f1,
        0x0acd048909ab0bc70e8c0e5c0a4c05420d9b109805f301ab04380c2004400f26,
        0x0a4404d10a3c04800e44047006ed0e240ca90edd0e1c0a6c06f50c680e7c023c,
        0x0cc10b5e0dcb097a0bc70dc30bd70dfb09ab0f360b560ec5092a0a540b5e0fe7,
        0x032e04d102ed04600562066c0068077e0450015a069d04d9074e061405db07e7,
    ),
    (
        0x061c09010962079f0ce905a3094a10980f0d0e7c078f0f76091a05f30fff09b3,
        0x0008072e0a4402bd07af02e50d720a240e0b023c021c0b8609010aed0d820982,
        0x0e6c03ff05d3069d03e710900bf710170e540c070bdf0a740ba70fd7064c0410,
        0x06f504180aed08c104d904a90c300a5c0e84001004500acd0ca90ca9029d0214,
        0x0d6a09db0b6e0fe70d220e840abd08b10bcf0c0709620d8a0b7609220d6a0cf9,
        0x023c01b3027403cf062c078604f9071e051a013a070506f5002807f703970450,
    ),
    (
        0x071600890942070e09ab0fa710780fbf06ed072e0da3091a0cd10d220f3e0fe7,
        0x08b90abd0142096a0b5e025c02a5093a0a8c02dd08990abd078f10880b050b0d,
        0x05e3082001ab01ab0b9f0deb0f3e1007061c05e30f460a4c0e5c10170480021c,
        0x05cb0e4c0664062402440abd0ad50d5a0e2c0a9d04480ad500990c480ca10932,
        0x0de309120cb10bf709db0c400e9d0c4809c30cd10f7e0b660af50e940c580e34,
        0x071605e303b7030e06f507cf06ad074e075e073e02ad06ed03cf033e039f05a3,
    ),
    (
        0x030603ff07a7016205eb08f10f2e09f30fc70fcf059b07ff04a90f1e071e06e5,
        0x036608a109eb0c0709e309420b0d0d9b08d9095201830387079f0af50b26071e,
        0x03660d9b06741048026c0fcf022c07ef0bff0204018304200c3805c306840868,
        0x0c780e9d044808e9053a04890e340ecd04700ea50afd05010cf10e840ecd0448,
        0x0bbf0f6e0ddb0ecd0f3e0c380bf70ead093a0a9d0a030b760d320f1e0b3e0bcf,
        0x041801f30306069d057a079f047806e50418073607460512075e057202b5071e,
    ),
    (
        0x0922056a0152015a05420f2e0faf0fb7100f065c0f9f08b1074e0fcf07cf0f3e,
        0x08e107f70b360aed04580ae509a30be701e3037e029d0b76091a092209cb0baf,
        0x0c7009b30f4605fb0a2c023c04180b970387065c023c0fb702b50dcb021c051a,
        0x0f150e34050a0c200e840c8004800acd017a0e640e6406ed00f90a950d110ead,
        0x0ad50ca10fcf094a0b0d0f2e0baf0b4e09720faf0db30edd091a0cc10d820c68,
        0x04f10450047002c50786004004e105d303cf010a01a3069d0204072605fb04e1,
    ),
    (
        0x0a3c00e107b701a30fa705d30f0507660e0b0e5407d70ec506fd0f960fbf07e7,
        0x03260ca102850bff01c30264035e01eb095a0b0507df00c909eb0f560d6a0add,
        0x03cf10500f9f05db07970bb7060308070b97058b0fe71017045002540c6005fb,
        0x0e5c0e8c0a2c102000b9063c0e5c02a504c10d090a9d08d906ed042804910d3a,
        0x100f0d9b0f760bd70d620dab0dbb0b760c0f0d8a0e9d0ab50be70dbb0cf10cb9,
        0x067c0366067404080450016a018307c706ad0705073e075607c7017203460162,
    ),
    (
        0x091a0a5400f9093a1017057209420f8e0b760572036e0f1e0d1a0e640f1e0fc7,
        0x07160add0b4601bb023c01b301db09cb01fb015a03ff00810f8609eb09fb0a84,
        0x03ff0fe70fff062404400fb709f30f4e0baf023c0d92063409b30c9005eb0e74,
        0x04d90eb50c5008d9093a00b906ad020c0f1503460e74089100e902dd062406e5,
        0x09bb0ecd0d9b10170b5e0abd0b4e0d9b08e90cc109bb0d9b0d820dcb0ab50952,
        0x03f7075605b307af079f077605e3019b07cf06d503f70603069d07760522011a,
    ),
    (
        0x07b708070786011a032e07860e7c097a06cd07160f5e061c0ce910500ea5068d,
        0x0b9f08990b660cb9032e0cf10b5e0c07094a032e09f301420b260f6e09bb0b76,
        0x0aad0c28052a0deb09b30418100f059b059302540de30f4e0204043003f70254,
        0x0aad0e6c0e5c0e9406840ec50ec50d3a09010cf10f760ce90cc100d90a540891,
        0x0abd09720b660b6e10070f0d0f8e0ca10b860bd70cd90dfb0b660ca90b860d42,
        0x0797057a0582050a05d3035e0705063c0664071607b707f703df012a03f702ed,
    ),
    (
        0x032607cf077e063c0df3095207460f5e0cb908d105d30efd0ddb0d2a0982074e,
        0x019b09d30122015201320aad0bd70d220942075e0aad01020b760baf09820a54,
        0x0bff0da3103004580e440fa7018b0da3060310170fff05bb04600fcf09cb0e4c,
        0x08c10b050aa5063c04e90e540c480add04a902e504100efd0450009104400d1a,
        0x0edd0d220dd30c990d6a0cc10bcf0ec509420cc90b160cb10c400da30b460ae5,
        0x0634064c04c106f5026c04f10346056a062c072e04b107ff07af028d011a031e,
    ),
    (
        0x07ef072e0746073e0f8606dd0f860ef505f30d8a0ec50fd705420786077e08a9,
        0x09bb00a100d903560e34094a00c9013a01f30b4601220152096a0dfb0c0f0f4e,
        0x0d6a08400dd30b3e0d8a09e303f701d301f3102804400c5004400e8c05ab07e7,
        0x064c04580901106806ad06540408041000a102bd044007360c200acd00d904f9,
        0x0baf0fc70ed50d6a0b2e0cf909220dbb0acd0b1e09e30c380f960c180cc90da3,
        0x06950306087002ed06d5030e087804c10102057203a707360489063c077e030e,
    ),
    (
        0x0532061c08200091079f0fc709fb08b90f8605db0f360ebd075e057a0f360766,
        0x070e09e309bb02d5092201ab01320b6e012a09bb0bff0a9d075e0f660e0b0d2a,
        0x03af0cc906341090079f0c0f0a0310680be705ab0c300dfb0bdf057204300d7a,
        0x0f0d061c0e440ae508a90d1104280c60029d02cd062c0eed0cb1057204a10952,
        0x093209b30f660f660b360bb70f860aa50d620d2a0f260abd0d2a0dab0db30cc1,
        0x05320776077602a500e907560428026c029d0397039f0470035e057a0830032e,
    ),
    (
        0x077e034e0091016a0f960e7c07f70f4e057a0f4e0fd70f660d3a068d0f050fa7,
        0x0a0b02c505520de309520a340bcf056a08e9015209e302fd0f8e0bdf08c10b46,
        0x04f10ddb0c500df3065405a30f2e0d4a05f305930be70e6c0afd0ff707e70448,
        0x0ad50a440c2005a30e740faf0d010edd0cc900890eed0e5c06bd06d5067c0edd,
        0x0d1a0e3c0f1e0fef0a950fe70b160cf10c990a030ba70d090d6a0d720c680e2c,
        0x03660316049904e903bf034603d707ef0470055a04a904e105d3058203ef058b,
    ),
    (
        0x037e075605b300f90f360dab0e0b09520d82092a0b560f050e940b760e84092a,
        0x02dd0b6e05a303760a54073603460bd70387091a0bdf04f1092209820d5a0bd7,
        0x09ab0d22058b0fbf0438059b05fb10380a8c0faf0f4e04f102e50baf038702f5,
        0x02fd0e74029d06a504380c2804a10ead00e10cd90ead0aad01720cb9068d0c20,
        0x0c990ac50d010d090f360f1e0d4a0bd70db30d1109f30d320c900b760e840cb1,
        0x05cb06ad05a3076606a5085006030776059b0102019b035e0172017a038f05eb,
    ),
    (
        0x013a06e5012a013a0d6a0faf0f460ec5056a0d2a0f460d2210480e13095a07af,
        0x013a01bb028d0ad50bd709720d3a04c10952057a015202b508b10d420b3e0d92,
        0x032e0df3043003e70db30e9d0c5005d303ff07b71020057a05fb0e130e740438,
        0x0b3e0cf90c800b6e0e540ce10f150e4c0cc1029504b104d10438028d0cd10cb9,
        0x0aad0f1e0dbb0e940bb70aa50f460d1a0b160b970d3a0deb0dc30d9b0b7e0abd,
        0x013a04a903ef02bd0532036e05a305db054207b706440746070e01ab022c05bb,
    ),
    (
        0x033e00b1013a0962077e0dcb0ef50807068d05420fff07860fff076e097a076e,
        0x0a95019b013203ff077e0a9d050a0baf07cf0183032e03560ebd0f26092a0d8a,
        0x05db0e4c038f07970de30fff039f0e030336046803df0f9f043005820c68024c,
        0x0a9d0cc90cd10cc90ab50e8c0ed50cc9069d0ead0cf904910d320ed50f8608d9,
        0x0d22094a09eb0d5a0ab5096a0d5a0ca9094a0ead0f960bbf0d220a0b0d090d1a,
        0x056a0122077e056a05c30397051a072e049107cf03df049103af03e7017a0346,
    ),
    (
        0x06cd07b705c3095a08280d520f3609ab0e240fbf0f560d320e7c06d50d6a06ad,
        0x091a075e016209db093a0da300e10ca1019b0264036600890bb70aad0b2e0aad,
        0x05a30eb5051a0448024c038f0ff7071e0ad50fbf0e4401c3091a04a102240fe7,
        0x0cf108e90ebd0f7e06c50e2c0254071e039f05820aad0a540c80033e0cb10db3,
        0x0ba7098a0dab0abd09620c0f0ddb0cc10b660b460d620cf909320d4a08e10982,
        0x067407ef03bf0776052a0214035e01d3053204e901930552056a029501c30726,
    ),
    (
        0x09db0142075601f30d820b860fef072e054a10070e6407cf05ab0fb706dd0d1a,
        0x03ff0cf90b0d039f0274034604d101930bff01a302cd09820fbf0d220a95095a,
        0x0b9f0b760bb70d1a03cf0bd703cf1098065c10880e8c05b301db07ef05c30428,
        0x0ae50ca10add0af50cc1029d0e7c0cf10e3c09420f6e06a50edd0c6000c902cd,
        0x0ae50c180add0df30bd709720d320f460f9f0d090f760d6a09930c990a950dab,
        0x0387043803af0582058b020c04d1070e0336032e051a0152054204d1035e0306,
    ),
    (
        0x075604a9076607cf0f660f0d0f5e0d1a050a0ff709420d1a0f960de306bd0387,
        0x0183012a03ef098a0d5a0b6e035603ef00a9051a03970ae508c10afd0d110d22,
        0x0da30fdf0193056a02850fd704380dfb0c80020c02540f260356043804480593,
        0x0c500c600ed50a950f860ecd0df308e90cb10e84034608d10ead0c400f9602d5,
        0x0d5a0cc90d820ed50abd0f050b97091a0ae50b660dfb0b1e0d5a0ca10c480d4a,
        0x018303df0542055203ef070506ed041805f30489035e07760562076602e5074e,
    ),
    (
        0x050a060309fb035610070f5e09720dd30cc90f660e03092a07c706950d8a0489,
        0x0d1a034e0d6a05db01db014a02dd0b4e01020306037e00f90bff0f860de30b2e,
        0x0d22039f0828038f03970faf0dab0b4e06140e540f560d7204800e540d9b0dfb,
        0x0e8c0e840e1c0e640b7e06dd0d0904380ead0e740f260d72052207760ed50501,
        0x0d920bcf0ae50c600b7e0a9d0d220d010b360baf0c300b7e098a0d620de30fa7,
        0x037e0552080703760582019b04e90542017a01fb036603f7030e034e010a06a5,
    ),
    (
        0x04d906c5073e09cb0d620e8c0e1306740ebd0e240d920f0d0fbf0e8c068d04f9,
        0x0ddb0a0309010c180a6c058b033e03bf03b7093a003002ed0b360b0d0bef0932,
        0x0a6c0a540dcb0f4609bb01f303d70e0b0e440fff0bb7041006440684067c0bf7,
        0x0cb90e5c0bc70add03b7013a0b360a340e8c041807360e7c04400a3c02a50c88,
        0x0b66095a0c180dbb0d1a09cb0cc90b260e440b760d32093209120d2a0d3a0d52,
        0x03060387060305cb0193058b075605b3070e0418077e051a059b011a069d0285,
    ),
    (
        0x01e3066408d101d3100f0e740ecd0797067407c7051a09a30e1c0ead04f9072e,
        0x09220bcf092203ef0deb008100d1078f01320716030602140b460a6c0a9d0ba7,
        0x0c2010680f8603c70c0f0d010c0f09930c480bef0f1e0b6603df05bb018b01e3,
        0x0f3e0c200b0d077e0a1400810ef50d9b0ed500f10f150dc303df0ec5055a0d8a,
        0x0b9f091a0b360c200ca108e10d820cc909b309c30f3e096a0bb70bdf0ea50d92,
        0x02f5037607cf058b04e1057a02ed078f06e50542053a06bd06a50428030e0356,
    ),
    (
        0x015a01db01f3069d0b8e06740dfb0eb50efd0dfb0664050102c5097203c7036e,
        0x09eb0a6c0a6c083800b1098a04e10de30112014208f90d110b6e0d4a0c990909,
        0x03ef0fff0d010ead05220ff70d520a8c056209eb0f360c400501060301e304e1,
        0x0ecd0e1c0e740ead0285056a001002ed0b3e03af03b707050532026c021c0254,
        0x0d9b0d720aed0e5c0b8e09fb0fdf0d720abd0c0f0e0b0c400b970bef0c990ec5,
        0x0736039f05f308880522056a022c050104f9060303b7067c07e701f303c7015a,
    ),
    (
        0x04c105f300a104e90ddb0da3051a0fd703e70d9b061404890c40064c038f0d4a,
        0x0e4409420a1c089109bb03cf0dbb095a039f01eb08c9049109d309e3098a0bbf,
        0x0c400fef03af079f031e0fdf0d9b09db01cb1068106804680d22033e03a7033e,
        0x0d7a0e640f860f46089100c90a540b7601620b7602b502a50cd10e3c0264039f,
        0x0b7e0f7e0cc10d010d820d420d920f5609520c180bcf0db30b560d220da30cd9,
        0x02fd037e069d071e002806d503cf06f503e7070e02cd053a014a056a0112070e,
    ),
    (
        0x066408f1097200580e3c0f460f1510300ae506141078066c070506ad09010da3,
        0x089906ad0d7a00c902240b760b7e094a024402a503df0bef0a34076609a309e3,
        0x0e1309d305b30e8c0af501cb0ddb03ff020c0eed0e2c0deb03e701db0c500430,
        0x08e90b260b660d4a0bd70ae50ca90f96051a06dd0c600e9402ad04c900a9031e,
        0x0eed0bc70d7a0f56094a0d4a0d6a0edd100f093a0d920d820b5e09c30cf90ddb,
        0x02b50705078604c90397032e08580410033e05cb04d905ab07cf076e06dd07af,
    ),
    (
        0x04b904c90366014a0e8c07760d7a100f04a10c6006dd04e1037608e90b86061c,
        0x07970cd90bff0b2e025c09b303d70d7a02c50132017a05120de30dbb0fef0ca1,
        0x063c0fcf0faf0fcf0ae5045804e90244007803df10070234027402c501bb05bb,
        0x0edd0ad50bff0e6c02b50a1c0f5e072e06c500d90f4e0e6c0376035600d10480,
        0x0d1109620d720f0d0c580f6e0d720b1e0dfb0b260ca10f6e0d3a0df30ee509d3,
        0x0766055a061406030705033e0766062405db041004d106240376016a014206e5,
    ),
    (
        0x0489064c05ab01c3038f0fef0fff0d4a0cd909720d8a0e5c0f8e08a90b7e0532,
        0x03af0d7a022c0a9502440a8c0993050a0c0f00b9013a01eb09e30d320bf70b26,
        0x0e8c0c680fb70c7002c50a9d074603f70a240d9b0a4c04080603030605a301a3,
        0x0b860add0ca90b1e04400bbf02fd0cc108b100e9009104e903c70e9400b10410,
        0x0f0d0d3a0abd0fd709720c070d52093a0fc70e0b0d110ddb0cb10b1e0912094a,
        0x05db04a1076e075e030606a507460336041003760316058202a50306038705c3,
    ),
    (
        0x07a708c1055a061c0d220deb0efd0d820edd0d620d4a05e30f360fe706a5031e,
        0x096209120cb100c1072e0deb0b97057a037600d1022403ef09c30f460c07097a,
        0x011a10380db30fef0d22067c03060a3407ef085804f90830024c03a701c30582,
        0x0ebd0ce10eb50d620b46039f0e5402240bd704700cc1053200c9018b02b502bd,
        0x08b90b660ce109820fb70f760fe70baf0f560982094208c9092209620b260b86,
        0x031604d9070504990654047806d5076e053a04f102fd04c90756035e029d0460,
    ),
    (
        0x097200a9039f00b102a510300edd0d3a0e940ead0dbb10170634100707c70fd7,
        0x00b902950a7400b103a70b360a640ac5013a09c30dd305b30d6a10070ad50a2c,
        0x0e740faf039f0c180366105003a70d010e2c05f30c480baf030e0244043801f3,
        0x0e7c0b2e0ecd0326036e02ad0bcf0ac50dbb052a0eb5090906ad028503ef04a1,
        0x097a09420c0709420cb10bf70edd0d3a092a0be70c48091a09b30f5609a30eed,
        0x00b90224012a07ef0366052207f702d5051205930532041003b705db01f30776,
    ),
    (
        0x099308e1035e096a0ce10dfb05520fff030e08f106cd035e06f5072603bf04d9,
        0x07cf0d520a9509fb0d7204b903060dbb03bf011207d7036e0f150a030f660e0b,
        0x0c280e740d420fa7057a01830d320a6c063c0f4e051a032601420664032e05d3,
        0x0b5e00c90bbf027c0c380ea503060c2804580f760552074e014a02e5052a068d,
        0x0d820f0d0efd0c480cb909620acd09720d9b0efd0f360e740add0be70cd10bb7,
        0x0326079707d70480016a05fb05d305bb06b5061c075605e304780501027407df,
    ),
    (
        0x01120000073601e307560c9007050b36051a03760f1e05eb0dbb0756067c04e9,
        0x00c9023c043800f1026407ef04b109fb0ca1051200890be70ee5094a07d70993,
        0x0e1c04b9075e0cc901a307ef0a8c0410060c0d620a5c074605db0542055a055a,
        0x06c504b9070e0d9200810542023c0b05042002d509420edd0d8a06a506440f6e,
        0x0f5609a30e640c500c180bd70ae50b160be70b4e0d7a0c500fc70d010d721017,
        0x01bb05d3018b05bb027c072604c10356042003bf048904c100b90705023407a7,
    ),
    (
        0x05820644071607050f0d0d010d820f46055a071e076e09620bff0a0b05220654,
        0x082000b104f901b30dd308b1094a0ba7018b026c03160dcb0d2a08e909930efd,
        0x0e0b0c500d720fd705bb03b709bb0d320e9d0b76077e0a0b0c90022c02b505c3,
        0x0ec50ead0edd108805620f26066c089906340b1e074610280397054a0a34065c,
        0x0f7e09820f360b260d5a0ef509520ff70b7e0f960faf0f2e0b0509e30cc10d8a,
        0x059b071607f707a7039f055a049104d9081001120776054a0501073e06b504c1,
    ),
    (
        0x07bf00f100f106f50fbf10070f3e0932103009fb0c3808d90e8c073608f10522,
        0x03df0499024c011a07760a7c05cb01cb0c8000a104280e0b0eb50b460cb1098a,
        0x01b30d4a09a30e640b5e04800dbb047002340e9404500bdf0dfb066c04a10828,
        0x0d110a7405720c38062c07860b970f3e0aed0c48057a0c280e24037e0aed0776,
        0x0ead0b56096a0e9d0c070d720d110e740aed0c480ecd0ee50d620ef50e640b9f,
        0x02dd0499030e052a012201c303970460034e0468033604a9021c037e032605d3,
    ),
    (
        0x02ad03a701b306030f8e0d4a0f0d0716091207af0fc705320be708b10d92050a,
        0x053a08b103d702c507b7057a0797048901bb097a052a0b660a8c0d920b5609eb,
        0x054a0d3210380f2601c3071e0da301db06640888074e09d30c4003560c580838,
        0x0d320edd04600ddb02fd04b10491095207160d92023c03af0b3602140e840460,
        0x09820e0b0b050ebd0c200ce10972100f0b260dcb0c280da30ce10b050dcb0be7,
        0x0408057204d90501078f02c5021407160654054a012a045801420387042004b9,
    ),
    (
        0x012a089103e7002006d504a10d9209fb0d0107050b7e07760acd070e0e940746,
        0x039f0d3a08e9014a0891039f09d306030d010b560c40034e0d920b4e0b1e0ce9,
        0x010a0cb107760baf0603079f0e130f05051203c706340ca1060c0f760cf91078,
        0x06fd037e033e0cb10b2e0899065c0dd304e1089902fd0d11092a0b5e07760ae5,
        0x0f5e0af50f9f0de30bbf0b760e2c0b6e0f360b360aed0fff0c200c600ef50edd,
        0x03e7036e01f30522046801830010028d05b301d304f903a701e3077e0410077e,
    ),
    (
        0x02c501fb010a0552065c096a06bd0e8c067c098205b30b8e0e540ee510700ddb,
        0x0b760ad50bc70b6600e104910b4e09320489043005eb099309b30bf70a8c0a34,
        0x03f710300a8c04e9090103df040810480b160df304a90cf10b5e0880074e0810,
        0x0274064c0542071600990bd70d5a0d090b7e0ca1092a06030674064c0cf10e84,
        0x09d3092a0f0d0aa50e1c0d1a0d8a0fc70f7e0fcf0ea50bef0fb710600bf70faf,
        0x015a060303c70099033e031e02a503bf02f5064c025c06c5005004b907660468,
    ),
    (
        0x029506cd080700e107ef074e08b9100710070d6a05bb05ab09220d3204f1064c,
        0x06bd071e08a9040802950552051a01e30b97098208e1098a0a9d099b0d010b4e,
        0x0183030e059b0ba702540c780cc9051a015a0a4c0b16031605b309620d7a0e2c,
        0x04a102b503260cf10899064401e30d6207560776033e097a0ce90c9904c90e4c,
        0x0dcb0da30fa70cd10c380e030fcf0f660de30d4a0b860c0f0c280d090ed50bef,
        0x05c303ef032e0562038705cb078f05e30458042002e501e302c5035603b706fd,
    ),
    (
        0x041801d30132ffff08b9066c0afd108810500ea50b660f4604200b5e08f90e74,
        0x02cd05120a240c5002c504890122089103c709320ab5ffff100709a30ab50f2e,
        0x0888056203a707af0c3007c708380baf09a307af09620922ffff07bf034e032e,
        0x06140d720c680ed50dcb094a06840f2e023408d90a840962030e0532ffff0c40,
        0x10070dab0bef0b4e0cc90ea50ec50d090cf9100f0c180fe70f360baf1017ffff,
        0x0132014200b10705045802dd0366ffff02cd02dd0468ffff061cffffffffffff,
    ),
    (
        0x010affffffffffff03df06c508e908f107cf08b909cbffff0d320f260d09ffff,
        0x038f0a6400f1ffff0b9f04f10bbfffff05bbffffffffffff0c0f0be70aed0972,
        0x030e01cb0736075effff035603970afdffff0fc704d10726ffff0c30ffffffff,
        0x061c055a08990ecd0c4802edffff06840afd0468ffff0ebdffffffffffff0c30,
        0x0af50c880ee5ffff0d09ffffffffffff0b0dffffffffffffffffffffffffffff,
        0x034602bd0460ffff066cffffffffffff018bffffffffffffffffffffffffffff,
    ),
    (
        0xffffffffffffffff0b0509eb0da3ffff0952ffffffffffff0cb9ffffffffffff,
        0x0858ffffffffffff091affffffffffffffffffffffffffff0ce10a2c0f5effff,
        0xffff03b701eb073effff0a4cffffffffffff0a14ffffffffffffffffffffffff,
        0x04780b66ffff0810ffffffffffff0b16ffffffffffff04b1ffffffffffffffff,
        0x09520ee50fefffff0e34ffffffffffff0c18ffffffffffffffffffffffffffff,
        0x049904f1ffffffff0430ffffffffffffffffffffffffffffffffffffffffffff,
    ),
    (
        0xffffffffffffffff08880d42ffffffffffffffffffffffffffffffffffffffff,
        0xffffffffffffffffffffffffffffffffffffffffffffffff08f9ffffffffffff,
        0xffff0dbb0d92ffffffffffffffffffffffffffffffffffffffffffffffffffff,
        0x0c99ffffffff0285ffffffffffffffffffffffffffffffffffffffffffffffff,
        0x0972ffffffffffffffffffffffffffffffffffffffffffffffffffffffffffff,
        0x012affffffffffffffffffffffffffffffffffffffffffffffffffffffffffff,
    ),
    (
        0xffffffffffffffff0c07ffffffffffffffffffffffffffffffffffffffffffff,
        0xffffffffffffffffffffffffffffffffffffffffffffffff095affffffffffff,
        0xffff0a24ffffffffffffffffffffffffffffffffffffffffffffffffffffffff,
        0xffffffffffff0c28ffffffffffffffffffffffffffffffffffffffffffffffff,
        0x0dc3ffffffffffffffffffffffffffffffffffffffffffffffffffffffffffff,
        0x033effffffffffffffffffffffffffffffffffffffffffffffffffffffffffff,
    ),
)
SEMAPHORES = (
    (0, 14, 28, 42, 56, 70),
    (1, 15, 29, 43, 56, 71),
    (2, 16, 30, 44, 56, 72),
    (3, 17, 31, 45, 56, 73),
    (4, 18, 32, 46, 56, 74),
    (5, 19, 33, 47, 56, 75),
    (6, 20, 34, 48, 56, 76),
    (7, 21, 35, 49, 56, 77),
    (8, 22, 36, 50, 56, 78),
    (9, 23, 37, 51, 56, 79),
    (10, 24, 38, 52, 56, 80),
    (11, 25, 39, 53, 57, 81),
    (12, 26, 40, 54, 58, 82),
    (13, 27, 41, 55, 59, 83),
    (0, 14, 28, 42, 60, 84),
    (1, 15, 29, 43, 61, 85),
    (2, 16, 30, 44, 62, 86),
    (3, 17, 31, 45, 63, 87),
    (4, 18, 32, 46, 64, 88),
    (5, 19, 33, 47, 65, 89),
    (6, 20, 34, 48, 66, 90),
    (7, 21, 35, 49, 67, 91),
    (8, 22, 36, 50, 68, 92),
    (9, 23, 37, 51, 69, 93),
    (10, 24, 38, 52, 56, 70),
    (11, 25, 39, 53, 57, 71),
    (12, 26, 40, 54, 58, 72),
    (13, 27, 41, 55, 59, 73),
    (0, 14, 28, 42, 60, 74),
    (1, 15, 29, 43, 61, 75),
    (2, 16, 30, 44, 62, 76),
    (3, 17, 31, 45, 63, 77),
    (4, 18, 32, 46, 64, 78),
    (5, 19, 33, 47, 65, 79),
    (6, 20, 34, 48, 66, 80),
    (7, 21, 35, 49, 67, 81),
    (8, 22, 36, 50, 68, 82),
    (9, 23, 37, 51, 69, 83),
    (10, 24, 38, 52, 56, 84),
    (11, 25, 39, 53, 57, 85),
    (12, 26, 40, 54, 58, 86),
    (13, 27, 41, 55, 59, 87),
    (0, 14, 28, 42, 60, 88),
    (1, 15, 29, 43, 61, 89),
    (2, 16, 30, 44, 62, 90),
    (3, 17, 31, 45, 63, 91),
    (4, 18, 32, 46, 64, 92),
    (5, 19, 33, 47, 65, 93),
    (6, 20, 34, 48, 66, 70),
    (7, 21, 35, 49, 67, 71),
    (8, 22, 36, 50, 68, 72),
    (9, 23, 37, 51, 69, 73),
    (10, 24, 38, 52, 56, 74),
    (11, 25, 39, 53, 57, 75),
    (12, 26, 40, 54, 58, 76),
    (13, 27, 41, 55, 59, 77),
    (0, 14, 28, 42, 60, 78),
    (1, 15, 29, 43, 61, 79),
    (2, 16, 30, 44, 62, 80),
    (3, 17, 31, 45, 63, 81),
    (4, 18, 32, 46, 64, 82),
    (5, 19, 33, 47, 65, 83),
    (6, 20, 34, 48, 66, 84),
    (7, 21, 35, 49, 67, 85),
    (8, 22, 36, 50, 68, 86),
    (9, 23, 37, 51, 69, 87),
    (10, 24, 38, 52, 56, 88),
    (11, 25, 39, 53, 57, 89),
    (12, 26, 40, 54, 58, 90),
    (13, 27, 41, 55, 59, 91),
    (0, 14, 28, 42, 60, 92),
    (1, 15, 29, 43, 61, 93),
    (2, 16, 30, 44, 62, 70),
    (3, 17, 31, 45, 63, 71),
    (4, 18, 32, 46, 64, 72),
    (5, 19, 33, 47, 65, 73),
    (6, 20, 34, 48, 66, 74),
    (7, 21, 35, 49, 67, 75),
    (8, 22, 36, 50, 68, 76),
    (9, 23, 37, 51, 69, 77),
    (10, 24, 38, 52, 56, 78),
    (11, 25, 39, 53, 57, 79),
    (12, 26, 40, 54, 58, 80),
    (13, 27, 41, 55, 59, 81),
    (0, 14, 28, 42, 60, 82),
    (1, 15, 29, 43, 61, 83),
    (2, 16, 30, 44, 62, 84),
    (3, 17, 31, 45, 63, 85),
    (4, 18, 32, 46, 64, 86),
    (5, 19, 33, 47, 65, 87),
    (6, 20, 34, 48, 66, 88),
    (7, 21, 35, 49, 67, 89),
)
NEEDS = (
    (
        0xffffffffffffffffffffffffffffffff,
        0xffffffffffffffffffffffffffffffff,
        0xffffffffffffffffffffffffffffffff,
        0xffffffffffffffffffffffffffffffff,
        0xffffffffffffffffffffffffffffffff,
        0xffffffffffffffffffffffffffffffff,
    ),
    (
        0xffffffffffffffffffffffffffffffff,
        0xffffffffffffffffffffffffffffffff,
        0xffffffffffffffffffffffffffffffff,
        0xffffffffffffffffffffffffffffffff,
        0xffffffffffffffffffffffffffffffff,
        0xffffffffffffffffffffffffffffffff,
    ),
    (
        0xffffffffffffffffffffffffffffffff,
        0xffffffffffffffffffffffffffffffff,
        0xffffffffffffffffffffffffffffffff,
        0xffffffffffffffffffffffffffffffff,
        0xffffffffffffffffffffffffffffffff,
        0xffffffffffffffffffffffffffffffff,
    ),
    (
        0xffffffffffffffffffffffffffffffff,
        0xffffffffffffffffffffffffffffffff,
        0xffffffffffffffffffffffffffffffff,
        0xffffffffffffffffffffffffffffffff,
        0xffffffffffffffffffffffffffffffff,
        0xffffffffffffffffffffffffffffffff,
    ),
    (
        0xffffffffffffffffffffffffffffffff,
        0xffffffffffffffffffffffffffffffff,
        0xffffffffffffffffffffffffffffffff,
        0xffffffffffffffffffffffffffffffff,
        0xffffffffffffffffffffffffffffffff,
        0xffffffffffffffffffffffffffffffff,
    ),
    (
        0xffffffffffffffffffffffffff00ffff,
        0xffffffffffffffffffffffffffffffff,
        0xffffff1cff0e0effff0eff1cff0e0e1c,
        0xffffffffffffff0effffff0effffffff,
        0xffffffffffffffffffffffffffffffff,
        0x46464646464646464646464646464646,
    ),
    (
        0xffffffffffffffffffffffff00ffffff,
        0xffffffffffffffffffffffffffffffff,
        0xffffffffffffff1cffff0effffff00ff,
        0xffffffffffffffffffffffffffffff00,
        0xffffffffffffffffffffffffffffffff,
        0x47474747474747474747474747474747,
    ),
    (
        0xffffffffffffffffffffffff010101ff,
        0xffffffffffffffffffffffffffffffff,
        0xffffff1dff0f0f1dffffff1dff0fff1d,
        0xffffffffffffffffffffff0fffffff01,
        0xffffffffffffffffffffffffffffffff,
        0x48484848484848484848484848484848,
    ),
    (
        0xffffffffffffffffffffffffffff0202,
        0xffffffffffffffffffffffffffffffff,
        0xffffff1effff10ffffff10ffff10ffff,
        0xffffffffffffffffffffff10ffffffff,
        0xffffffffffffffffffffffffffffffff,
        0x49494949494949494949494949494949,
    ),
    (
        0xffffffffffffffffffffffffff03ff03,
        0xffffffffffffffffffffffffffffffff,
        0xffffff1fffff11ffffffffffffff0311,
        0xffffffffffffff11ffffffffffffffff,
        0xffffffffffffffffffffffffffffffff,
        0x4a4a4a4a4a4a4a4a4a4a4a4a4a4a4a4a,
    ),
    (
        0xffffffff4b4b4b4b4b4b4b4bffffffff,
        0xffffffffffffffffffffffff4b4b4b4b,
        0x214b4bffffff12ffffff12ffffff12ff,
        0xff2fff4bffffff12ffffff12ffffffff,
        0xffff2f2f132f1313132f13130513132f,
        0xffffffffffffffffffffffffffff04ff,
    ),
    (
        0xff0505054c4c4c4c4c05ffffff05ffff,
        0x2f21ffffffffff2fff21ff2f4c4c4c4c,
        0x224c4cffff13ffffffffffffffffffff,
        0xff30ff4cffff2fffffff2fff132f2f13,
        0xffff30301430ff221430ff2106ff05ff,
        0xffffffffffffffffffffffffffffffff,
    ),
    (
        0x06ff22064d4d4d4d064c4cffffffffff,
        0xff22ffffffff14ffff14ff304d4d4d4d,
        0xff4d4dffffffffffffffffffff14ffff,
        0xffff314dff143014ffff144c143030ff,
        0xff31ff2215ffffff15ff30ffffffff14,
        0xffffffffffffffffffffffffffffffff,
    ),
    (
        0xff07ff314e4e4e4e4d4dffffffffffff,
        0x2323ffffff15ff31ffff15154e4e4e4e,
        0xff4e4effffffffff23154dffffffffff,
        0xffffff4eff3131ffff31314dff151515,
        0xff32ffffffffff23ffffff3116ff31ff,
        0xffffffffffffffffffffffffffffffff,
    ),
    (
        0xffff32ff084f4f4f4eff4effffffffff,
        0x3224ff32ff16243216ffffffff4f4f4f,
        0x24084f24ffffffffff4e16ffffffffff,
        0xffffff16163232ffffff324eff16ffff,
        0xff3333ffffffffff17ffffff09ff16ff,
        0xffffffffffffffffffffffff24ffffff,
    ),
    (
        0xffff09ff0a0a09094fff4fffffffffff,
        0x33ffffffffffffff3333ffff4fff3325,
        0x2518184fffffffffff4f174f17ffffff,
        0x0affff0a33ffffffffff3317ffffffff,
        0xffffff25ffffffffffffffff18ffffff,
        0xff50ffffffffffffffffffffffffffff,
    ),
    (
        0xffffffffffff0a0affffffffffffffff,
        0xffffff5026ffffffffffffffffffffff,
        0xff2626ffff26ff18ffff2618ffffff18,
        0xffffffffffffffffffffffffffff50ff,
        0xffff272627ff18ff3534ffff0aff3434,
        0x50ff50ff50505050505050505050ff50,
    ),
    (
        0xffffffff0b2727ffffff27ffffffffff,
        0xffffff51ffffffffffffffffffffffff,
        0xff1919ffffffffffffffff0bffffffff,
        0xffff5119ffffffffffffffffffffffff,
        0xffff35ff1919ffff1affffff3527ffff,
        0x5151ff35515151515151515151515151,
    ),
    (
        0xffffffffff0c0c0cff0cff0c36ffffff,
        0xffffffffffffffffffffffffffffffff,
        0xff1affff1affffffffffffffffffffff,
        0xffffff1affffffff52ffffffff52ffff,
        0xffff28ff361affff361a28ffffffffff,
        0x5252525252525252ff52525252ff5252,
    ),
    (
        0xffffffff290d0dff37ffffffff37ffff,
        0xffffffffffffffffffffff535329ffff,
        0xff1b1bffffffffffffffff0dffffffff,
        0x0dffff1bffffff1bffff53ffffffffff,
        0xffff29ff371bffffff0dff3737ff37ff,
        0x53535353ff5353535353ffffff535353,
    ),
    (
        0xffffffff2affff00ffffffffffffffff,
        0xffffff54ff5454ffff54ffffffffffff,
        0xff1cffffff1cffffffffffffffffffff,
        0xff0eff0effff00ffffff545454ff54ff,
        0x2b1dffff0eff1cff0e1cffff2a00ffff,
        0x545454ff54ffff5454ffffffff54ff54,
    ),
    (
        0xffffffffff01ffffff01ffffffffffff,
        0xffffffffffffffffff55ffff1dff55ff,
        0xff55ff55ffffffffffffffff55ffffff,
        0xffffffffffffffffffffff55ffff2bff,
        0x1d2bff1d0f0f1dff01ff01ffffffffff,
        0x55ff55ff5555555555ff55ffff55ff55,
    ),
    (
        0xffffff5656565656ff56562cffffffff,
        0xffff2cffff2cffffffffffff56561056,
        0xff10561effffffff1e10ff1effffff10,
        0xffffffffffffffffffff1056ff0256ff,
        0xffffffff10ff2c2c2cffffffffff2cff,
        0xff56ffffffffffffffffffffffffffff,
    ),
    (
        0xffff2d03ff5757ffff03ffffffffffff,
        0x1fffffffffffff11ffffffff57575757,
        0xff57ffffff111157ffffffffffff11ff,
        0xffff57ffffffffff1111115711ffff11,
        0x032dffffffffffffffff1f11ff0303ff,
        0xffffffffffffffffffffffffffffffff,
    ),
    (
        0xffffffffffffff58ff5858ff04ffffff,
        0xffffffffffffffffff12ffff2eff5858,
        0x20ff5858ffff5812ffffff58ffffffff,
        0xff2effffffffff2effff1212ffff12ff,
        0xffff20ff12ffffff122eff2e122effff,
        0xffffffffffffffff58ffffffff5820ff,
    ),
    (
        0x21ffff05ffffffffffffffffffffffff,
        0xffffffff21ff21ffff132fffff5959ff,
        0xff5959ffff131313ff59ffff21ffff59,
        0xffff2f592f052f5905ffff13ffffff05,
        0x0513ff2fffffffffff2f13ffffff2f13,
        0xffffffff59ffffffffff59595921ffff,
    ),
    (
        0xff30ffffffffffffffffffff22ffff30,
        0x14ffff14ff30ffffffffff14ff5aff5a,
        0xffff5affffffffffffff5affffffffff,
        0x30ffffffffffff5affffff5affff5aff,
        0xffff30ff22ffffff0614ff2214ffff22,
        0xffffff5aff5a5affff5affff5affffff,
    ),
    (
        0xffffffff5bffffffff5b5bffffffffff,
        0xff15ff15ffffffffffff15ffff5bff5b,
        0xffffffff07ffffffffffffffffffffff,
        0xff5bffffffffff5b3115ffffff15ff15,
        0x1523ff23ffffffffffff23ffffffffff,
        0xffff155bffffffffffffff5b5bff5bff,
    ),
    (
        0xff32ff5cff08ffffffffffffffffffff,
        0xffffffffffffff32ffffffffffffffff,
        0x08ffffffffffff5cffffffffffffff5c,
        0x16ff3216ffff5cffffffffff5cff5cff,
        0xffffff32ffff32ff24ffffffffff2408,
        0x5cff5cff5c5cffffffff085cff5cffff,
    ),
    (
        0xffffffff09ffffffffff5dffffffffff,
        0xffffffff5dff5dff5d5dffffffffff5d,
        0xff1717ffffffff09ffffffffff255dff,
        0x17ffff5dffffff5dff09ffff5d33ff17,
        0xffff09ff25ffffffffff331725ffffff,
        0x5d5d5dffff5dff33ffffff5dffffffff,
    ),
    (
        0xff0affffff0affffff26ffffffffffff,
        0x18ff46ffffffffffffff46ffff46ff46,
        0xff26180affffffffffffffffff26ffff,
        0xffffffffff18ffff18ff18ffffffffff,
        0x0affffffffff2626ffff26ffffffffff,
        0x34ffff4646ff46ffffffffffffffffff,
    ),
    (
        0xff47ffff47ff0bffffff470bffffffff,
        0xffff47ffffffffff47ffffff474727ff,
        0xff0bffffffffff0bff19ffffffffffff,
        0x19ffffffff47ffffffffff47ffff35ff,
        0xffffff3527ffffff19ffffffffffffff,
        0x47ffffffffffffffffffffffffffff47,
    ),
    (
        0xff0cffffffff48ff36ffffffffffffff,
        0x36ffff1affffff48ffffffffffffffff,
        0xffffffffffffffffff2828ffffffffff,
        0xffffff48ffffff1aff1a1aff36ff48ff,
        0x0cffff3636ffffffffffffffffff1aff,
        0x1aff48ffffffffffffff0cffff48ff48,
    ),
    (
        0xffffff3729ffffff49ffffffffffff29,
        0xff2949ffffffffff37ffffffffffff49,
        0xffffff1bffffff1bff0d0dffffffffff,
        0x0dffffffffffffffffffff49ff49ffff,
        0x29ffffffffffffffff37ff37ffff3737,
        0x1bff1bffff29ff49ffffffffffffffff,
    ),
    (
        0xffffffffffffffffffffffffffffffff,
        0xffffffffff2affffffffffff4affffff,
        0xffffffffff4a4affffffffffff1cffff,
        0xffffff00ffffff00ffffff00ff0eff4a,
        0xff00ffff1cffffffffffff2affffffff,
        0xff4a0e4a00ffffffff4affffffff4aff,
    ),
    (
        0xff1dffffff4bffffffffffffffffff4b,
        0x1dffffffffffffffffff1dffffffffff,
        0xffffffffffffffff1dffffffffffffff,
        0xffffff4b01ffffff2b2bff4bffffffff,
        0xffffffffffffffffffffffffffffffff,
        0xffffff0fff01ff01ffff01ff4b4bffff,
    ),
    (
        0xffffffffff1effffffff2cffffffff4c,
        0xff1effffffffffffffffff10ff4cffff,
        0xffffff4cffff4cffffffffffffffffff,
        0xffffffff02ffffff2cffff4cffffffff,
        0xffffff1effffffffffffffffffffffff,
        0xff4cff102cffffffff1e4cff4cff4cff,
    ),
    (
        0xff03ffffff4dff4dffffff032dff1fff,
        0xffff114dffffffffffffff4dffff4dff,
        0xffffffffff1103ffffffffffffffffff,
        0x11ffffffffffff11ffffffffffffff4d,
        0xff1f1fff1fff2dffffffffffffffffff,
        0xff11ff03ffffffff03ffffffffffff2d,
    ),
    (
        0xffffffffffffffffffffff4e2eff4eff,
        0xffffffffffffffffffffffffff4effff,
        0xffffffffffffff4effff4effff20ffff,
        0xff12ff12ffffffff2e0404ffffffff4e,
        0xffffffffff12ffff20202effffffffff,
        0xff2e12ffffffffffffffff04ffffffff,
    ),
    (
        0xffffffffffffffffffffffffffffffff,
        0xffff4fffffff4fffffffffffffffffff,
        0xffffffffff4fff13ffffff13ffffffff,
        0xffffffff0505ffffffffffffff4fffff,
        0xffffffffff21ffffffffffffffffffff,
        0xff21ffffffffffffffffffffffffff13,
    ),
    (
        0xffffffffffffffffff50ffffffff50ff,
        0xffffffffffffffffffffffffffffffff,
        0xffffffffffffffffffff06ffffffffff,
        0xffffffffffffffff30ffffffffffff50,
        0xffffffffffffffff14ffffffffffffff,
        0xffff1414ffffffff06ff22063022ffff,
    ),
    (
        0xffff07ff07ff51ffffffffffffffffff,
        0xffffffffffffffffff31ffffffffffff,
        0xffff51ffffffffffff07ffffff5151ff,
        0x1515ffffffffff07ffffffffffffffff,
        0xffffff31ff23ffff3115ffffffffffff,
        0x23ff23ffff3115ffffffffffffffffff,
    ),
    (
        0xff24ffffffffffffffffffffff52ffff,
        0xffff16ffffffffffffffffffff2416ff,
        0xffff24ffffffffffffffffffffffffff,
        0xffffffffffffff08ffffffffffffff16,
        0xffffffffff16ffffffffffffff16ffff,
        0xff16ffff16ffff1608ff08ff24ffffff,
    ),
    (
        0xffffffffffffffffffffffffffffffff,
        0x33ffffffffffffffffffffffff25ffff,
        0xffffffffffffffffffffffffffffffff,
        0x53ffffffffffffffffffffff33ffffff,
        0xffff2533ffffff25ffffffffffffffff,
        0xff1709ffffffffff09ff25ffffffffff,
    ),
    (
        0xffffffffffffffffffffffffffffffff,
        0xffffffffffffffffffff18ff34ff54ff,
        0xffffffffffffffffffffffffffffffff,
        0xffffffffffffffffffffffffffffffff,
        0xffffffffffffffffffffffffffffff34,
        0xffffffffffffff34ffffffff26ffff18,
    ),
    (
        0xffffffffffffffffffffffffffffffff,
        0xffff35ffffffffffffffffffffffffff,
        0xffffffffffffffffffffffffffffffff,
        0xffffffffffffffffffffffffffffffff,
        0xffffff27ffffffffffffffffff0bffff,
        0xff19ff0bffffffffff0bffffffffffff,
    ),
    (
        0x0cffffffffffffffffffffffffffffff,
        0xffffffff56ffffffffffffffffffffff,
        0xff0cffff0cffffffffffffffffffffff,
        0xffffffffffffffffffff1affffffffff,
        0xffffffffffffff2836ffffffffffffff,
        0xffff1affff28ffffffff28ffffffff1a,
    ),
    (
        0xffffffffffffff29ffffffffffffffff,
        0xffffffffffffffffffff37ffffffffff,
        0xffffffffffffffffffff5729ffffffff,
        0xffff0dffffffffffffffffffffffffff,
        0xffffffffffffffffffffffffffffffff,
        0xffffffffffffffffffffffffffffffff,
    ),
    (
        0xffffffffffffffffffffff1cffffffff,
        0xffffffff1cffffffffffff3cffffffff,
        0x58ffffffffffffffffffffffffffffff,
        0xffffffffffffffffffffffffffffffff,
        0xffff2affffffffffffffffffffffffff,
        0xffffffffffffff1cffffffffffffffff,
    ),
    (
        0xffffffffffffffffffffffffffffffff,
        0xffffffff1dffffffffffffffffffffff,
        0xffffffffffffffffff0fffffffffffff,
        0xffffffffffffffffffffffffffffffff,
        0xffffffffffffff0fffffffffffffffff,
        0xffffffffffffffffffffffffffffffff,
    ),
    (
        0xffffffff5affffffffffffffffffffff,
        0xffffffffff10ffffffffffffffff1eff,
        0xffffffffffffffffffffffffffffffff,
        0xffffffffffffff5affffffffffffffff,
        0xffffffffffff2cffffffffffffffffff,
        0xffffff02ffffffffffffffff102cffff,
    ),
    (
        0x2dffffff03ff2dffffff2d03ffff5bff,
        0xffffffff2dffffffffffffff1f2dffff,
        0xffffffffffffffffffffffffffffffff,
        0xffffffffffffffffffffffffffffffff,
        0xffffffffffffffffffffffffffffff03,
        0xffffffffffffffffffffff2dffffffff,
    ),
    (
        0xffffff40ffffffffffffffffffffffff,
        0xffffffffffffffffffffffffffffffff,
        0xff04ffff12ffffffffffffffffffffff,
        0xffffffffffffffffffffffffffffffff,
        0xffffffffffffffffffffff20ff202eff,
        0xffffffffff04ffff2effffffffffffff,
    ),
    (
        0xffffffffffffffffffffffffff2fffff,
        0xffffffffffffffffffffffffffffffff,
        0xffffffff5dffffffffffffffffffffff,
        0xffffffffffffffffffffffffffffffff,
        0xffff2fffffffffffff0521ffffffffff,
        0xffff13ffffffffff21ffffffffffffff,
    ),
    (
        0xffffffffffffffffffffffffffffffff,
        0xffffffffffffffffffffffffffffffff,
        0xffff14ffffffffffffffffffffffffff,
        0xffffffffffffffffffffffffffffffff,
        0xffff06ffffffffffffffffffffffffff,
        0x06ffffffffffffffff30ffffffffffff,
    ),
    (
        0xffffffff31ffffffffffffffffffffff,
        0xffffffffffffffffffffffffffffffff,
        0xffffff15ffffffff15ffffffffffffff,
        0xffffffffffffffffffffffffffffffff,
        0x31ffffffffffffff07ffffffff15ffff,
        0xffffffffffff3115ffff23ffffffffff,
    ),
    (
        0xffffffffffffff08ffffffffffffffff,
        0xffffffffffffffffffffffffffffffff,
        0xffff24ffff16ffffffffffff44ffffff,
        0xffffffffffffffffffffffffffffffff,
        0xffffffffffffff16ffffffffffffffff,
        0xffffffffffffffffffffffffffffffff,
    ),
    (
        0xffffffffffffff49ff25ff25ffffffff,
        0xffff25ffffffffffffffffffffffffff,
        0x17ffffffffffffffffff09ffffffffff,
        0xffffffffffffffffffffffffffffffff,
        0xffffffffffffffff33ffffffffffffff,
        0xffffff09ffff09ffffffffffff33ffff,
    ),
    (
        0xffffffffffffffffffffffffffffffff,
        0xffffffffffffffff34ff26ffffffffff,
        0xffffffffffffffffffffffffffffffff,
        0xffffff0affffffffffff18ffffffffff,
        0xffffff34ffffffff26ffffffffffffff,
        0xffffffffffffffffffffffffffffffff,
    ),
    (
        0xffffffffffffff4bffffffffffffffff,
        0xffffffffffffff27ffffffffffffffff,
        0xff0bffffffffffffffffffffffffffff,
        0xffffffff0bffffffffffff4bffffff0b,
        0xffffffff2719ffffffffffffffffffff,
        0xff35ffffffff19ffffffffff35ffffff,
    ),
    (
        0xffffffffffffff4cffffffff28ffffff,
        0xffffffffffffffffff1affffffffff36,
        0xffffffff4cffffffffffffffffffffff,
        0xffffffffffffffffffffffffffffffff,
        0xffffffffffffffffffffffffffffffff,
        0xffffffffffffffffffffffffffffffff,
    ),
    (
        0xffffffffffffffffffff29ffffffff0d,
        0xffffffffffffffffffffffffffff4dff,
        0xffffffffffffffffffffffffffffff1b,
        0xffffffffffffffffffffffffffff1bff,
        0x29ffffff1cffffffffffffff37ffffff,
        0xffffffffffffffffffffffffffffffff,
    ),
    (
        0xffffffffffffffffffffff4effffffff,
        0xffffffffffffffffffffffffff1cffff,
        0xffffffffffffffffffffffffffffffff,
        0xffffffffffffff2affffffffffffffff,
        0xffffffffffffffffffffffffffffffff,
        0xffffffffffffffffffffffffffffffff,
    ),
    (
        0xffffffff1dffffffffffffffffffff4f,
        0xffffffffffffffffffffffffffffffff,
        0xffff3d4fffffffffffffffffffffffff,
        0xffffffffffffffffffffffffffffffff,
        0xffffffffffff0fffff1dff1dffffffff,
        0xffff1dffffffffffffffffffffffffff,
    ),
    (
        0xffffffffffff2cffffffffffffffffff,
        0xffffffffffffffffffffffffff2cffff,
        0xffffffffffffffffffffffffff02ffff,
        0xffffffffffff5050ffffffffffffffff,
        0xffffffff2cffffffffffffff02ffffff,
        0xff1effffffffffffffffffff2cffffff,
    ),
    (
        0xffffffffffffffffffffff1fffffffff,
        0xffffffffffffffffffffffffffff51ff,
        0xffffffffffffffff11ffffff3fffffff,
        0xffff51ff03ff2d2dffffffffffffffff,
        0x1fffff03ffffffffffffffffffffffff,
        0x11ffffffffffffffffffff2dffffffff,
    ),
    (
        0xff40ffffffffffffffffffffffffffff,
        0xffffffffffffffffffffffffffffffff,
        0xffffffffffffffffffffffffffffffff,
        0xffffffffffffffffff04ffffffffffff,
        0xffffffff20ffffffffffffffff12ffff,
        0xff12ffffffffffffffffffffffffffff,
    ),
    (
        0xffff41ff05ffffffffffffffffffffff,
        0xffffffffffffffffffffffffffffffff,
        0xffffffffffffffffffffffffffffffff,
        0xffffffffffffffffffffffffffffffff,
        0xffffffffffff05ffffffff21ffffffff,
        0xffffffffffffffffffffffffffffffff,
    ),
    (
        0xffffffffffffffffffffffffffffffff,
        0xffffffff30ffffffffff42ffffffffff,
        0xffffffff42ffffff54ffffffffffffff,
        0xffffffffffffffffffffffffffffffff,
        0x22ffffffffffffffff22ffff30ffffff,
        0xffffffffffffffffff06ff22ff22ffff,
    ),
    (
        0xffffffffffffffffffffffffffffffff,
        0xffffffffffffffffffffffffffff15ff,
        0xffffffffffffffffffffffff43ffff55,
        0xffffffff07ffffffffffffffffffffff,
        0xffffffffffffff07ffffffff0707ffff,
        0xffffffffffffffffffffffffffffffff,
    ),
    (
        0xffffffffffffffffffffffffffffffff,
        0xffffffffffffffffffffffff32ffffff,
        0xffffffffffffffff08ffffffffffffff,
        0xffffffffffffffffffffffffffffffff,
        0x08ffffffffffffffff16ffffffffff32,
        0xffffffffffffffffffffffffffffffff,
    ),
    (
        0xffffffffffffffffffffffffffff45ff,
        0xffffffffffffffffffffffffffffffff,
        0xffffffffffffffffffff25ffffffffff,
        0xffffff17ffffffffffffffffffffffff,
        0xff17ffffffff25ffffffffffffffffff,
        0xffffffffffffffffffffffffffffffff,
    ),
    (
        0xffffffffffffffffffffffffffffffff,
        0xffffffffffffffffffffffffffffffff,
        0xff58ffffffff0affffffffffffffffff,
        0xffffffffffffffff18ffffffffffffff,
        0xff34ffffffffffffffffffffffffffff,
        0xffffffffffffffffffffffffffffffff,
    ),
    (
        0xffffffffffffffffffffffffffffffff,
        0xffffffffffffffffffffffffffffffff,
        0xffffffffffffffffffffffffffff27ff,
        0xffffffffffffffffffffffffffffffff,
        0x0bffffffff35ffffffffffffffffffff,
        0xffffffffffffffffffffffff35ffffff,
    ),
    (
        0xffffffffffffffffffffffffffffffff,
        0xffffffffffffffffffffffffffffffff,
        0xffffffffffffffffffffffffffffffff,
        0xffffffffffffffffffffffff1affffff,
        0xffffff36ffffffffffffffffffffff0c,
        0x1affffffff1affffffffffffffffffff,
    ),
    (
        0xffffffffffffffffffffffffffffffff,
        0xffffffffffffffffffffffffffffffff,
        0xffffffffffffffffffffffffffffffff,
        0xffffffff37ffffffffffffffffffffff,
        0xffffffffffffffffffffffffffffffff,
        0xffffffffffffffffffffffffffffffff,
    ),
    (
        0xffffffffffffffffffffffffffffffff,
        0xffffffffffffffffffffffffffffffff,
        0xffffffffffffffffffffffff1cffffff,
        0xffffffffffffffffffffffffffffffff,
        0xff2affffff0effffffffffffffffffff,
        0xffffffffffffffffffffffffffffffff,
    ),
    (
        0xffffffffffffffffffff5dffffffffff,
        0xffffffffffffffffffffffffffffffff,
        0xffffffffffffffffffffffffffffff3d,
        0xffffffffffffffffffffffffffffffff,
        0xffffffffffffffffffffffffffffffff,
        0xffffffffffffffffffffffffffffffff,
    ),
    (
        0xffffffffffffffffffffffffffffffff,
        0xffffffffffffffffffffffffffffffff,
        0xffffffffffffffffffffffffffffffff,
        0xffffffffffffffffffffffffffffffff,
        0xffffffffff02ffffffffffffffffffff,
        0xffffffffffffffffffffffffffffffff,
    ),
    (
        0xffffffffffffffffffffffffffffffff,
        0xffffffffffffffffffffffffffffffff,
        0xffffffffffffffffffffffffffffffff,
        0xffffffffffffffffffffffffffffffff,
        0xffffffffffffffffffffffffffffffff,
        0xffffffffffffffffffffffffffffffff,
    ),
    (
        0xffffffffffffffffffffffffffffffff,
        0xffffffffffffffffffffffffffffffff,
        0xffffffffffffffffffffffffffffffff,
        0xffffffffffffffffffffffffffffffff,
        0xffffffffffffffffffffffffffffffff,
        0xffffffffffffffffffffffffffffffff,
    ),
    (
        0xffffffffffffffffffffffffffffffff,
        0xffffffffffffffffffffffffffffffff,
        0xffffffffffffff13ffffffffffffffff,
        0xffffffffffffffffffffffffffffffff,
        0xffffffffffffffffffffffffffffffff,
        0xffffffffffffffffffffffffffffffff,
    ),
    (
        0xffffffffffffffffffffffffffffffff,
        0xffffffffffffffffffffffffffffffff,
        0xffffffffffffffffffffffffffffffff,
        0xffffffffffffffffffffffffffffffff,
        0xffffffffffffffffffffffffffffffff,
        0xffffffffffffffffffffffffffffffff,
    ),
    (
        0xffffffffffffffffffffffffffffffff,
        0xffffffffffffffffffffffffffffffff,
        0xff23ffffffffffffffffffffffffffff,
        0xffffffffffffffffffffffffffffffff,
        0xffffffffffffffffffffffffffffffff,
        0xffffffffffffffffffffffffffffffff,
    ),
    (
        0xffffffffffffffffffffffffffffffff,
        0xffffffffffffffffffffffffffffffff,
        0xffffffffffffffffffffffffffffffff,
        0xffffffffffffffffffffffffffffffff,
        0xffffffffffffffffffffffffffffffff,
        0xffffffffffffffffffffffffffffffff,
    ),
    (
        0xffffffffffffffffffffffffffffffff,
        0xffffffffffffffffffffffffffffffff,
        0xffffffffffffffffffffffffffffffff,
        0xffffffffffffffffffffffffffffffff,
        0xffffffffffffffffffffffffffffffff,
        0xffffffffffffffffffffffffffffffff,
    ),
    (
        0xffffffffffffffffffffffffffffffff,
        0xffffffffffffffffffffffffffffffff,
        0xffffffffffffffffffffffffffffffff,
        0xffffffffffffffffffffffffffffffff,
        0xffffffffffffffffffffffffffffffff,
        0xffffffffffffffffffffffffffffffff,
    ),
    (
        0xffffffffffffffffffffffffffffffff,
        0xffffffffffffffffffffffffffffffff,
        0xffffffffffffffffffffffffffffffff,
        0xffffffffffffffffffffffffffffffff,
        0xffffffffffffffffffffffffffffffff,
        0xffffffffffffffffffffffffffffffff,
    ),
    (
        0xffffffffffffffffffffffffffffffff,
        0xffffffffffffffffffffffffffffffff,
        0xffffffffffffffffffffffffffffffff,
        0xffffffffffffffffffffffffffffffff,
        0xffffffffffffffffffffffffffffffff,
        0xffffffffffffffffffffffffffffffff,
    ),
    (
        0xffffffffffffffffffffffffffffffff,
        0xffffffffffffffffffffffffffffffff,
        0xffffffffffffffffffffffffffffffff,
        0xffffffffffffffffffffffffffffffff,
        0xffffffffffffffffffffffffffffffff,
        0xffffffffffffffffffffffffffffffff,
    ),
    (
        0xffffffffffffffffffffffffffffffff,
        0xffffffffffffffffffffffffffffffff,
        0xffffffffffffffffffffffffffffffff,
        0xffffffffffffffffffffffffffffffff,
        0xffffffffffffffffffffffffffffffff,
        0xffffffffffffffffffffffffffffffff,
    ),
    (
        0xffffffffffffffffffffffffffffffff,
        0xffffffffffffffffffffffffffffffff,
        0xffffffffffffffffffffffffffffffff,
        0xffffffffffffffffffffffffffffffff,
        0xffffffffffffffffffffffffffffffff,
        0xffffffffffffffffffffffffffffffff,
    ),
)
LATE = (
    (0x0000, 0x0889, 0x0000, 0x7777, 0x0000, 0x0000),
    (0x0000, 0x09eb, 0x0000, 0x7777, 0x0000, 0x0000),
    (0x000c, 0x0dcb, 0x0111, 0x7777, 0x0000, 0x0000),
    (0x0008, 0x0cfe, 0x0111, 0x7777, 0x0000, 0x0000),
    (0x000d, 0x0ccd, 0x1111, 0x7777, 0x0000, 0x0000),
    (0x8fb1, 0xf040, 0x3faf, 0x0888, 0x0000, 0x8000),
    (0x6f77, 0xf012, 0x0eff, 0x8989, 0x0000, 0x8000),
    (0xbfff, 0xf308, 0x3e7f, 0x888d, 0x0000, 0x8000),
    (0xb7ff, 0xe351, 0x2df7, 0x08df, 0x0000, 0x8000),
    (0xdcf7, 0xff47, 0x6ffe, 0x171d, 0x0000, 0xc800),
    (0x60f7, 0x9ce6, 0x83df, 0xffbc, 0x7fff, 0x0000),
    (0xf7ef, 0x83ff, 0xd1db, 0xcf77, 0x3fff, 0x0000),
    (0xf8af, 0xa33f, 0xdfdf, 0xf777, 0x7fff, 0x0000),
    (0x79af, 0x8aff, 0xd7fb, 0xf761, 0x577f, 0x0800),
    (0xfcfb, 0xa77f, 0xb9bf, 0xf7f7, 0x77ff, 0x0000),
    (0xfb1f, 0xf3ff, 0x2df7, 0x3ffd, 0x177f, 0x0000),
    (0xfffb, 0xb79c, 0xef6f, 0xd86d, 0x3fff, 0x8080),
    (0x6fb9, 0xf804, 0x7fdf, 0x9fff, 0x3fff, 0x98e0),
    (0xfff7, 0xf605, 0x5ffd, 0xbea3, 0x3fff, 0xcc08),
    (0x6b7e, 0xb88e, 0x75f3, 0xc59d, 0x3fff, 0x8680),
    (0xff7f, 0x6fa7, 0xf7e6, 0x1bfe, 0xffff, 0xc880),
    (0xf7ff, 0x0f9a, 0xafdf, 0xff7f, 0xffff, 0xa680),
    (0x7bde, 0x6fff, 0xff7d, 0x8cff, 0xffff, 0x40e0),
    (0xd6bf, 0x1fee, 0xf7f3, 0xfedb, 0xffff, 0x0004),
    (0x2bff, 0x5b5f, 0xbc9b, 0x7fff, 0xffff, 0xc5da),
    (0xbcef, 0x7f3f, 0xf7fd, 0xeffd, 0xffff, 0x1342),
    (0x3fdf, 0x6e9d, 0xff9f, 0x6777, 0xffff, 0xccf8),
    (0x7f9f, 0x4eff, 0x33fe, 0xef2c, 0xffff, 0xde6a),
    (0xa6ef, 0xdffb, 0xf7fb, 0xfbef, 0xffff, 0xa9b4),
    (0xf2df, 0xefff, 0x3f5f, 0xff3f, 0xffff, 0xebe2),
    (0xf7ff, 0xefef, 0xabbf, 0xf75f, 0xffff, 0xadc0),
    (0xad6f, 0x1aff, 0x97fd, 0xfdf6, 0xffff, 0xeaec),
    (0xff8f, 0x8bff, 0xff3b, 0xbf57, 0xffff, 0xfec8),
    (0xf3ff, 0xfeee, 0xbbff, 0xffff, 0xffff, 0xd9fb),
    (0xff4f, 0xcf7f, 0xffdb, 0xff77, 0xffff, 0xffbc),
    (0xd6bf, 0x3dbf, 0x5bff, 0xeb3f, 0xffff, 0xddf9),
    (0xfe5f, 0x92f8, 0x9ff3, 0xffff, 0xffff, 0xfffb),
    (0xdf7f, 0xbfff, 0xdedb, 0x6ff7, 0xffff, 0x7fff),
    (0xffff, 0xffde, 0xfff7, 0xfef6, 0xffff, 0xfffd),
    (0xefbb, 0xbfff, 0xefff, 0xdfff, 0xffff, 0xffff),
    (0x37ff, 0xdfde, 0xfadf, 0xff7f, 0xffff, 0xf7ff),
    (0xdfff, 0xffff, 0xfeef, 0xffdf, 0xffff, 0xffdf),
    (0xffff, 0xffff, 0xf6ef, 0xdfff, 0xffef, 0x7fff),
    (0xffff, 0xfebf, 0xf7ff, 0xffff, 0xffff, 0xffff),
    (0xefff, 0xfbf7, 0xfffd, 0xfdfb, 0xffff, 0xf6ff),
    (0xf7ee, 0xffff, 0xfff7, 0x75cb, 0xffff, 0xfffd),
    (0xbbff, 0xf7ff, 0xffeb, 0xff7d, 0xefff, 0xffff),
    (0xffbf, 0xdfff, 0xff5f, 0xdffb, 0xffff, 0xf7ff),
    (0x5fff, 0xdfff, 0xffff, 0xffbf, 0xffff, 0xffff),
    (0xff7f, 0xee7b, 0xffdf, 0x75ff, 0xffff, 0xffff),
    (0xfeff, 0xfaff, 0xdfff, 0xffff, 0xfff7, 0xffff),
    (0xeddf, 0x7fff, 0xdfaf, 0xff7b, 0xffff, 0xfeff),
    (0xefff, 0xffdf, 0xff5f, 0xef7f, 0xffff, 0xffff),
    (0xb7fe, 0xf9ff, 0xf6ff, 0xbff7, 0xffff, 0xfeef),
    (0xffff, 0xffbf, 0xfff7, 0xfffe, 0xffff, 0xf6ff),
    (0xfffe, 0xfffc, 0x7fdf, 0xfff7, 0xffff, 0xfffd),
    (0xffff, 0xffff, 0xf7fb, 0xfeff, 0xffff, 0xffef),
    (0xffff, 0xfdff, 0xd7af, 0xffff, 0xdfff, 0xeffe),
    (0xfff3, 0xffff, 0xbfff, 0xf5f3, 0xffff, 0xfcff),
    (0xe7ff, 0x7f7f, 0x7fef, 0xfcef, 0xfff7, 0xdffd),
    (0xffbf, 0xbffb, 0xf7ff, 0xffff, 0xbfff, 0xffff),
    (0xf5ff, 0xffff, 0xffef, 0xffff, 0xdfff, 0xffff),
    (0xffbf, 0xffff, 0x7fab, 0xf7f7, 0xf7df, 0xff7f),
    (0xf6f3, 0xfffd, 0xffff, 0xffff, 0xfff7, 0xfffe),
    (0x7f7f, 0xffbf, 0xffff, 0xfff6, 0xffff, 0xffff),
    (0xffff, 0xafff, 0xfddf, 0xffff, 0xfffd, 0xffff),
    (0xfdff, 0xff7f, 0xffff, 0xbfff, 0xffff, 0xbfff),
    (0x7fff, 0xffff, 0xfffd, 0xfbf7, 0xffff, 0xffff),
    (0xfffe, 0x7bf7, 0xffff, 0xefff, 0xffff, 0xffff),
    (0xffff, 0xffff, 0xffff, 0xf7ff, 0xffff, 0xffff),
    (0xffff, 0xfbff, 0xfff7, 0xbfff, 0xffff, 0xffff),
    (0xffff, 0xffff, 0xffff, 0xffff, 0xfffe, 0xffdf),
    (0xfbff, 0xffff, 0xffff, 0xffff, 0xffff, 0xffff),
    (0xffff, 0xffff, 0xffff, 0xffff, 0xffff, 0xffff),
    (0xffff, 0xffff, 0xffff, 0xffff, 0xffff, 0xffff),
    (0xffff, 0xfeff, 0xffff, 0xffff, 0xffff, 0xffff),
    (0xffff, 0xffff, 0xffff, 0xffff, 0xffff, 0xffff),
    (0xffff, 0xffff, 0xbfff, 0xffff, 0xffff, 0xffff),
    (0xffff, 0xffff, 0xffff, 0xffff, 0xffff, 0xffff),
    (0xffff, 0xffff, 0xffff, 0xffff, 0xffff, 0xffff),
    (0xffff, 0xffff, 0xffff, 0xffff, 0xffff, 0xffff),
    (0xffff, 0xffff, 0xffff, 0xffff, 0xffff, 0xffff),
    (0xffff, 0xffff, 0xffff, 0xffff, 0xffff, 0xffff),
    (0xffff, 0xffff, 0xffff, 0xffff, 0xffff, 0xffff),
    (0xffff, 0xffff, 0xffff, 0xffff, 0xffff, 0xffff),
    (0xffff, 0xffff, 0xffff, 0xffff, 0xffff, 0xffff),
    (0xffff, 0xffff, 0xffff, 0xffff, 0xffff, 0xffff),
    (0xfffe, 0xfffe, 0xfffe, 0xfffe, 0xfffe, 0xfee8),
    (0xfee8, 0xfee8, 0xfee8, 0xfee8, 0xe880, 0xe880),
    (0xe880, 0xe880, 0xe880, 0xe880, 0xe880, 0xc800),
    (0xc000, 0x8000, 0xc000, 0xc000, 0x8000, 0x8000),
    (0x8000, 0x8000, 0x8000, 0x8000, 0x8000, 0x8000),
)
LATE_BY = 7
NO_WAIT = 0xFF
GAIN_STEP = 4
SLOTS = 33
UNITS = 129
UNIT = 16
LANES = 128
STARTS = (0, 8, 16, 24, 32, 40, 48, 56, 64, 72, 80, 88, 96, 104, 112, 120)
OPPOSITE = (1, 0, 3, 2, 5, 4)
ORDER = (5, 3, 1, 2, 0, 4)
SENDS = 6
NOTHING = 0xFFFF


SIZES = dict(zip(STARTS, (b - a for a, b in zip(STARTS, STARTS[1:] + (UNITS,)))))


def size_of(entry):
    return 0 if entry == NOTHING else SIZES[entry % UNITS]


def neighbour_position(p, d):
    x, y = divmod(p, 4)
    if d == 0:
        x = (x + 1) % 4
    if d == 1:
        x = (x + 3) % 4
    if d == 2:
        y = (y + 1) % 4
    if d == 3:
        y = (y + 3) % 4
    return 4 * x + y


def signed(word):
    return word - (1 << 32) if word >= 1 << 31 else word


def entries(step, d):
    return [(PLAN[step][d] >> (16 * p)) & 0xFFFF for p in range(16)]


def mask_of(flags):
    return sum(1 << p for p, flag in enumerate(flags) if flag)


def gather_kernel(re_ref, im_ref, held, part, part_in, send_sem, recv_sem, load_sem, pair_sem):
    bins = re_ref.shape[0]
    tiles = re_ref.shape[1]
    fr = lax.axis_index("fr")
    sr = lax.axis_index("sr")
    sc = lax.axis_index("sc")
    z, x, y = sr // 4, sr % 4, sc
    p = 4 * x + y
    steps = len(PLAN)

    xp, xm = (x + 1) % 4, (x + 3) % 4
    yp, ym = (y + 1) % 4, (y + 3) % 4
    zp, zm = (z + 1) % 4, (z + 3) % 4
    targets = (
        (fr, 4 * z + xp, y),
        (fr, 4 * z + xm, y),
        (fr, sr, yp),
        (fr, sr, ym),
        (fr, 4 * zp + x, y),
        (fr, 4 * zm + x, y),
    )
    ahead = (4 * (xp - x), 4 * (xm - x), yp - y, ym - y, 16, -16)
    twin = (1 - fr, sr, sc)
    shift = 16 * (y % 2)

    barrier = pltpu.get_barrier_semaphore()
    for device in targets + (twin,):
        pl.semaphore_signal(barrier, inc=1, device_id=device, device_id_type=MESH)
    loads = []
    for f in range(bins):
        for half in range(2):
            for i, ref in enumerate((re_ref, im_ref)):
                place = 4 * f + 2 * half + i
                source = ref.at[f, :, :, pl.ds(half * LANES, LANES)]
                target = held.at[pl.ds(place * tiles, tiles)]
                loads.append(pltpu.make_async_copy(source, target, load_sem.at[0]))
    for load in loads:
        load.start()

    everything = held.at[pl.ds(0, UNITS - 1)]
    pltpu.make_async_copy(everything, everything, load_sem.at[0]).wait()
    pl.semaphore_wait(barrier, 7)

    def chosen(step, d):
        words = [jnp.int32(signed((PLAN[step][d] >> (32 * i)) & 0xFFFFFFFF)) for i in range(8)]
        words = [jnp.where(y < 2, words[i], words[i + 1]) for i in range(0, 8, 2)]
        word = jnp.where(
            x < 2,
            jnp.where(x == 0, words[0], words[1]),
            jnp.where(x == 2, words[2], words[3]),
        )
        return lax.shift_right_logical(word, shift) & 0xFFFF

    def needed(step, d):
        words = [jnp.int32(signed((NEEDS[step][d] >> (32 * i)) & 0xFFFFFFFF)) for i in range(4)]
        word = jnp.where(
            x < 2,
            jnp.where(x == 0, words[0], words[1]),
            jnp.where(x == 2, words[2], words[3]),
        )
        return lax.shift_right_logical(word, 8 * y) & 0xFF

    def guarded(mask, action):
        if mask == 0:
            return
        if mask == 0xFFFF:
            action()
            return
        pl.when((lax.shift_right_logical(jnp.int32(mask), p) & 1) == 1)(action)

    def transfer(step, d, source, target, size, arrival):
        return pltpu.make_async_remote_copy(
            src_ref=held.at[pl.ds(source, size)],
            dst_ref=held.at[pl.ds(target, size)],
            send_sem=send_sem.at[SENDS * d + step % SENDS],
            recv_sem=recv_sem.at[arrival],
            device_id=targets[d],
            device_id_type=MESH,
        )

    def for_each_size(sizes, action, among=0xFFFF):
        for size in sorted(set(sizes) - {0}):
            guarded(mask_of(v == size for v in sizes) & among, functools.partial(action, size))

    def send(step, d):
        waits = mask_of((NEEDS[step][d] >> (8 * q)) & 255 != NO_WAIT for q in range(16))

        def arrived(size):
            transfer(step, d, 0, UNITS, size, needed(step, d)).wait_recv()

        def action(size):
            source = chosen(step, d)
            transfer(step, d, source, source - UNITS * ahead[d], size, SEMAPHORES[step][d]).start()

        sizes = [size_of(v) for v in entries(step, d)]
        for_each_size(sizes, arrived, waits)
        for_each_size(sizes, action)

    def receive(step, d):
        sent = [size_of(v) for v in entries(step, d)]
        coming = [sent[neighbour_position(q, OPPOSITE[d])] for q in range(16)]
        for_each_size(coming, lambda size: transfer(step, d, 0, UNITS, size, SEMAPHORES[step][d]).wait_recv(), LATE[step][d])

    def finish(step, d):
        sent = [size_of(v) for v in entries(step, d)]
        for_each_size(sent, lambda size: transfer(step, d, 0, UNITS, size, SEMAPHORES[step][d]).wait_send())

    exchange = pltpu.make_async_remote_copy(
        src_ref=part,
        dst_ref=part_in,
        send_sem=pair_sem.at[0],
        recv_sem=pair_sem.at[1],
        device_id=twin,
        device_id_type=MESH,
    )

    for step in range(steps):
        if step >= LATE_BY:
            for d in range(6):
                receive(step - LATE_BY, d)
        for d in ORDER:
            if step >= SENDS:
                finish(step - SENDS, d)
            send(step, d)
        if step == 0:
            total = jnp.zeros((tiles, UNIT, LANES), jnp.float32)
            for i in range(4 * bins):
                piece = held[pl.ds(i * tiles, tiles)].astype(jnp.float32)
                total += piece * piece
            total = total.reshape(tiles * UNIT, LANES)
            power = jnp.sum(total.T, axis=0, keepdims=True)
            part[...] = jnp.broadcast_to(power, part.shape)
            exchange.start()
        if step == GAIN_STEP:
            exchange.wait()
            power = part[...] + part_in[...]
            gain = 1.0 / jnp.sqrt(power * (1.0 / 2048.0))
            gain = jnp.concatenate([gain, gain], axis=0)
            high = gain.astype(jnp.bfloat16).astype(jnp.float32)
            middle = (gain - high).astype(jnp.bfloat16).astype(jnp.float32)
            low = gain - high - middle
            row = lax.broadcasted_iota(jnp.int32, (UNIT, LANES), 0)
            rest = jnp.where(row == 1, middle, low)
            held[UNITS - 1] = jnp.where(row == 0, high, rest).astype(jnp.bfloat16)
    for step in range(steps - LATE_BY, steps):
        for d in range(6):
            receive(step, d)
    for step in range(steps - SENDS, steps):
        for d in range(6):
            finish(step, d)


def gathered(re, im):
    bins, tiles = re.shape[:2]
    steps = len(PLAN)
    return pl.pallas_call(
        gather_kernel,
        out_shape=jax.ShapeDtypeStruct((SLOTS * UNITS, UNIT, LANES), jnp.bfloat16),
        in_specs=[pl.BlockSpec(memory_space=pltpu.HBM)] * 2,
        out_specs=pl.BlockSpec(memory_space=pltpu.VMEM),
        scratch_shapes=[
            pltpu.VMEM((8, 128), jnp.float32),
            pltpu.VMEM((8, 128), jnp.float32),
            pltpu.SemaphoreType.DMA((6 * SENDS,)),
            pltpu.SemaphoreType.DMA((max(map(max, SEMAPHORES)) + 1,)),
            pltpu.SemaphoreType.DMA((1,)),
            pltpu.SemaphoreType.DMA((2,)),
        ],
        compiler_params=pltpu.CompilerParams(
            collective_id=0, has_side_effects=True, vmem_limit_bytes=24 << 20
        ),
        name="gather_blocks",
    )(re, im)


GROUP = 11


def gain_row(tile):
    wide = tile.astype(jnp.float32)
    return wide[0:1] + wide[1:2] + wide[2:3]


def spectra(held, f, first):
    halves = [held[pl.ds(first + 32 * f + 16 * h, 16)].reshape(256, LANES) for h in range(2)]
    return jnp.concatenate(halves, axis=1)


def cross_kernel(plan, held, out, order, staged, own_column, sem, order_sem):
    bins = out.shape[0]
    fetch = pltpu.make_async_copy(plan, order, order_sem)
    fetch.start()
    own_row = gain_row(held[UNITS - 1]) * (1.0 / 16.0)
    own_column[...] = jnp.broadcast_to(own_row, (128, 128)).T
    fetch.wait()

    def group(i, carry):
        for j in range(GROUP):
            place = i * GROUP + j
            first = order[0, place] * UNITS
            weight = own_column[...] * gain_row(held[first + UNITS - 1])
            for f in range(bins):
                mine, other = spectra(held, f, 0), spectra(held, f, first)
                full = lax.dot_general(
                    mine, other, (((1,), (1,)), ((), ())), preferred_element_type=jnp.float32
                )
                staged[place, f, :, :128] = (full[:128, :128] + full[128:, 128:]) * weight
                staged[place, f, :, 128:] = (full[128:, :128] - full[:128, 128:]) * weight
            pltpu.make_async_copy(staged.at[place], out.at[:, place], sem).start()
        return carry

    lax.fori_loop(0, SLOTS // GROUP, group, 0)
    pltpu.make_async_copy(staged, staged, sem).wait()


def local(spec_re, spec_im, offsets):
    bins, rows, segs = spec_re.shape
    tiles = rows // UNIT
    re = spec_re.reshape(bins, tiles, UNIT, segs)
    im = spec_im.reshape(bins, tiles, UNIT, segs)
    re = pltpu.with_memory_space_constraint(re, pltpu.HBM)
    im = pltpu.with_memory_space_constraint(im, pltpu.HBM)
    held = gathered(re, im)
    cross = pl.pallas_call(
        cross_kernel,
        in_specs=[pl.BlockSpec(memory_space=pl.ANY), pl.BlockSpec(memory_space=pltpu.VMEM)],
        out_specs=pl.BlockSpec(memory_space=pltpu.HBM),
        out_shape=jax.ShapeDtypeStruct((bins, SLOTS, rows, 256), jnp.float32),
        scratch_shapes=[
            pltpu.SMEM((1, SLOTS), jnp.int32),
            pltpu.VMEM((SLOTS, bins, rows, 256), jnp.float32),
            pltpu.VMEM((rows, rows), jnp.float32),
            pltpu.SemaphoreType.DMA,
            pltpu.SemaphoreType.DMA,
        ],
        compiler_params=pltpu.CompilerParams(vmem_limit_bytes=30 << 20),
        name="cross_products",
    )(offsets, held)
    return cross[:, None]


def solution(mesh):
    placed = (P("fr", ("sr", "sc"), None), P("fr", ("sr", "sc"), None), P(("sr", "sc"), None))
    return jax.shard_map(
        local,
        mesh=mesh,
        in_specs=placed,
        out_specs=P("fr", ("sr", "sc"), None, None, None),
        check_vma=False,
    )
```
